32 devices in a mesh: pb: 4 (over y, x), wa: 8 (over z, core).
Axes of the slice: x: 2, y: 2, z: 4, core: 2. Of those that a mesh axis runs over, the one named last changes fastest.
Arguments:
- quartets: int32 [1024, 4, 128], P(('pb', 'wa')), may hold values from -1 to 49151, as said below
- counts: int32 [32], P(('pb', 'wa')), may hold values from 1 to 32, as said below
- eig: bfloat16 [24, 49152], P(None, 'pb'), may hold values from -1.1953125 to 1.1953125
- freq: bfloat16 [49152], P('pb'), may hold values from 0.5 to 2
- phi: bfloat16 [144, 1152], replicated, may hold values from -0.5390625 to 0.5390625
- cells: int32 [8, 9], replicated, may hold values from -2 to 2
Outputs:
- rates: float32 [49152], P(('pb', 'wa'))
The draws below stay inside these ranges and needn't reach their ends.
Inputs may be any that keep to these rules, and one draw needn't show every extreme that they name: quartets[b, 0, n] is a mode of one of the 1024 q-points of the owner group of slot b (from 0 to 12287); the other three entries are all -1 or all modes of the mesh, and then their q-points and that of the first add up as q1 + q2 = q3 + q4 on the mesh. The used slots of a device are its first counts slots; some device has exactly 32.
All inputs are finite; a program needn't handle non-finite values.
Results may differ from the reference program's by a relative error of at most 0.0023.
Values may be sent and summed in bfloat16 or wider, within the bound.
No kernel may reach another device: no remote copies, remote signals or barrier semaphores. Data moves between devices by JAX's collectives and lax.ppermute only.
A program may use at most 64 MiB of HBM per device.

```python
import math
import jax
import jax.numpy as jnp
from jax import lax

QMESH = 16
BRANCHES = 12
CLUSTERS = 8
BLOCK = 128
BLK_DEV = 32
NQ = 4096
NMODE = 49152
Q_DEV = 1024
WORKERS = 32
SHARD_BLK = 256
NBLK = 1024


def mesh_point(across, along, upward):
    return (across * QMESH + along) * QMESH + upward


def draw_quartets(key, part):
    local_q = jax.random.randint(jax.random.fold_in(key, 1), (NBLK, 1), 0, Q_DEV)
    owner = (jnp.arange(NBLK, dtype=jnp.int32) // SHARD_BLK)[:, None]
    first_q = owner * Q_DEV + local_q
    second_q = jax.random.randint(jax.random.fold_in(key, 2), (NBLK, BLOCK), 0, NQ)
    third_q = jax.random.randint(jax.random.fold_in(key, 3), (NBLK, BLOCK), 0, NQ)
    square = QMESH * QMESH
    fourth_q = mesh_point(jnp.remainder(first_q // square + second_q // square - third_q // square, QMESH), jnp.remainder(first_q // QMESH % QMESH + second_q // QMESH % QMESH - third_q // QMESH % QMESH, QMESH), jnp.remainder(first_q % QMESH + second_q % QMESH - third_q % QMESH, QMESH))
    branch_draw = jax.random.randint(jax.random.fold_in(key, 4), (4, NBLK, BLOCK), 0, BRANCHES)
    pad_length = jax.random.randint(jax.random.fold_in(key, 5), (NBLK, 1), 0, BLOCK // 2 + 1)
    padded = jnp.arange(BLOCK, dtype=jnp.int32)[None, :] >= BLOCK - pad_length
    first_mode = local_q * BRANCHES + branch_draw[0]
    second_mode = jnp.where(padded, -1, second_q * BRANCHES + branch_draw[1])
    third_mode = jnp.where(padded, -1, third_q * BRANCHES + branch_draw[2])
    fourth_mode = jnp.where(padded, -1, fourth_q * BRANCHES + branch_draw[3])
    return jnp.stack([first_mode, second_mode, third_mode, fourth_mode], axis=1).astype(jnp.int32)


def draw_counts(key, part):
    first_draw = jax.random.randint(jax.random.fold_in(key, 11), (WORKERS,), 1, BLK_DEV + 1)
    second_draw = jax.random.randint(jax.random.fold_in(key, 12), (WORKERS,), 1, BLK_DEV + 1)
    chosen = jax.random.randint(jax.random.fold_in(key, 13), (), 0, WORKERS)
    tally = jnp.maximum(1, first_draw * second_draw // BLK_DEV)
    tally = jnp.where(jnp.arange(WORKERS, dtype=jnp.int32) == chosen, BLK_DEV, tally)
    return tally.astype(jnp.int32)


def with_ends(values, key, low, high):
    place = [jax.random.randint(jax.random.fold_in(key, axis), (), 0, length) for axis, length in enumerate(values.shape)]
    widest = values.shape.index(max(values.shape))
    beside = place[:widest] + [(place[widest] + 1) % values.shape[widest]] + place[widest + 1:]
    return values.at[tuple(place)].set(low).at[tuple(beside)].set(high)


def steps_of(rng, extent, shards, low, largest):
    def one(position, shards_of):
        steps = jax.random.uniform(jax.random.fold_in(jax.random.fold_in(rng, 6), position), (shards_of,), jnp.float32, low / len(shards), largest / len(shards))
        return jnp.repeat(jnp.exp(steps), extent[position] // shards_of).reshape((-1,) + (1,) * (len(extent) - position - 1))

    factor_of = one(*shards[0])
    for cut in shards[1:]:
        factor_of = factor_of * one(*cut)
    return factor_of


def centred(rng, extent, spread, limit, shards=(), held_as=jnp.bfloat16):
    drawn = jax.random.normal(rng, extent, jnp.float32) * spread
    if len(shards) > 0:
        drawn = steps_of(rng, extent, shards, -0.22, 0.18) * drawn
    return jnp.clip(drawn, min=-limit, max=limit).astype(held_as)


def setup_inputs(seed: int = 0) -> dict:
    key_list = jax.random.split(jax.random.key(seed), 7)
    return {
        "quartets": draw_quartets(jax.random.fold_in(key_list[6], 71), 0),
        "counts": draw_counts(jax.random.fold_in(key_list[6], 71), 0),
        "eig": centred(key_list[2], (2 * BRANCHES, NMODE), 0.2, 1.1953125, ((1, 4),)),
        "freq": jnp.clip(jnp.exp(math.log(2.0) - 1.3862944 * jax.random.uniform(key_list[3], (NMODE,), jnp.float32) ** steps_of(key_list[3], (NMODE,), ((0, 4),), -0.2, 0.2)), 0.5, 2.0).astype(jnp.bfloat16),
        "phi": centred(key_list[4], (BRANCHES * BRANCHES, CLUSTERS * BRANCHES * BRANCHES), 0.09, 0.5390625),
        "cells": with_ends(jax.random.randint(key_list[5], (CLUSTERS, 9), -2, 3), jax.random.fold_in(key_list[5], 1), -2, 2).astype(jnp.int32),
    }


smearing = 0.5

def outer_pair(first, second, branches):
    count = first.shape[1]
    first_re = first[:branches][:, None, :]
    first_im = first[branches:][:, None, :]
    second_re = second[:branches][None, :, :]
    second_im = second[branches:][None, :, :]
    real = (first_re * second_re - first_im * second_im).reshape(branches * branches, count)
    imag = (first_re * second_im + first_im * second_re).reshape(branches * branches, count)
    return (real, imag)

def cluster_phase(other_modes, cells, branches):
    points = other_modes // branches
    coords = [points // (QMESH * QMESH), points // QMESH % QMESH, points % QMESH]
    shift = jnp.zeros((cells.shape[0], other_modes.shape[1]), jnp.int32)
    for which in range(3):
        sign = 1 if which == 0 else -1
        for axis_c in range(3):
            shift = shift + sign * cells[:, 3 * which + axis_c][:, None] * coords[axis_c][which][None, :]
    angle = jnp.remainder(shift, QMESH).astype(jnp.float32) * (2.0 * math.pi / QMESH)
    return (jnp.cos(angle), jnp.sin(angle))

def occupation(value):
    return 1.0 / (jnp.exp(value) - 1.0)

def contributions(first_modes, other_modes, other_spots, valid, first_vectors, first_freqs, vectors, frequencies, phi, cells):
    branches = vectors.shape[0] // 2
    count = first_modes.shape[0]
    clusters = cells.shape[0]
    first_vec = jnp.take(first_vectors, first_modes, axis=1).astype(jnp.float32)
    first_freq = jnp.take(first_freqs, first_modes).astype(jnp.float32)
    flat_spots = other_spots.reshape(3 * count)
    gathered = jnp.take(vectors, flat_spots, axis=1).astype(jnp.float32)
    other_freq = jnp.take(frequencies, flat_spots).astype(jnp.float32).reshape(3, count)
    second_vec = gathered[:, :count]
    third_vec = gathered[:, count:2 * count]
    fourth_vec = gathered[:, 2 * count:]
    far_re, far_im = outer_pair(third_vec, fourth_vec, branches)
    far_im = -far_im
    cosine, sine = cluster_phase(other_modes, cells, branches)
    wide_re = cosine[:, None, :] * far_re[None] - sine[:, None, :] * far_im[None]
    wide_im = cosine[:, None, :] * far_im[None] + sine[:, None, :] * far_re[None]
    wide_re = wide_re.reshape(clusters * branches * branches, count).astype(jnp.bfloat16)
    wide_im = wide_im.reshape(clusters * branches * branches, count).astype(jnp.bfloat16)
    weighted_re = jnp.dot(phi, wide_re, preferred_element_type=jnp.float32)
    weighted_im = jnp.dot(phi, wide_im, preferred_element_type=jnp.float32)
    near_re, near_im = outer_pair(first_vec, second_vec, branches)
    value_re = lax.optimization_barrier(jnp.sum(near_re * weighted_re - near_im * weighted_im, axis=0))
    value_im = lax.optimization_barrier(jnp.sum(near_re * weighted_im + near_im * weighted_re, axis=0))
    mismatch = first_freq + other_freq[0] - other_freq[1] - other_freq[2]
    delta = jnp.exp(-(mismatch / smearing) ** 2) / (smearing * math.sqrt(math.pi))
    weight = (1.0 + occupation(other_freq[0])) * occupation(other_freq[1]) * occupation(other_freq[2]) / occupation(first_freq)
    product = first_freq * other_freq[0] * other_freq[1] * other_freq[2]
    return jnp.where(valid, (value_re * value_re + value_im * value_im) * delta * weight / product, 0.0)

def reference(quartets, counts, eig, freq, phi, cells):
    total_blocks = quartets.shape[0]
    block = quartets.shape[2]
    group = math.gcd(BLK_DEV, 16)
    index = jnp.arange(total_blocks, dtype=jnp.int32)
    used = index % BLK_DEV < jnp.take(counts, index // BLK_DEV)
    rank = (jnp.cumsum(used.astype(jnp.int32)) - 1).astype(jnp.int32)
    target = jnp.where(used, rank, total_blocks).astype(jnp.int32)
    order = jnp.zeros((total_blocks,), jnp.int32).at[target].set(index, mode='drop')
    total = jnp.sum(used.astype(jnp.int32)).astype(jnp.int32)
    offsets = (index // SHARD_BLK * (Q_DEV * BRANCHES)).astype(jnp.int32)
    rounds = (total + group - 1) // group

    def one_round(step, rates):
        start = (step * group).astype(jnp.int32)
        picks = lax.dynamic_slice_in_dim(order, start, group, 0)
        blocks = jnp.take(quartets, picks, axis=0)
        live = start + jnp.arange(group, dtype=jnp.int32) < total
        first_modes = (blocks[:, 0, :] + jnp.take(offsets, picks)[:, None]).reshape(group * block)
        others = jnp.transpose(blocks[:, 1:, :], (1, 0, 2)).reshape(3, group * block)
        valid = (others[0] >= 0) & jnp.repeat(live, block)
        clamped = jnp.maximum(others, 0)
        terms = contributions(first_modes, clamped, clamped, valid, eig, freq, eig, freq, phi, cells)
        return rates.at[first_modes].add(terms)
    return lax.fori_loop(0, rounds, one_round, jnp.zeros((eig.shape[1],), jnp.float32))
```

```python
import functools
import math

import jax
import jax.numpy as jnp
from jax import lax
from jax.experimental import pallas as pl
from jax.experimental.pallas import tpu as pltpu
from jax.sharding import PartitionSpec as P

QMESH = 16
LANES = 128
SUB = 8
GROUPS = 4
SLOT = LANES // GROUPS

smearing = 0.5


def occupation(value):
    return 1.0 / (jnp.exp(value) - 1.0)


def row_iota(rows):
    return lax.broadcasted_iota(jnp.int32, (rows, LANES), 0)


def freq_chunk(piece, comps, half, start):
    per_row = half // comps
    parts = []
    at = start
    while at < start + LANES:
        row, lane = divmod(at, per_row)
        width = min(per_row - lane, start + LANES - at)
        parts.append(piece[row : row + 1, half + lane : half + lane + width])
        at += width
    return parts[0] if len(parts) == 1 else jnp.concatenate(parts, axis=1)


def fill_table(pieces, table, comps, half):
    shards = len(pieces) // 2
    for block in range(shards // GROUPS):
        for side in range(2):
            for start in range(0, half, LANES):
                stack = []
                for g in range(GROUPS):
                    piece = pieces[2 * (block * GROUPS + g) + side]
                    stack.append(piece[:, start : start + LANES].astype(jnp.float32))
                    line = freq_chunk(piece, comps, half, start).astype(jnp.float32)
                    stack.append(jnp.broadcast_to(line, (SLOT - comps, LANES)))
                row = (2 * block + side) * half + start
                table[row : row + LANES, :] = jnp.concatenate(stack, axis=0).T


def kernel(
    branches,
    half,
    heads,
    order,
    total,
    rows_hbm,
    meta,
    first_table,
    phi,
    cells,
    *refs,
):
    pieces = refs[:-7]
    out, table, near, spots, wide, acc, sems = refs[-7:]
    comps = 2 * branches
    clusters = SUB
    log = QMESH.bit_length() - 1
    count = total[0]

    def load(i):
        slot = lax.rem(i, 2)
        return pltpu.make_async_copy(rows_hbm.at[order[i]], spots.at[slot], sems.at[slot])

    @pl.when(count > 0)
    def _():
        load(0).start()

    fill_table(pieces, table, comps, half)
    acc[...] = jnp.zeros_like(acc)

    def one_block(i, carry):
        slot = lax.rem(i, 2)
        load(i).wait()

        @pl.when(i + 1 < count)
        def _():
            load(i + 1).start()

        for which in range(3):
            for n in range(LANES):
                at = which * LANES + n
                near[at : at + 1, :] = table[pl.ds(spots[slot, which, n], 1), :]
        info = meta[order[i]]
        others = []
        points = []
        for which in range(3):
            word = info[which + 1 : which + 2, :]
            group = lax.shift_right_logical(word, 16)
            points.append(word & 0xFFFF)
            flat = near[which * LANES : (which + 1) * LANES, :].T
            pick = flat[:SLOT]
            for g in range(1, GROUPS):
                pick = jnp.where(group == g, flat[g * SLOT : (g + 1) * SLOT], pick)
            others.append(pick)
        second, third, fourth = others
        local = info[0:1, :]
        head = lax.shift_right_arithmetic(local, 7)
        hot = jnp.where(row_iota(LANES) == (local & (LANES - 1)), 1.0, 0.0).astype(jnp.bfloat16)
        spread = jnp.dot(first_table[...], hot, preferred_element_type=jnp.float32)
        first = jnp.zeros((comps, LANES), jnp.float32)
        for h in range(heads):
            first = jnp.where(head == h, spread[h * comps : (h + 1) * comps], first)
        lines = spread[heads * comps :]
        first_freq = jnp.sum(
            jnp.where(row_iota(lines.shape[0]) == head, lines, 0.0), axis=0, keepdims=True
        )
        shift = jnp.zeros((clusters, LANES), jnp.int32)
        for which in range(3):
            p = points[which]
            coords = (
                lax.shift_right_logical(p, 2 * log),
                lax.shift_right_logical(p, log) & (QMESH - 1),
                p & (QMESH - 1),
            )
            for axis in range(3):
                shift = shift + cells[3 * which + axis] * coords[axis]
        angle = (shift & (QMESH - 1)).astype(jnp.float32) * (2.0 * math.pi / QMESH)
        cosine, sine = jnp.cos(angle), jnp.sin(angle)
        turned = []
        for d in range(branches):
            re = fourth[d : d + 1]
            im = fourth[branches + d : branches + d + 1]
            turned.append((cosine * re + sine * im, sine * re - cosine * im))
        for c in range(branches):
            re = third[c : c + 1]
            im = third[branches + c : branches + c + 1]
            for d in range(0, branches, 2):
                at = (c * branches + d) * clusters
                pair_re, pair_im = [], []
                for tre, tim in turned[d : d + 2]:
                    pair_re.append(re * tre + im * tim)
                    pair_im.append(re * tim - im * tre)
                both = (jnp.concatenate(pair_re, axis=0), jnp.concatenate(pair_im, axis=0))
                for side in range(2):
                    wide[at : at + 2 * clusters, side * LANES : (side + 1) * LANES] = both[
                        side
                    ].astype(jnp.bfloat16)
        weighted = jnp.dot(phi[...], wide[...], preferred_element_type=jnp.float32)
        tail = branches - SUB
        low = row_iota(SUB) < tail
        head_re = jnp.zeros((SUB, LANES), jnp.float32)
        head_im, tail_re, tail_im = head_re, head_re, head_re
        for b in range(branches):
            wre = weighted[b * SUB : (b + 1) * SUB, :LANES]
            wim = weighted[b * SUB : (b + 1) * SUB, LANES:]
            re, im = second[b : b + 1], second[branches + b : branches + b + 1]
            head_re = head_re + (re * wre - im * wim)
            head_im = head_im + (re * wim + im * wre)
        for j in range(branches * tail // SUB):
            at = branches * SUB + j * SUB
            wre = weighted[at : at + SUB, :LANES]
            wim = weighted[at : at + SUB, LANES:]
            b = 2 * j
            re = jnp.where(low, second[b : b + 1], second[b + 1 : b + 2])
            im = jnp.where(
                low, second[branches + b : branches + b + 1], second[branches + b + 1 : branches + b + 2]
            )
            tail_re = tail_re + (re * wre - im * wim)
            tail_im = tail_im + (re * wim + im * wre)
        top_re, mid, top_im = first[:SUB], first[SUB : 2 * SUB], first[2 * SUB :]
        turned_mid = jnp.concatenate([mid[tail:], mid[:tail]], axis=0)
        end_re = jnp.where(low, mid, turned_mid)
        end_im = jnp.where(low, turned_mid, mid)
        value_re = jnp.sum(
            top_re * head_re - top_im * head_im + (end_re * tail_re - end_im * tail_im),
            axis=0,
            keepdims=True,
        )
        value_im = jnp.sum(
            top_re * head_im + top_im * head_re + (end_re * tail_im + end_im * tail_re),
            axis=0,
            keepdims=True,
        )
        f2, f3, f4 = (e[comps : comps + 1] for e in others)
        mismatch = first_freq + f2 - f3 - f4
        delta = jnp.exp(-((mismatch / smearing) ** 2)) / (smearing * math.sqrt(math.pi))
        weight = (
            (1.0 + occupation(f2)) * occupation(f3) * occupation(f4) / occupation(first_freq)
        )
        product = first_freq * f2 * f3 * f4
        term = (value_re * value_re + value_im * value_im) * delta * weight / product
        term = jnp.where(local >= 0, term, 0.0)
        placed = jnp.where(row_iota(acc.shape[0]) == head, term, 0.0)
        parts = []
        for _ in range(3):
            part = placed.astype(jnp.bfloat16)
            parts.append(part)
            placed = placed - part.astype(jnp.float32)
        sums = lax.dot_general(
            jnp.concatenate(parts, axis=0),
            hot,
            (((1,), (1,)), ((), ())),
            preferred_element_type=jnp.float32,
        )
        size = acc.shape[0]
        acc[...] += sums[:size] + sums[size : 2 * size] + sums[2 * size :]
        return carry

    lax.fori_loop(0, count, one_block, 0)
    out[...] = acc[:heads, :]


def body(quartets, counts, eig, freq, phi, cells):
    comps, local = eig.shape
    branches = comps // 2
    shards = lax.axis_size("pb")
    workers = lax.axis_size("wa")
    held = quartets.shape[0]
    block = quartets.shape[2]
    half = local // 2
    mine = lax.axis_index("pb")
    worker = lax.axis_index("wa")
    side = worker % 2
    kept = local // workers
    heads = -(-kept // LANES)
    clusters = cells.shape[0]

    def half_shard(which):
        vectors = lax.dynamic_slice_in_dim(eig, which * half, half, 1)
        lines = lax.dynamic_slice_in_dim(freq, which * half, half, 0)
        return jnp.concatenate([vectors, lines.reshape(comps, half // comps)], axis=1)

    own = half_shard(side)
    pieces = [own, half_shard(1 - side)]
    far = [
        lax.ppermute(own, "pb", [(i, i ^ k) for i in range(shards)]) for k in range(1, shards)
    ]
    for piece in far:
        pieces += [piece, lax.ppermute(piece, "wa", [(i, i ^ 1) for i in range(workers)])]

    slots = jnp.arange(held, dtype=jnp.int32)[:, None, None]
    marked = jnp.where(slots < counts[0], quartets, -1)
    pool = lax.all_gather(marked, "wa", axis=0, tiled=True)
    index = jnp.arange(pool.shape[0], dtype=jnp.int32)
    first = pool[:, 0, :] - worker * kept
    valid = (pool[:, 1, :] >= 0) & (first >= 0) & (first < kept)
    flags = jnp.any(valid, axis=1)
    place = jnp.cumsum(flags.astype(jnp.int32)) - 1
    order = jnp.sum(
        jnp.where((place[None, :] == index[:, None]) & flags[None, :], index[None, :], 0), axis=1
    )
    total = jnp.sum(flags.astype(jnp.int32)).reshape(1)
    modes = jnp.maximum(pool[:, 1:, :], 0)
    owner = modes // local
    inner = modes - owner * local
    near = owner ^ mine
    rows = (near // GROUPS) * local + ((inner // half) ^ side) * half + inner % half
    words = modes // branches + (near % GROUPS) * 65536
    meta = jnp.concatenate([jnp.where(valid, first, -1)[:, None, :], words], axis=1)

    own_vectors = lax.dynamic_slice_in_dim(eig, worker * kept, kept, 1)
    own_vectors = jnp.pad(own_vectors, ((0, 0), (0, heads * LANES - kept)))
    own_vectors = jnp.concatenate(
        [
            own_vectors[:branches],
            own_vectors[branches + SUB :],
            own_vectors[branches : branches + SUB],
        ],
        axis=0,
    )
    own_vectors = own_vectors.reshape(comps, heads, LANES).transpose(1, 0, 2)
    own_lines = lax.dynamic_slice_in_dim(freq, worker * kept, kept, 0)
    own_lines = jnp.pad(own_lines, (0, heads * LANES - kept)).reshape(heads, LANES)
    padded = -(-heads // 16) * 16
    first_table = jnp.concatenate(
        [
            own_vectors.reshape(heads * comps, LANES),
            own_lines,
            jnp.zeros((padded - heads, LANES), own_lines.dtype),
        ],
        axis=0,
    )
    grid_phi = phi.reshape(branches, branches, clusters, branches, branches)
    grid_phi = grid_phi.transpose(1, 0, 3, 4, 2)
    width = phi.shape[1]
    ordered_phi = jnp.concatenate(
        [
            grid_phi[:, :SUB].reshape(branches * SUB, width),
            grid_phi[:, SUB:].reshape(branches * (branches - SUB), width),
        ],
        axis=0,
    )
    signed = jnp.concatenate([cells[:, :3], -cells[:, 3:]], axis=1)
    spread_cells = jnp.broadcast_to(signed.T[:, :, None], (9, clusters, LANES))

    vmem = pl.BlockSpec(memory_space=pltpu.VMEM)
    smem = pl.BlockSpec(memory_space=pltpu.SMEM)
    rates = pl.pallas_call(
        functools.partial(kernel, branches, half, heads),
        out_shape=jax.ShapeDtypeStruct((heads, LANES), jnp.float32),
        in_specs=[smem, smem, pl.BlockSpec(memory_space=pl.ANY)] + [vmem] * (4 + len(pieces)),
        out_specs=vmem,
        scratch_shapes=[
            pltpu.VMEM((shards // GROUPS * local, LANES), jnp.float32),
            pltpu.VMEM((3 * LANES, LANES), jnp.float32),
            pltpu.SMEM((2, 3, LANES), jnp.int32),
            pltpu.VMEM((width, 2 * LANES), jnp.bfloat16),
            pltpu.VMEM((padded, LANES), jnp.float32),
            pltpu.SemaphoreType.DMA((2,)),
        ],
        compiler_params=pltpu.CompilerParams(vmem_limit_bytes=32 * 1024 * 1024),
    )(order, total, rows, meta, first_table, ordered_phi, spread_cells, *pieces)
    return rates.reshape(heads * LANES)[:kept]


def solution(mesh):
    placed = (P(("pb", "wa"), None, None), P(("pb", "wa")), P(None, "pb"), P("pb"), P(), P())
    return jax.shard_map(
        body, mesh=mesh, in_specs=placed, out_specs=P(("pb", "wa")), check_vma=False
    )
```

```python
import functools
import math

import jax
import jax.numpy as jnp
from jax import lax
from jax.experimental import pallas as pl
from jax.experimental.pallas import tpu as pltpu
from jax.sharding import PartitionSpec as P

QMESH = 16
LANES = 128
SUB = 8
GROUPS = 4
SLOT = LANES // GROUPS
PARTS = 4

smearing = 0.5


def occupation(value):
    return 1.0 / (jnp.exp(value) - 1.0)


def row_iota(rows):
    return lax.broadcasted_iota(jnp.int32, (rows, LANES), 0)


def window(kept):
    return -(-(kept + LANES - math.gcd(kept, LANES)) // LANES)


def prepare(branches, local, kept, offset, *refs):
    pool, (rows_out, meta_out, flags_out) = refs[:-3], refs[-3:]
    mine = lax.axis_index("pb")
    side = lax.rem(lax.axis_index("wa"), 2)
    start = lax.axis_index("wa") * kept
    lead = lax.rem(start, LANES)
    shards = lax.axis_size("pb")
    modes = jnp.concatenate([r[...].astype(jnp.int32) for r in pool], axis=0) + offset
    count = modes.shape[0]
    heading = (row_iota(count) & (PARTS - 1)) == 0
    safe = jnp.maximum(modes, 0)
    middle = safe.astype(jnp.float32) + 0.5
    owner = (middle * (1.0 / local)).astype(jnp.int32)
    point = (middle * (1.0 / branches)).astype(jnp.int32)
    near = owner ^ mine
    group = near
    if shards == GROUPS:
        group = jnp.where(near == 1, 1 + side, jnp.where(near == 2, 2 - side, near))
    rows_out[...] = (group >> 2) * local + (safe - owner * local)
    following = pltpu.roll(modes, count - 1, 0)
    first = modes - start
    valid = heading & (following >= 0) & (first >= 0) & (first < kept)
    meta_out[...] = jnp.where(
        heading, jnp.where(valid, first + lead, -1), point + (group & (GROUPS - 1)) * 65536
    )
    flags_out[...] = lax.dot_general(
        jnp.ones((SUB, LANES), jnp.bfloat16),
        jnp.where(valid, 1.0, 0.0).astype(jnp.bfloat16),
        (((1,), (1,)), ((), ())),
        preferred_element_type=jnp.float32,
    )


def fill_table(shards, lines, table):
    comps, local = shards[0].shape
    for block in range(len(shards) // GROUPS):
        for t in range(local // LANES):
            stack = []
            for g in range(GROUPS):
                at = block * GROUPS + g
                stack.append(shards[at][:, t * LANES : (t + 1) * LANES].astype(jnp.float32))
                line = lines[at][t : t + 1, :].astype(jnp.float32)
                stack.append(jnp.broadcast_to(line, (SLOT - comps, LANES)))
            row = block * local + t * LANES
            table[row : row + LANES, :] = jnp.concatenate(stack, axis=0).T


def held_rows(e, branches):
    out = []
    for v in range(branches * branches // SUB):
        low, high = v * SUB // branches, (v * SUB + SUB - 1) // branches
        if low == high:
            out.append(jnp.broadcast_to(e[low : low + 1], (SUB, LANES)))
        else:
            cut = high * branches - v * SUB
            out.append(jnp.where(row_iota(SUB) < cut, e[low : low + 1], e[high : high + 1]))
    return out


def cycled_rows(e, branches):
    period = math.lcm(SUB, branches)
    twice = jnp.concatenate([e[:branches]] * (period // branches), axis=0)
    return [twice[v * SUB : (v + 1) * SUB] for v in range(period // SUB)]


def kernel(branches, kept, shards, order, total, rows_hbm, meta, phi, cells, *refs):
    vectors, lines = refs[:shards], refs[shards : 2 * shards]
    out, table, near_a, near_b, spots_a, spots_b, wide, own, acc, sems = refs[2 * shards :]
    comps = 2 * branches
    pairs = branches * branches
    clusters = SUB
    heads = out.shape[0]
    log = QMESH.bit_length() - 1
    count = total[0]

    last = rows_hbm.shape[0] - 1

    def load(i, spots, which):
        return pltpu.make_async_copy(
            rows_hbm.at[order[jnp.minimum(i, last)]], spots, sems.at[which]
        )

    load(0, spots_a, 0).start()
    load(1, spots_b, 1).start()

    fill_table(vectors, lines, table)
    start = lax.axis_index("wa") * kept // LANES
    own_lines = lines[0][...].astype(jnp.float32)
    line_rows = row_iota(own_lines.shape[0])
    tops = []
    for h in range(heads):
        at = pl.multiple_of((start + h) * LANES, LANES)
        own[h * comps : (h + 1) * comps, :] = vectors[0][:, pl.ds(at, LANES)].astype(jnp.float32)
        tops.append(
            jnp.sum(jnp.where(line_rows == start + h, own_lines, 0.0), axis=0, keepdims=True)
        )
    filler = own.shape[0] - heads * comps - heads
    tops.append(jnp.zeros((filler, LANES), jnp.float32))
    own[heads * comps :, :] = jnp.concatenate(tops, axis=0)
    first_table = own[...].astype(jnp.bfloat16)
    acc[...] = jnp.zeros_like(acc)

    def gather(spots, near):
        for which in range(3):
            for n in range(LANES):
                at = which * LANES + n
                near[at : at + 1, :] = table[pl.ds(spots[which + 1, n], 1), :]

    def contract(i, near):
        info = meta[order[i]]
        others = []
        points = []
        for which in range(3):
            word = info[which + 1 : which + 2, :]
            group = lax.shift_right_logical(word, 16)
            points.append(word & 0xFFFF)
            flat = near[which * LANES : (which + 1) * LANES, :].T
            pick = flat[:SLOT]
            for g in range(1, GROUPS):
                pick = jnp.where(group == g, flat[g * SLOT : (g + 1) * SLOT], pick)
            others.append(pick)
        second, third, fourth = others
        local = info[0:1, :]
        head = lax.shift_right_arithmetic(local, 7)
        hot = jnp.where(row_iota(LANES) == (local & (LANES - 1)), 1.0, 0.0).astype(jnp.bfloat16)
        spread = jnp.dot(first_table, hot, preferred_element_type=jnp.float32)
        first = jnp.zeros((comps, LANES), jnp.float32)
        for h in range(heads):
            first = jnp.where(head == h, spread[h * comps : (h + 1) * comps], first)
        tail = spread[heads * comps :]
        first_freq = jnp.sum(
            jnp.where(row_iota(tail.shape[0]) == head, tail, 0.0), axis=0, keepdims=True
        )
        shift = jnp.zeros((clusters, LANES), jnp.int32)
        for which in range(3):
            p = points[which]
            coords = (
                lax.shift_right_logical(p, 2 * log),
                lax.shift_right_logical(p, log) & (QMESH - 1),
                p & (QMESH - 1),
            )
            for axis in range(3):
                shift = shift + cells[3 * which + axis] * coords[axis]
        angle = (shift & (QMESH - 1)).astype(jnp.float32) * (2.0 * math.pi / QMESH)
        cosine, sine = jnp.cos(angle), jnp.sin(angle)
        third_re, third_im = held_rows(third, branches), held_rows(third[branches:], branches)
        fourth_re, fourth_im = cycled_rows(fourth, branches), cycled_rows(fourth[branches:], branches)
        period = len(fourth_re)
        far = []
        for v in range(pairs // SUB):
            are, aim, bre, bim = third_re[v], third_im[v], fourth_re[v % period], fourth_im[v % period]
            far.append((are * bre - aim * bim, -(are * bim + aim * bre)))
        for k in range(clusters):
            cos_k, sin_k = cosine[k : k + 1], sine[k : k + 1]
            for v in range(0, pairs // SUB, 2):
                both = [(cos_k * re - sin_k * im, cos_k * im + sin_k * re) for re, im in far[v : v + 2]]
                at = k * pairs + v * SUB
                for part in range(2):
                    wide[at : at + 2 * SUB, part * LANES : (part + 1) * LANES] = jnp.concatenate(
                        [both[0][part], both[1][part]], axis=0
                    ).astype(jnp.bfloat16)
        weighted = jnp.dot(phi[...], wide[...], preferred_element_type=jnp.float32)
        first_re, first_im = held_rows(first, branches), held_rows(first[branches:], branches)
        second_re, second_im = cycled_rows(second, branches), cycled_rows(second[branches:], branches)
        sum_re = jnp.zeros((SUB, LANES), jnp.float32)
        sum_im = sum_re
        for v in range(pairs // SUB):
            are, aim, bre, bim = first_re[v], first_im[v], second_re[v % period], second_im[v % period]
            near_re, near_im = are * bre - aim * bim, are * bim + aim * bre
            wre = weighted[v * SUB : (v + 1) * SUB, :LANES]
            wim = weighted[v * SUB : (v + 1) * SUB, LANES:]
            sum_re = sum_re + (near_re * wre - near_im * wim)
            sum_im = sum_im + (near_re * wim + near_im * wre)
        value_re = jnp.sum(sum_re, axis=0, keepdims=True)
        value_im = jnp.sum(sum_im, axis=0, keepdims=True)
        f2, f3, f4 = (e[comps : comps + 1] for e in others)
        mismatch = first_freq + f2 - f3 - f4
        delta = jnp.exp(-((mismatch / smearing) ** 2)) / (smearing * math.sqrt(math.pi))
        weight = (
            (1.0 + occupation(f2)) * occupation(f3) * occupation(f4) / occupation(first_freq)
        )
        product = first_freq * f2 * f3 * f4
        term = (value_re * value_re + value_im * value_im) * delta * weight / product
        term = jnp.where(local >= 0, term, 0.0)
        size = acc.shape[0]
        placed = jnp.where(row_iota(size) == head, term, 0.0)
        parts = []
        for _ in range(3):
            part = placed.astype(jnp.bfloat16)
            parts.append(part)
            placed = placed - part.astype(jnp.float32)
        sums = lax.dot_general(
            jnp.concatenate(parts, axis=0),
            hot,
            (((1,), (1,)), ((), ())),
            preferred_element_type=jnp.float32,
        )
        acc[...] += sums[:size] + sums[size : 2 * size] + sums[2 * size :]

    load(0, spots_a, 0).wait()
    gather(spots_a, near_a)

    def half_step(i, here, there, spots_here, spots_there, which_here, which_there):
        load(i + 2, spots_here, which_here).start()
        load(i + 1, spots_there, which_there).wait()
        gather(spots_there, there)
        contract(i, here)

    def two_blocks(j, carry):
        i = 2 * j
        half_step(i, near_a, near_b, spots_a, spots_b, 0, 1)

        @pl.when(i + 1 < count)
        def _():
            half_step(i + 1, near_b, near_a, spots_b, spots_a, 1, 0)

        return carry

    lax.fori_loop(0, lax.div(count + 1, 2), two_blocks, 0)
    even = lax.rem(count, 2) == 0

    @pl.when(even)
    def _():
        load(0, spots_b, 1).wait()

    @pl.when(jnp.logical_not(even))
    def _():
        load(0, spots_a, 0).wait()

    out[...] = acc[:heads, :]


def body(quartets, counts, eig, freq, phi, cells):
    comps, local = eig.shape
    branches = comps // 2
    shards = lax.axis_size("pb")
    workers = lax.axis_size("wa")
    held, parts, block = quartets.shape
    kept = local // workers
    heads = window(kept)
    clusters = cells.shape[0]
    offset = local * shards // 2
    both = ("pb", "wa")
    lines = freq.reshape(local // LANES, LANES)

    def swap(x):
        return lax.ppermute(x, "wa", [(i, i ^ 1) for i in range(workers)])

    def across(x, even, odd):
        pairs = []
        for p in range(shards):
            for w in range(workers):
                pairs.append((p * workers + w, (p ^ (odd if w % 2 else even)) * workers + w))
        return lax.ppermute(x, both, pairs)

    if shards == GROUPS:
        vectors, rows_of = [eig], [lines]
        for owned, kind in ((eig, vectors), (lines, rows_of)):
            one = across(owned, 1, 2)
            far = across(one, 2, 1)
            kind += [one, swap(one), far]
    else:
        vectors, rows_of = [eig], [lines]
        for k in range(1, shards):
            vectors.append(across(eig, k, k))
            rows_of.append(across(lines, k, k))

    slots = jnp.arange(held, dtype=jnp.int32)[:, None, None]
    coded = (jnp.where(slots < counts[0], quartets, -1) - offset).astype(jnp.int16)
    coded = coded.reshape(held * parts, block)
    line_up = [coded]
    for k in range(2, workers, 2):
        line_up.append(lax.ppermute(coded, "wa", [(i, i ^ k) for i in range(workers)]))
    column = jnp.concatenate(line_up, axis=0)
    total_rows = workers * held * parts
    rows, meta, flags = pl.pallas_call(
        functools.partial(prepare, branches, local, kept, offset),
        out_shape=[
            jax.ShapeDtypeStruct((total_rows, LANES), jnp.int32),
            jax.ShapeDtypeStruct((total_rows, LANES), jnp.int32),
            jax.ShapeDtypeStruct((SUB, total_rows), jnp.float32),
        ],
    )(column, swap(column))
    blocks = total_rows // parts
    index = jnp.arange(blocks, dtype=jnp.int32)
    owned = flags[0].reshape(blocks, parts)[:, 0] > 0.5
    place = jnp.cumsum(owned.astype(jnp.int32)) - 1
    order = jnp.sum(
        jnp.where((place[None, :] == index[:, None]) & owned[None, :], index[None, :], 0), axis=1
    )
    total = jnp.sum(owned.astype(jnp.int32)).reshape(1)
    signed = jnp.concatenate([cells[:, :3], -cells[:, 3:]], axis=1)
    spread_cells = jnp.broadcast_to(signed.T[:, :, None], (9, clusters, LANES))

    vmem = pl.BlockSpec(memory_space=pltpu.VMEM)
    smem = pl.BlockSpec(memory_space=pltpu.SMEM)
    padded = -(-heads // 16) * 16
    own_rows = -(-heads * (comps + 1) // 16) * 16
    rates = pl.pallas_call(
        functools.partial(kernel, branches, kept, shards),
        out_shape=jax.ShapeDtypeStruct((heads, LANES), jnp.float32),
        in_specs=[smem, smem, pl.BlockSpec(memory_space=pl.ANY)] + [vmem] * (3 + 2 * shards),
        out_specs=vmem,
        scratch_shapes=[
            pltpu.VMEM((shards // GROUPS * local, LANES), jnp.float32),
            pltpu.VMEM((3 * LANES, LANES), jnp.float32),
            pltpu.VMEM((3 * LANES, LANES), jnp.float32),
            pltpu.SMEM((parts, LANES), jnp.int32),
            pltpu.SMEM((parts, LANES), jnp.int32),
            pltpu.VMEM((phi.shape[1], 2 * LANES), jnp.bfloat16),
            pltpu.VMEM((own_rows, LANES), jnp.float32),
            pltpu.VMEM((padded, LANES), jnp.float32),
            pltpu.SemaphoreType.DMA((2,)),
        ],
        compiler_params=pltpu.CompilerParams(vmem_limit_bytes=32 * 1024 * 1024),
    )(
        order,
        total,
        rows.reshape(blocks, parts, LANES),
        meta.reshape(blocks, parts, LANES),
        phi,
        spread_cells,
        *vectors,
        *rows_of,
    )
    rates = rates.reshape(heads * LANES)
    if heads * LANES == kept:
        return rates
    return lax.dynamic_slice_in_dim(rates, lax.axis_index("wa") * kept % LANES, kept, 0)


def solution(mesh):
    placed = (P(("pb", "wa"), None, None), P(("pb", "wa")), P(None, "pb"), P("pb"), P(), P())
    return jax.shard_map(
        body, mesh=mesh, in_specs=placed, out_specs=P(("pb", "wa")), check_vma=False
    )
```

```python
import functools
import math

import jax
import jax.numpy as jnp
from jax import lax
from jax.experimental import pallas as pl
from jax.experimental.pallas import tpu as pltpu
from jax.sharding import PartitionSpec as P


QMESH = 16
LANES = 128
SUB = 8
GROUPS = 4
SLOT = LANES // GROUPS
PARTS = 4

smearing = 0.5


def occupation(value):
    return 1.0 / (jnp.exp(value) - 1.0)


def row_iota(rows):
    return lax.broadcasted_iota(jnp.int32, (rows, LANES), 0)


def window(kept):
    return -(-(kept + LANES - math.gcd(kept, LANES)) // LANES)


def prepare(branches, local, kept, offset, *refs):
    pool, (rows_out, meta_out, flags_out) = refs[:-3], refs[-3:]
    mine = lax.axis_index("pb")
    side = lax.rem(lax.axis_index("wa"), 2)
    start = lax.axis_index("wa") * kept
    lead = lax.rem(start, LANES)
    shards = lax.axis_size("pb")
    modes = jnp.concatenate([r[...].astype(jnp.int32) for r in pool], axis=0) + offset
    count = modes.shape[0]
    heading = (row_iota(count) & (PARTS - 1)) == 0
    safe = jnp.maximum(modes, 0)
    middle = safe.astype(jnp.float32) + 0.5
    owner = (middle * (1.0 / local)).astype(jnp.int32)
    point = (middle * (1.0 / branches)).astype(jnp.int32)
    near = owner ^ mine
    slot = near
    if shards == GROUPS:
        slot = jnp.where(near == 1, 1 + side, jnp.where(near == 2, 2 - side, near))
    inner = safe - owner * local
    depth = local // GROUPS
    group = ((inner.astype(jnp.float32) + 0.5) * (1.0 / depth)).astype(jnp.int32)
    rows_out[...] = (slot - group) * depth + inner
    following = pltpu.roll(modes, count - 1, 0)
    first = modes - start
    valid = heading & (following >= 0) & (first >= 0) & (first < kept)
    meta_out[...] = jnp.where(
        heading, jnp.where(valid, first + lead, -1), point + group * 65536
    )
    flags_out[...] = lax.dot_general(
        jnp.ones((SUB, LANES), jnp.bfloat16),
        jnp.where(valid, 1.0, 0.0).astype(jnp.bfloat16),
        (((1,), (1,)), ((), ())),
        preferred_element_type=jnp.float32,
    )


def fill_table(vectors, lines, table, base):
    comps, local = vectors.shape
    depth = local // GROUPS
    for t in range(depth // LANES):
        stack = []
        for g in range(GROUPS):
            at = g * depth + t * LANES
            stack.append(vectors[:, at : at + LANES].astype(jnp.float32))
            line = lines[at // LANES : at // LANES + 1, :].astype(jnp.float32)
            stack.append(jnp.broadcast_to(line, (SLOT - comps, LANES)))
        row = base + t * LANES
        table[row : row + LANES, :] = jnp.concatenate(stack, axis=0).T


def early(kept, heads, near, *refs):
    vectors, lines = refs[:near], refs[near : 2 * near]
    table, own = refs[2 * near :]
    comps, local = vectors[0].shape
    for at in range(near):
        fill_table(vectors[at], lines[at], table, at * (local // GROUPS))
    start = lax.axis_index("wa") * kept // LANES
    own_lines = lines[0][...].astype(jnp.float32)
    line_rows = row_iota(own_lines.shape[0])
    parts = []
    for h in range(heads):
        at = pl.multiple_of((start + h) * LANES, LANES)
        parts.append(vectors[0][:, pl.ds(at, LANES)].astype(jnp.float32))
    for h in range(heads):
        parts.append(
            jnp.sum(jnp.where(line_rows == start + h, own_lines, 0.0), axis=0, keepdims=True)
        )
    filler = own.shape[0] - heads * comps - heads
    parts.append(jnp.zeros((filler, LANES), jnp.float32))
    own[...] = jnp.concatenate(parts, axis=0).astype(jnp.bfloat16)


def held_rows(e, branches):
    out = []
    for v in range(branches * branches // SUB):
        low, high = v * SUB // branches, (v * SUB + SUB - 1) // branches
        if low == high:
            out.append(jnp.broadcast_to(e[low : low + 1], (SUB, LANES)))
        else:
            cut = high * branches - v * SUB
            out.append(jnp.where(row_iota(SUB) < cut, e[low : low + 1], e[high : high + 1]))
    return out


def cycled_rows(e, branches):
    period = math.lcm(SUB, branches)
    twice = jnp.concatenate([e[:branches]] * (period // branches), axis=0)
    return [twice[v * SUB : (v + 1) * SUB] for v in range(period // SUB)]


def kernel(
    branches,
    base,
    order,
    total,
    rows_any,
    meta,
    table_in,
    own,
    phi_hbm,
    cells,
    vectors,
    lines,
    out,
    table,
    near_a,
    near_b,
    spots_a,
    spots_b,
    phi,
    wide,
    acc,
    sems,
):
    comps = 2 * branches
    pairs = branches * branches
    clusters = SUB
    heads = out.shape[0]
    log = QMESH.bit_length() - 1
    count = total[0]
    last = rows_any.shape[0] - 1

    def block_at(i):
        return order[jnp.minimum(i, last)]

    def load(i, spots, which):
        return pltpu.make_async_copy(rows_any.at[block_at(i)], spots, sems.at[which])

    fetch_phi = pltpu.make_async_copy(phi_hbm, phi, sems.at[2])
    fetch_phi.start()
    load(0, spots_a, 0).start()
    load(1, spots_b, 1).start()
    fill_table(vectors, lines, table, base)
    acc[...] = jnp.zeros_like(acc)

    def gather(spots, near):
        for which in range(3):
            for n in range(LANES):
                at = which * LANES + n
                near[at : at + 1, :] = table[pl.ds(spots[which + 1, n], 1), :]

    def contract(info, near):
        others = []
        points = []
        for which in range(3):
            word = info[which + 1 : which + 2, :]
            group = lax.shift_right_logical(word, 16)
            points.append(word & 0xFFFF)
            flat = near[which * LANES : (which + 1) * LANES, :].T
            pick = flat[:SLOT]
            for g in range(1, GROUPS):
                pick = jnp.where(group == g, flat[g * SLOT : (g + 1) * SLOT], pick)
            others.append(pick)
        second, third, fourth = others
        local = info[0:1, :]
        head = lax.shift_right_arithmetic(local, 7)
        hot = jnp.where(row_iota(LANES) == (local & (LANES - 1)), 1.0, 0.0).astype(jnp.bfloat16)
        spread = jnp.dot(own[...], hot, preferred_element_type=jnp.float32)
        first = jnp.zeros((comps, LANES), jnp.float32)
        for h in range(heads):
            first = jnp.where(head == h, spread[h * comps : (h + 1) * comps], first)
        tail = spread[heads * comps :]
        first_freq = jnp.sum(
            jnp.where(row_iota(tail.shape[0]) == head, tail, 0.0), axis=0, keepdims=True
        )
        shift = jnp.zeros((clusters, LANES), jnp.int32)
        for which in range(3):
            p = points[which]
            coords = (
                lax.shift_right_logical(p, 2 * log),
                lax.shift_right_logical(p, log) & (QMESH - 1),
                p & (QMESH - 1),
            )
            for axis in range(3):
                shift = shift + cells[3 * which + axis] * coords[axis]
        angle = (shift & (QMESH - 1)).astype(jnp.float32) * (2.0 * math.pi / QMESH)
        cosine, sine = jnp.cos(angle), jnp.sin(angle)
        third_re, third_im = held_rows(third, branches), held_rows(third[branches:], branches)
        fourth_re, fourth_im = cycled_rows(fourth, branches), cycled_rows(fourth[branches:], branches)
        period = len(fourth_re)
        far = []
        for v in range(pairs // SUB):
            are, aim, bre, bim = third_re[v], third_im[v], fourth_re[v % period], fourth_im[v % period]
            far.append((are * bre - aim * bim, -(are * bim + aim * bre)))
        for k in range(clusters):
            cos_k, sin_k = cosine[k : k + 1], sine[k : k + 1]
            for v in range(0, pairs // SUB, 2):
                both = [(cos_k * re - sin_k * im, cos_k * im + sin_k * re) for re, im in far[v : v + 2]]
                at = k * pairs + v * SUB
                for part in range(2):
                    wide[at : at + 2 * SUB, part * LANES : (part + 1) * LANES] = jnp.concatenate(
                        [both[0][part], both[1][part]], axis=0
                    ).astype(jnp.bfloat16)
        weighted = jnp.dot(phi[...], wide[...], preferred_element_type=jnp.float32)
        first_re, first_im = held_rows(first, branches), held_rows(first[branches:], branches)
        second_re, second_im = cycled_rows(second, branches), cycled_rows(second[branches:], branches)
        sum_re = jnp.zeros((SUB, LANES), jnp.float32)
        sum_im = sum_re
        for v in range(pairs // SUB):
            are, aim, bre, bim = first_re[v], first_im[v], second_re[v % period], second_im[v % period]
            near_re, near_im = are * bre - aim * bim, are * bim + aim * bre
            wre = weighted[v * SUB : (v + 1) * SUB, :LANES]
            wim = weighted[v * SUB : (v + 1) * SUB, LANES:]
            sum_re = sum_re + (near_re * wre - near_im * wim)
            sum_im = sum_im + (near_re * wim + near_im * wre)
        value_re = jnp.sum(sum_re, axis=0, keepdims=True)
        value_im = jnp.sum(sum_im, axis=0, keepdims=True)
        f2, f3, f4 = (e[comps : comps + 1] for e in others)
        mismatch = first_freq + f2 - f3 - f4
        delta = jnp.exp(-((mismatch / smearing) ** 2)) / (smearing * math.sqrt(math.pi))
        weight = (
            (1.0 + occupation(f2)) * occupation(f3) * occupation(f4) / occupation(first_freq)
        )
        product = first_freq * f2 * f3 * f4
        term = (value_re * value_re + value_im * value_im) * delta * weight / product
        term = jnp.where(local >= 0, term, 0.0)
        size = acc.shape[0]
        placed = jnp.where(row_iota(size) == head, term, 0.0)
        parts = []
        for _ in range(3):
            part = placed.astype(jnp.bfloat16)
            parts.append(part)
            placed = placed - part.astype(jnp.float32)
        sums = lax.dot_general(
            jnp.concatenate(parts, axis=0),
            hot,
            (((1,), (1,)), ((), ())),
            preferred_element_type=jnp.float32,
        )
        acc[...] += sums[:size] + sums[size : 2 * size] + sums[2 * size :]

    load(0, spots_a, 0).wait()
    gather(spots_a, near_a)
    fetch_phi.wait()
    side_a, side_b = (near_a, spots_a, 0), (near_b, spots_b, 1)

    def half_step(i, here, there):
        load(i + 2, *here[1:]).start()
        load(i + 1, *there[1:]).wait()
        gather(there[1], there[0])
        contract(meta[block_at(i)], here[0])

    def two_blocks(j, carry):
        half_step(2 * j, side_a, side_b)

        @pl.when(2 * j + 1 < count)
        def _():
            half_step(2 * j + 1, side_b, side_a)

        return carry

    lax.fori_loop(0, lax.div(count + 1, 2), two_blocks, 0)
    even = lax.rem(count, 2) == 0

    @pl.when(even)
    def _():
        load(0, *side_b[1:]).wait()

    @pl.when(jnp.logical_not(even))
    def _():
        load(0, *side_a[1:]).wait()

    out[...] = acc[:heads, :]


def body(quartets, counts, eig, freq, phi, cells):
    comps, local = eig.shape
    branches = comps // 2
    shards = lax.axis_size("pb")
    workers = lax.axis_size("wa")
    held, parts, block = quartets.shape
    kept = local // workers
    heads = window(kept)
    clusters = cells.shape[0]
    offset = local * shards // 2
    both = ("pb", "wa")
    lines = freq.reshape(local // LANES, LANES)

    def swap(x):
        return lax.ppermute(x, "wa", [(i, i ^ 1) for i in range(workers)])

    def across(x, even, odd):
        pairs = []
        for p in range(shards):
            for w in range(workers):
                pairs.append((p * workers + w, (p ^ (odd if w % 2 else even)) * workers + w))
        return lax.ppermute(x, both, pairs)

    if shards == GROUPS:
        vectors, rows_of = [eig], [lines]
        for owned, kind in ((eig, vectors), (lines, rows_of)):
            one = across(owned, 1, 2)
            far = across(one, 2, 1)
            kind += [one, swap(one), far]
    else:
        vectors, rows_of = [eig], [lines]
        for k in range(1, shards):
            vectors.append(across(eig, k, k))
            rows_of.append(across(lines, k, k))

    slots = jnp.arange(held, dtype=jnp.int32)[:, None, None]
    coded = (jnp.where(slots < counts[0], quartets, -1) - offset).astype(jnp.int16)
    coded = coded.reshape(held * parts, block)
    line_up = [coded]
    for k in range(2, workers, 2):
        line_up.append(lax.ppermute(coded, "wa", [(i, i ^ k) for i in range(workers)]))
    column = jnp.concatenate(line_up, axis=0)
    other_column = swap(column)
    vmem = pl.BlockSpec(memory_space=pltpu.VMEM)
    smem = pl.BlockSpec(memory_space=pltpu.SMEM)
    hbm = pl.BlockSpec(memory_space=pl.ANY)
    far_space = pl.BlockSpec(memory_space=pltpu.HBM)
    total_rows = workers * held * parts
    rows, meta, flags = pl.pallas_call(
        functools.partial(prepare, branches, local, kept, offset),
        out_shape=[
            jax.ShapeDtypeStruct((total_rows, LANES), jnp.int32),
            jax.ShapeDtypeStruct((total_rows, LANES), jnp.int32),
            jax.ShapeDtypeStruct((SUB, total_rows), jnp.float32),
        ],
        in_specs=[vmem, vmem],
        compiler_params=pltpu.CompilerParams(vmem_limit_bytes=16 * 1024 * 1024),
    )(column, other_column)
    blocks = total_rows // parts
    index = jnp.arange(blocks, dtype=jnp.int32)
    owned = flags[0].reshape(blocks, parts)[:, 0] > 0.5
    place = jnp.cumsum(owned.astype(jnp.int32)) - 1
    order = jnp.sum(
        jnp.where((place[None, :] == index[:, None]) & owned[None, :], index[None, :], 0), axis=1
    )
    total = jnp.sum(owned.astype(jnp.int32)).reshape(1)
    signed = jnp.concatenate([cells[:, :3], -cells[:, 3:]], axis=1)
    spread_cells = jnp.broadcast_to(signed.T[:, :, None], (9, clusters, LANES))

    padded = -(-heads // 16) * 16
    own_rows = -(-heads * (comps + 1) // 16) * 16
    depth = local // GROUPS
    near = shards - 1
    table, own = pl.pallas_call(
        functools.partial(early, kept, heads, near),
        out_shape=[
            jax.ShapeDtypeStruct((shards * depth, LANES), jnp.float32),
            jax.ShapeDtypeStruct((own_rows, LANES), jnp.bfloat16),
        ],
        in_specs=[vmem] * (2 * near),
        out_specs=[vmem, vmem],
        compiler_params=pltpu.CompilerParams(vmem_limit_bytes=16 * 1024 * 1024),
    )(*vectors[:near], *rows_of[:near])
    rates, _ = pl.pallas_call(
        functools.partial(kernel, branches, near * depth),
        out_shape=[
            jax.ShapeDtypeStruct((heads, LANES), jnp.float32),
            jax.ShapeDtypeStruct(table.shape, table.dtype),
        ],
        in_specs=[smem, smem, hbm, vmem, vmem, vmem, far_space] + [vmem] * 3,
        out_specs=[vmem, vmem],
        input_output_aliases={4: 1},
        scratch_shapes=[
            pltpu.VMEM((3 * LANES, LANES), jnp.float32),
            pltpu.VMEM((3 * LANES, LANES), jnp.float32),
            pltpu.SMEM((parts, LANES), jnp.int32),
            pltpu.SMEM((parts, LANES), jnp.int32),
            pltpu.VMEM(phi.shape, phi.dtype),
            pltpu.VMEM((phi.shape[1], 2 * LANES), jnp.bfloat16),
            pltpu.VMEM((padded, LANES), jnp.float32),
            pltpu.SemaphoreType.DMA((3,)),
        ],
        compiler_params=pltpu.CompilerParams(vmem_limit_bytes=16 * 1024 * 1024),
    )(
        order,
        total,
        rows.reshape(blocks, parts, LANES),
        meta.reshape(blocks, parts, LANES),
        table,
        own,
        phi,
        spread_cells,
        vectors[near],
        rows_of[near],
    )
    rates = rates.reshape(heads * LANES)
    if heads * LANES == kept:
        return rates
    return lax.dynamic_slice_in_dim(rates, lax.axis_index("wa") * kept % LANES, kept, 0)


def solution(mesh):
    placed = (P(("pb", "wa"), None, None), P(("pb", "wa")), P(None, "pb"), P("pb"), P(), P())
    return jax.shard_map(
        body, mesh=mesh, in_specs=placed, out_specs=P(("pb", "wa")), check_vma=False
    )
```

```python
import functools
import math

import jax
import jax.numpy as jnp
from jax import lax
from jax.experimental import pallas as pl
from jax.experimental.pallas import tpu as pltpu
from jax.sharding import PartitionSpec as P


QMESH = 16
LANES = 128
SUB = 8
GROUPS = 4
SLOT = LANES // GROUPS
PARTS = 4
AHEAD = 2
DEPTH = 256

smearing = 0.5


def occupation(value):
    return 1.0 / (jnp.exp(value) - 1.0)


def row_iota(rows):
    return lax.broadcasted_iota(jnp.int32, (rows, LANES), 0)


def window(kept):
    return -(-(kept + LANES - math.gcd(kept, LANES)) // LANES)


def prepare(branches, local, kept, offset, *refs):
    pool, (rows_out, meta_out, flags_out) = refs[:-3], refs[-3:]
    mine = lax.axis_index("pb")
    side = lax.rem(lax.axis_index("wa"), 2)
    start = lax.axis_index("wa") * kept
    lead = lax.rem(start, LANES)
    shards = lax.axis_size("pb")
    modes = jnp.concatenate([r[...].astype(jnp.int32) for r in pool], axis=0) + offset
    count = modes.shape[0]
    heading = (row_iota(count) & (PARTS - 1)) == 0
    safe = jnp.maximum(modes, 0)
    middle = safe.astype(jnp.float32) + 0.5
    owner = (middle * (1.0 / local)).astype(jnp.int32)
    point = (middle * (1.0 / branches)).astype(jnp.int32)
    near = owner ^ mine
    slot = near
    if shards == GROUPS:
        slot = jnp.where(near == 1, 1 + side, jnp.where(near == 2, 2 - side, near))
    inner = safe - owner * local
    depth = local // GROUPS
    group = ((inner.astype(jnp.float32) + 0.5) * (1.0 / depth)).astype(jnp.int32)
    rows_out[...] = (slot - group) * depth + inner
    following = pltpu.roll(modes, count - 1, 0)
    first = modes - start
    valid = heading & (following >= 0) & (first >= 0) & (first < kept)
    meta_out[...] = jnp.where(
        heading, jnp.where(valid, first + lead, -1), point + group * 65536
    )
    flags_out[...] = lax.dot_general(
        jnp.ones((SUB, LANES), jnp.bfloat16),
        jnp.where(valid, 1.0, 0.0).astype(jnp.bfloat16),
        (((1,), (1,)), ((), ())),
        preferred_element_type=jnp.float32,
    )


def fill_table(vectors, lines, table, base):
    comps, local = vectors.shape
    depth = local // GROUPS
    for t in range(depth // LANES):
        stack = []
        for g in range(GROUPS):
            at = g * depth + t * LANES
            stack.append(vectors[:, at : at + LANES].astype(jnp.float32))
            line = lines[at // LANES : at // LANES + 1, :].astype(jnp.float32)
            stack.append(jnp.broadcast_to(line, (SLOT - comps, LANES)))
        row = base + t * LANES
        table[row : row + LANES, :] = jnp.concatenate(stack, axis=0).T


def early(kept, heads, near, *refs):
    vectors, lines = refs[:near], refs[near : 2 * near]
    phi_in, table, own, phi = refs[2 * near :]
    phi[...] = phi_in[...]
    comps, local = vectors[0].shape
    for at in range(near):
        fill_table(vectors[at], lines[at], table, at * (local // GROUPS))
    start = lax.axis_index("wa") * kept // LANES
    own_lines = lines[0][...].astype(jnp.float32)
    line_rows = row_iota(own_lines.shape[0])
    parts = []
    for h in range(heads):
        at = pl.multiple_of((start + h) * LANES, LANES)
        parts.append(vectors[0][:, pl.ds(at, LANES)].astype(jnp.float32))
    for h in range(heads):
        parts.append(
            jnp.sum(jnp.where(line_rows == start + h, own_lines, 0.0), axis=0, keepdims=True)
        )
    filler = own.shape[0] - heads * comps - heads
    parts.append(jnp.zeros((filler, LANES), jnp.float32))
    own[...] = jnp.concatenate(parts, axis=0).astype(jnp.bfloat16)


def held_rows(e, branches):
    out = []
    for v in range(branches * branches // SUB):
        low, high = v * SUB // branches, (v * SUB + SUB - 1) // branches
        if low == high:
            out.append(jnp.broadcast_to(e[low : low + 1], (SUB, LANES)))
        else:
            cut = high * branches - v * SUB
            out.append(jnp.where(row_iota(SUB) < cut, e[low : low + 1], e[high : high + 1]))
    return out


def cycled_rows(e, branches):
    period = math.lcm(SUB, branches)
    twice = jnp.concatenate([e[:branches]] * (period // branches), axis=0)
    return [twice[v * SUB : (v + 1) * SUB] for v in range(period // SUB)]


def kernel(
    branches,
    base,
    order,
    total,
    rows_any,
    meta,
    table_in,
    own,
    phi,
    cells,
    vectors,
    lines,
    out,
    table,
    gathered_a,
    gathered_b,
    pair_a,
    pair_b,
    single_a,
    single_b,
    wide_a,
    wide_b,
    product_a,
    product_b,
    placed,
    place,
    acc,
    spots,
    sems,
):
    comps = 2 * branches
    pairs = branches * branches
    groups = pairs // SUB
    clusters = SUB
    heads = out.shape[0]
    log = QMESH.bit_length() - 1
    count = total[0]
    last = rows_any.shape[0] - 1
    gathered, pair, single = (gathered_a, gathered_b), (pair_a, pair_b), (single_a, single_b)
    wide, product = (wide_a, wide_b), (product_a, product_b)

    def block_at(i):
        return order[jnp.clip(i, 0, last)]

    def load(i, p):
        return pltpu.make_async_copy(rows_any.at[block_at(i)], spots.at[p], sems.at[p])

    def gather(p):
        into = gathered[p]
        for which in range(3):
            for n in range(LANES):
                at = which * LANES + n
                into[at : at + 1, :] = table[pl.ds(spots[p, which + 1, n], 1), :]
                yield

    def one_hot(local):
        inside = local & (LANES - 1)
        return jnp.where(row_iota(LANES) == inside, 1.0, 0.0).astype(jnp.bfloat16)

    def choose(i, rows, pair_out, single_out):
        info = meta[block_at(i)]
        local = jnp.where(i < count, info[0:1, :], -1)
        head = lax.shift_right_arithmetic(local, 7)
        spread = jnp.dot(own[...], one_hot(local), preferred_element_type=jnp.float32)
        flats = [rows[w * LANES : (w + 1) * LANES, :].T for w in range(3)]
        yield
        shift = jnp.zeros((clusters, LANES), jnp.int32)
        for which in range(3):
            p = info[which + 1 : which + 2, :] & 0xFFFF
            coords = (
                lax.shift_right_logical(p, 2 * log),
                lax.shift_right_logical(p, log) & (QMESH - 1),
                p & (QMESH - 1),
            )
            for axis in range(3):
                shift = shift + cells[3 * which + axis] * coords[axis]
            yield
        angle = (shift & (QMESH - 1)).astype(jnp.float32) * (2.0 * math.pi / QMESH)
        single_out[0:SUB, :] = jnp.cos(angle)
        yield
        single_out[SUB : 2 * SUB, :] = jnp.sin(angle)
        yield
        others = []
        for which in range(3):
            group = lax.shift_right_logical(info[which + 1 : which + 2, :], 16)
            masks = [group == g for g in range(1, GROUPS)]
            pick = []
            for r in range(0, SLOT, SUB):
                value = flats[which][r : r + SUB]
                for g in range(1, GROUPS):
                    at = g * SLOT + r
                    value = jnp.where(masks[g - 1], flats[which][at : at + SUB], value)
                pick.append(value)
                yield
            others.append(jnp.concatenate(pick, axis=0))
        second, third, fourth = others
        third_re, third_im = held_rows(third, branches), held_rows(third[branches:], branches)
        fourth_re, fourth_im = cycled_rows(fourth, branches), cycled_rows(fourth[branches:], branches)
        period = len(fourth_re)
        for v in range(groups):
            are, aim, bre, bim = third_re[v], third_im[v], fourth_re[v % period], fourth_im[v % period]
            pair_out[v * SUB : (v + 1) * SUB, :] = are * bre - aim * bim
            at = pairs + v * SUB
            pair_out[at : at + SUB, :] = -(are * bim + aim * bre)
            yield
        at = 2 * SUB
        single_out[at : at + SLOT, :] = second
        first = jnp.zeros((comps, LANES), jnp.float32)
        for h in range(heads):
            first = jnp.where(head == h, spread[h * comps : (h + 1) * comps], first)
            yield
        tail = spread[heads * comps :]
        first_freq = jnp.sum(
            jnp.where(row_iota(tail.shape[0]) == head, tail, 0.0), axis=0, keepdims=True
        )
        at += SLOT
        single_out[at : at + comps, :] = first
        at += comps
        wanted = [first_freq] + [e[comps : comps + 1] for e in others]
        wanted.append(local.astype(jnp.float32))
        for n, line in enumerate(wanted):
            single_out[at + n : at + n + 1, :] = line
        yield

    def join(single_in, product_out):
        at = 2 * SUB
        second = single_in[at : at + comps, :]
        at += SLOT
        first = single_in[at : at + comps, :]
        at += comps
        f1, f2, f3, f4, local = (single_in[at + n : at + n + 1, :] for n in range(5))
        yield
        mismatch = f1 + f2 - f3 - f4
        delta = jnp.exp(-((mismatch / smearing) ** 2)) / (smearing * math.sqrt(math.pi))
        yield
        weight = (1.0 + occupation(f2)) * occupation(f3) * occupation(f4) / occupation(f1)
        yield
        at = 2 * pairs
        product_out[at : at + 1, :] = delta * weight / (f1 * f2 * f3 * f4)
        product_out[at + 1 : at + 2, :] = local
        yield
        first_re, first_im = held_rows(first, branches), held_rows(first[branches:], branches)
        second_re, second_im = cycled_rows(second, branches), cycled_rows(second[branches:], branches)
        period = len(second_re)
        for v in range(groups):
            are, aim, bre, bim = first_re[v], first_im[v], second_re[v % period], second_im[v % period]
            product_out[v * SUB : (v + 1) * SUB, :] = are * bre - aim * bim
            at = pairs + v * SUB
            product_out[at : at + SUB, :] = are * bim + aim * bre
            yield

    def turn(pair_in, single_in, wide_out):
        for k in range(clusters):
            cos_k, sin_k = single_in[k : k + 1, :], single_in[SUB + k : SUB + k + 1, :]
            for v in range(0, groups, 2):
                both = []
                for u in (v, v + 1):
                    re = pair_in[u * SUB : (u + 1) * SUB, :]
                    im = pair_in[pairs + u * SUB : pairs + (u + 1) * SUB, :]
                    both.append((cos_k * re - sin_k * im, cos_k * im + sin_k * re))
                at = k * pairs + v * SUB
                for part in range(2):
                    wide_out[at : at + 2 * SUB, part * LANES : (part + 1) * LANES] = jnp.concatenate(
                        [both[0][part], both[1][part]], axis=0
                    ).astype(jnp.bfloat16)
                yield

    def finish(i, weighted, product_in):
        sum_re = jnp.zeros((SUB, LANES), jnp.float32)
        sum_im = sum_re
        for v in range(groups):
            rows = slice(v * SUB, (v + 1) * SUB)
            nre = product_in[rows, :]
            nim = product_in[pairs + v * SUB : pairs + (v + 1) * SUB, :]
            wre, wim = weighted[rows, :LANES], weighted[rows, LANES:]
            sum_re = sum_re + (nre * wre - nim * wim)
            sum_im = sum_im + (nre * wim + nim * wre)
            yield
        value_re = jnp.sum(sum_re, axis=0, keepdims=True)
        value_im = jnp.sum(sum_im, axis=0, keepdims=True)
        yield
        at = 2 * pairs
        factor = product_in[at : at + 1, :]
        local = product_in[at + 1 : at + 2, :].astype(jnp.int32)
        local = jnp.where(i >= 0, local, -1)
        term = (value_re * value_re + value_im * value_im) * factor
        size = acc.shape[0]
        rest = jnp.where(row_iota(size) == lax.shift_right_arithmetic(local, 7), term, 0.0)
        place[0:1, :] = local
        yield
        for n in range(3):
            part = rest.astype(jnp.bfloat16)
            placed[n * size : (n + 1) * size, :] = part
            rest = rest - part.astype(jnp.float32)
        yield

    def run(*tracks):
        total_steps = max(n for _, n in tracks)
        done = [0] * len(tracks)
        for step in range(1, total_steps + 1):
            for t, (track, n) in enumerate(tracks):
                while done[t] * total_steps < step * n:
                    next(track, None)
                    done[t] += 1
        for track, _ in tracks:
            for _ in track:
                pass

    gather_steps = 3 * LANES
    choose_steps = 20 + groups + heads
    join_steps = 4 + groups
    turn_steps = clusters * groups // 2
    finish_steps = groups + 3

    pieces = [(at, min(at + DEPTH, clusters * pairs)) for at in range(0, clusters * pairs, DEPTH)]

    def multiply(wide_in, held):
        for low, high in pieces:
            part = jnp.dot(phi[:, low:high], wide_in[low:high, :], preferred_element_type=jnp.float32)
            held[:] = [part if not held else held[0] + part]
            yield

    def step(i, p):
        load(i + 3, 1 - p).start()
        load(i + 2, p).wait()
        sums = lax.dot_general(
            placed[...],
            one_hot(place[0:1, :]),
            (((1,), (1,)), ((), ())),
            preferred_element_type=jnp.float32,
        )
        weighted = []
        run(
            (choose(i + 1, gathered[1 - p], pair[1 - p], single[1 - p]), choose_steps),
            (multiply(wide[1 - p], weighted), len(pieces)),
            (turn(pair[p], single[p], wide[p]), turn_steps),
            (join(single[p], product[p]), join_steps),
            (gather(p), gather_steps),
        )
        run((finish(i - 1, weighted[0], product[1 - p]), finish_steps))
        size = acc.shape[0]
        acc[...] += sums[:size] + sums[size : 2 * size] + sums[2 * size :]

    load(0, 0).start()
    load(1, 1).start()
    acc[...] = jnp.zeros_like(acc)
    placed[...] = jnp.zeros_like(placed)
    place[...] = jnp.zeros_like(place)
    fill_table(vectors, lines, table, base)
    load(0, 0).wait()
    run((gather(0), gather_steps))
    load(2, 0).start()
    load(1, 1).wait()
    run((choose(0, gathered_a, pair_a, single_a), choose_steps), (gather(1), gather_steps))

    def two_steps(j, carry):
        step(2 * j, 0)

        @pl.when(2 * j + 1 < count + 2)
        def _():
            step(2 * j + 1, 1)

        return carry

    lax.fori_loop(0, lax.div(count + 3, 2), two_steps, 0)
    even = lax.rem(count, 2) == 0

    @pl.when(even)
    def _():
        load(0, 0).wait()

    @pl.when(jnp.logical_not(even))
    def _():
        load(0, 1).wait()

    out[...] = acc[:heads, :]


def rates_call(branches, base, heads, padded, *args):
    rows, table, phi = args[2], args[4], args[6]
    pairs = branches * branches
    singles = 2 * SUB + SLOT + 2 * branches + SUB
    vmem = pl.BlockSpec(memory_space=pltpu.VMEM)
    smem = pl.BlockSpec(memory_space=pltpu.SMEM)
    loose = pl.BlockSpec(memory_space=pl.ANY)
    rates, _ = pl.pallas_call(
        functools.partial(kernel, branches, base),
        out_shape=[
            jax.ShapeDtypeStruct((heads, LANES), jnp.float32),
            jax.ShapeDtypeStruct(table.shape, table.dtype),
        ],
        in_specs=[smem, smem, loose] + [vmem] * 7,
        out_specs=[vmem, vmem],
        input_output_aliases={4: 1},
        scratch_shapes=[
            *[pltpu.VMEM((3 * LANES, LANES), jnp.float32)] * 2,
            *[pltpu.VMEM((2 * pairs, LANES), jnp.float32)] * 2,
            *[pltpu.VMEM((singles, LANES), jnp.float32)] * 2,
            *[pltpu.VMEM((phi.shape[1], 2 * LANES), jnp.bfloat16)] * 2,
            *[pltpu.VMEM((2 * pairs + SUB, LANES), jnp.float32)] * 2,
            pltpu.VMEM((3 * padded, LANES), jnp.bfloat16),
            pltpu.VMEM((SUB, LANES), jnp.int32),
            pltpu.VMEM((padded, LANES), jnp.float32),
            pltpu.SMEM((AHEAD, *rows.shape[1:]), jnp.int32),
            pltpu.SemaphoreType.DMA((AHEAD,)),
        ],
        compiler_params=pltpu.CompilerParams(vmem_limit_bytes=16 * 1024 * 1024),
    )(*args)
    return rates


def body(quartets, counts, eig, freq, phi, cells):
    comps, local = eig.shape
    branches = comps // 2
    shards = lax.axis_size("pb")
    workers = lax.axis_size("wa")
    held, parts, block = quartets.shape
    kept = local // workers
    heads = window(kept)
    clusters = cells.shape[0]
    offset = local * shards // 2
    both = ("pb", "wa")
    lines = freq.reshape(local // LANES, LANES)

    def swap(x):
        return lax.ppermute(x, "wa", [(i, i ^ 1) for i in range(workers)])

    def across(x, even, odd):
        pairs = []
        for p in range(shards):
            for w in range(workers):
                pairs.append((p * workers + w, (p ^ (odd if w % 2 else even)) * workers + w))
        return lax.ppermute(x, both, pairs)

    if shards == GROUPS:
        vectors, rows_of = [eig], [lines]
        for owned, kind in ((eig, vectors), (lines, rows_of)):
            one = across(owned, 1, 2)
            far = across(one, 2, 1)
            kind += [one, swap(one), far]
    else:
        vectors, rows_of = [eig], [lines]
        for k in range(1, shards):
            vectors.append(across(eig, k, k))
            rows_of.append(across(lines, k, k))

    slots = jnp.arange(held, dtype=jnp.int32)[:, None, None]
    coded = (jnp.where(slots < counts[0], quartets, -1) - offset).astype(jnp.int16)
    coded = coded.reshape(held * parts, block)
    line_up = [coded]
    for k in range(2, workers, 2):
        line_up.append(lax.ppermute(coded, "wa", [(i, i ^ k) for i in range(workers)]))
    column = jnp.concatenate(line_up, axis=0)
    other_column = swap(column)
    vmem = pl.BlockSpec(memory_space=pltpu.VMEM)
    smem = pl.BlockSpec(memory_space=pltpu.SMEM)
    hbm = pl.BlockSpec(memory_space=pl.ANY)
    far_space = pl.BlockSpec(memory_space=pltpu.HBM)
    total_rows = workers * held * parts
    rows, meta, flags = pl.pallas_call(
        functools.partial(prepare, branches, local, kept, offset),
        out_shape=[
            jax.ShapeDtypeStruct((total_rows, LANES), jnp.int32),
            jax.ShapeDtypeStruct((total_rows, LANES), jnp.int32),
            jax.ShapeDtypeStruct((SUB, total_rows), jnp.float32),
        ],
        in_specs=[vmem, vmem],
        compiler_params=pltpu.CompilerParams(vmem_limit_bytes=16 * 1024 * 1024),
    )(column, other_column)
    blocks = total_rows // parts
    index = jnp.arange(blocks, dtype=jnp.int32)
    owned = flags[0].reshape(blocks, parts)[:, 0] > 0.5
    place = jnp.cumsum(owned.astype(jnp.int32)) - 1
    order = jnp.sum(
        jnp.where((place[None, :] == index[:, None]) & owned[None, :], index[None, :], 0), axis=1
    )
    total = jnp.sum(owned.astype(jnp.int32)).reshape(1)
    signed = jnp.concatenate([cells[:, :3], -cells[:, 3:]], axis=1)
    spread_cells = jnp.broadcast_to(signed.T[:, :, None], (9, clusters, LANES))

    padded = -(-heads // 16) * 16
    own_rows = -(-heads * (comps + 1) // 16) * 16
    depth = local // GROUPS
    near = shards - 1
    table, own, phi = pl.pallas_call(
        functools.partial(early, kept, heads, near),
        out_shape=[
            jax.ShapeDtypeStruct((shards * depth, LANES), jnp.float32),
            jax.ShapeDtypeStruct((own_rows, LANES), jnp.bfloat16),
            jax.ShapeDtypeStruct(phi.shape, phi.dtype),
        ],
        in_specs=[vmem] * (2 * near + 1),
        out_specs=[vmem] * 3,
        compiler_params=pltpu.CompilerParams(vmem_limit_bytes=16 * 1024 * 1024),
    )(*vectors[:near], *rows_of[:near], phi)
    rates = rates_call(
        branches,
        near * depth,
        heads,
        padded,
        order,
        total,
        rows.reshape(blocks, parts, LANES),
        meta.reshape(blocks, parts, LANES),
        table,
        own,
        phi,
        spread_cells,
        vectors[near],
        rows_of[near],
    )
    rates = rates.reshape(heads * LANES)
    if heads * LANES == kept:
        return rates
    return lax.dynamic_slice_in_dim(rates, lax.axis_index("wa") * kept % LANES, kept, 0)


def solution(mesh):
    placed = (P(("pb", "wa"), None, None), P(("pb", "wa")), P(None, "pb"), P("pb"), P(), P())
    return jax.shard_map(
        body, mesh=mesh, in_specs=placed, out_specs=P(("pb", "wa")), check_vma=False
    )
```

```python
import functools
import math

import jax
import jax.numpy as jnp
from jax import lax
from jax.experimental import pallas as pl
from jax.experimental.pallas import tpu as pltpu
from jax.sharding import PartitionSpec as P


QMESH = 16
LANES = 128
SUB = 8
GROUPS = 4
SLOT = LANES // GROUPS
PARTS = 4
AHEAD = 2
DEPTH = 256

smearing = 0.5


def occupation(value):
    return 1.0 / (jnp.exp(value) - 1.0)


def row_iota(rows):
    return lax.broadcasted_iota(jnp.int32, (rows, LANES), 0)


def window(kept):
    return -(-(kept + LANES - math.gcd(kept, LANES)) // LANES)


def prepare(branches, local, kept, offset, *refs):
    pool, (rows_out, meta_out, order_out) = refs[:-3], refs[-3:]
    mine = lax.axis_index("pb")
    side = lax.rem(lax.axis_index("wa"), 2)
    start = lax.axis_index("wa") * kept
    lead = lax.rem(start, LANES)
    shards = lax.axis_size("pb")
    modes = jnp.concatenate([r[...].astype(jnp.int32) for r in pool], axis=0) + offset
    count = modes.shape[0]
    heading = (row_iota(count) & (PARTS - 1)) == 0
    safe = jnp.maximum(modes, 0)
    middle = safe.astype(jnp.float32) + 0.5
    owner = (middle * (1.0 / local)).astype(jnp.int32)
    point = (middle * (1.0 / branches)).astype(jnp.int32)
    near = owner ^ mine
    slot = near
    if shards == GROUPS:
        slot = jnp.where(near == 1, 1 + side, jnp.where(near == 2, 2 - side, near))
    inner = safe - owner * local
    depth = local // GROUPS
    group = ((inner.astype(jnp.float32) + 0.5) * (1.0 / depth)).astype(jnp.int32)
    rows_out[...] = (slot - group) * depth + inner
    if shards == GROUPS:
        group = jnp.where(near == GROUPS - 1, group ^ (lax.axis_index("wa") & (GROUPS - 1)), group)
    following = pltpu.roll(modes, count - 1, 0)
    first = modes - start
    valid = heading & (following >= 0) & (first >= 0) & (first < kept)
    meta_out[...] = jnp.where(
        heading, jnp.where(valid, first + lead, -1), point + group * 65536
    )
    lanes = (((1,), (1,)), ((), ()))
    marks = lax.dot_general(
        jnp.ones((SUB, LANES), jnp.bfloat16),
        jnp.where(valid, 1.0, 0.0).astype(jnp.bfloat16),
        lanes,
        preferred_element_type=jnp.float32,
    )
    blocks = count // PARTS

    def index(rows, dim):
        return lax.broadcasted_iota(jnp.int32, (rows, blocks), dim)

    fold = jnp.where(index(count, 0) // PARTS == index(count, 1), 1.0, 0.0).astype(jnp.bfloat16)
    found = jnp.dot(marks.astype(jnp.bfloat16), fold, preferred_element_type=jnp.float32) > 0.5
    before = jnp.where(index(blocks, 0) <= index(blocks, 1), 1.0, 0.0).astype(jnp.bfloat16)
    rank = jnp.dot(
        jnp.where(found, 1.0, 0.0).astype(jnp.bfloat16), before, preferred_element_type=jnp.float32
    )
    spot = jnp.where(found, rank, 0.0)[0:1, :].astype(jnp.int32)
    chosen = jnp.where(index(blocks, 0) + 1 == spot, 1.0, 0.0).astype(jnp.bfloat16)
    number = index(SUB, 1)
    order = jnp.zeros((SUB, blocks), jnp.float32)
    for digit, scale in ((number & 15, 1.0), (number >> 4, 16.0)):
        order = order + scale * lax.dot_general(
            digit.astype(jnp.float32).astype(jnp.bfloat16),
            chosen,
            lanes,
            preferred_element_type=jnp.float32,
        )
    order_out[:, :blocks] = order[0:1, :].astype(jnp.int32)
    order_out[:, blocks:] = jnp.broadcast_to(rank[0:1, blocks - 1 :], (1, LANES)).astype(jnp.int32)


def shard_quarters(vectors, lines):
    depth = vectors.shape[1] // GROUPS

    def quarter(g):
        def chunk(t):
            at = g * depth + t * LANES
            row = at // LANES
            return vectors[:, at : at + LANES], lines[row : row + 1, :]

        return chunk

    return [quarter(g) for g in range(GROUPS)], depth


def piece_quarters(pieces, depth):
    def quarter(piece):
        def chunk(t):
            return piece[:, t * LANES : (t + 1) * LANES], piece[t : t + 1, depth : depth + LANES]

        return chunk

    return [quarter(piece) for piece in pieces], depth


def fill_table(source, table, base):
    quarters, depth = source
    for t in range(depth // LANES):
        stack = []
        for quarter in quarters:
            vectors, line = quarter(t)
            stack.append(vectors.astype(jnp.float32))
            filler = SLOT - vectors.shape[0]
            stack.append(jnp.broadcast_to(line.astype(jnp.float32), (filler, LANES)))
        row = base + t * LANES
        table[row : row + LANES, :] = jnp.concatenate(stack, axis=0).T


def begin(kept, heads, vectors, lines, phi_in, cells_in, table, own, phi, cells):
    comps = vectors.shape[0]
    phi[...] = phi_in[...]
    cell = cells_in[...]
    for j in range(cell.shape[1]):
        column = cell[:, j : j + 1]
        cells[j] = jnp.broadcast_to(column if j < 3 else -column, (cell.shape[0], LANES))
    fill_table(shard_quarters(vectors, lines), table, 0)
    start = lax.axis_index("wa") * kept // LANES
    own_lines = lines[...].astype(jnp.float32)
    line_rows = row_iota(own_lines.shape[0])
    parts = []
    for h in range(heads):
        at = pl.multiple_of((start + h) * LANES, LANES)
        parts.append(vectors[:, pl.ds(at, LANES)].astype(jnp.float32))
    for h in range(heads):
        parts.append(
            jnp.sum(jnp.where(line_rows == start + h, own_lines, 0.0), axis=0, keepdims=True)
        )
    filler = own.shape[0] - heads * comps - heads
    parts.append(jnp.zeros((filler, LANES), jnp.float32))
    own[...] = jnp.concatenate(parts, axis=0).astype(jnp.bfloat16)


def extend(slots, pieces, table_in, *refs):
    table = refs[-1]
    whole = len(slots)
    for n, slot in enumerate(slots):
        vectors, lines = refs[n], refs[whole + n]
        fill_table(shard_quarters(vectors, lines), table, slot * vectors.shape[1] // GROUPS)
    if pieces:
        parts = refs[2 * whole : -1]
        depth = parts[0].shape[1] - LANES
        fill_table(piece_quarters(parts, depth), table, (GROUPS - 1) * depth)


def held_rows(e, branches):
    out = []
    for v in range(branches * branches // SUB):
        low, high = v * SUB // branches, (v * SUB + SUB - 1) // branches
        if low == high:
            out.append(jnp.broadcast_to(e[low : low + 1], (SUB, LANES)))
        else:
            cut = high * branches - v * SUB
            out.append(jnp.where(row_iota(SUB) < cut, e[low : low + 1], e[high : high + 1]))
    return out


def cycled_rows(e, branches):
    period = math.lcm(SUB, branches)
    twice = jnp.concatenate([e[:branches]] * (period // branches), axis=0)
    return [twice[v * SUB : (v + 1) * SUB] for v in range(period // SUB)]


def kernel(
    branches,
    base,
    order,
    rows_any,
    meta,
    table_in,
    own,
    phi,
    cells,
    vectors,
    lines,
    out,
    table,
    gathered_a,
    gathered_b,
    pair_a,
    pair_b,
    single_a,
    single_b,
    wide_a,
    wide_b,
    product_a,
    product_b,
    placed,
    place,
    acc,
    spots,
    sems,
):
    comps = 2 * branches
    pairs = branches * branches
    groups = pairs // SUB
    clusters = SUB
    heads = out.shape[0]
    log = QMESH.bit_length() - 1
    last = rows_any.shape[0] - 1
    count = order[0, last + 1]
    gathered, pair, single = (gathered_a, gathered_b), (pair_a, pair_b), (single_a, single_b)
    wide, product = (wide_a, wide_b), (product_a, product_b)

    def block_at(i):
        return order[0, jnp.clip(i, 0, last)]

    def load(i, p):
        return pltpu.make_async_copy(rows_any.at[block_at(i)], spots.at[p], sems.at[p])

    def gather(p):
        into = gathered[p]
        for which in range(3):
            for n in range(LANES):
                at = which * LANES + n
                into[at : at + 1, :] = table[pl.ds(spots[p, which + 1, n], 1), :]
                yield

    def one_hot(local):
        inside = local & (LANES - 1)
        return jnp.where(row_iota(LANES) == inside, 1.0, 0.0).astype(jnp.bfloat16)

    def choose(i, rows, pair_out, single_out):
        info = meta[block_at(i)]
        local = jnp.where(i < count, info[0:1, :], -1)
        head = lax.shift_right_arithmetic(local, 7)
        spread = jnp.dot(own[...], one_hot(local), preferred_element_type=jnp.float32)
        flats = [rows[w * LANES : (w + 1) * LANES, :].T for w in range(3)]
        yield
        shift = jnp.zeros((clusters, LANES), jnp.int32)
        for which in range(3):
            p = info[which + 1 : which + 2, :] & 0xFFFF
            coords = (
                lax.shift_right_logical(p, 2 * log),
                lax.shift_right_logical(p, log) & (QMESH - 1),
                p & (QMESH - 1),
            )
            for axis in range(3):
                shift = shift + cells[3 * which + axis] * coords[axis]
            yield
        angle = (shift & (QMESH - 1)).astype(jnp.float32) * (2.0 * math.pi / QMESH)
        single_out[0:SUB, :] = jnp.cos(angle)
        yield
        single_out[SUB : 2 * SUB, :] = jnp.sin(angle)
        yield
        others = []
        for which in range(3):
            group = lax.shift_right_logical(info[which + 1 : which + 2, :], 16)
            masks = [group == g for g in range(1, GROUPS)]
            pick = []
            for r in range(0, SLOT, SUB):
                value = flats[which][r : r + SUB]
                for g in range(1, GROUPS):
                    at = g * SLOT + r
                    value = jnp.where(masks[g - 1], flats[which][at : at + SUB], value)
                pick.append(value)
                yield
            others.append(jnp.concatenate(pick, axis=0))
        second, third, fourth = others
        third_re, third_im = held_rows(third, branches), held_rows(third[branches:], branches)
        fourth_re, fourth_im = cycled_rows(fourth, branches), cycled_rows(fourth[branches:], branches)
        period = len(fourth_re)
        for v in range(groups):
            are, aim, bre, bim = third_re[v], third_im[v], fourth_re[v % period], fourth_im[v % period]
            pair_out[v * SUB : (v + 1) * SUB, :] = are * bre - aim * bim
            at = pairs + v * SUB
            pair_out[at : at + SUB, :] = -(are * bim + aim * bre)
            yield
        at = 2 * SUB
        single_out[at : at + SLOT, :] = second
        first = jnp.zeros((comps, LANES), jnp.float32)
        for h in range(heads):
            first = jnp.where(head == h, spread[h * comps : (h + 1) * comps], first)
            yield
        tail = spread[heads * comps :]
        first_freq = jnp.sum(
            jnp.where(row_iota(tail.shape[0]) == head, tail, 0.0), axis=0, keepdims=True
        )
        at += SLOT
        single_out[at : at + comps, :] = first
        at += comps
        wanted = [first_freq] + [e[comps : comps + 1] for e in others]
        wanted.append(local.astype(jnp.float32))
        for n, line in enumerate(wanted):
            single_out[at + n : at + n + 1, :] = line
        yield

    def join(single_in, product_out):
        at = 2 * SUB
        second = single_in[at : at + comps, :]
        at += SLOT
        first = single_in[at : at + comps, :]
        at += comps
        f1, f2, f3, f4, local = (single_in[at + n : at + n + 1, :] for n in range(5))
        yield
        mismatch = f1 + f2 - f3 - f4
        delta = jnp.exp(-((mismatch / smearing) ** 2)) / (smearing * math.sqrt(math.pi))
        yield
        weight = (1.0 + occupation(f2)) * occupation(f3) * occupation(f4) / occupation(f1)
        yield
        at = 2 * pairs
        product_out[at : at + 1, :] = delta * weight / (f1 * f2 * f3 * f4)
        product_out[at + 1 : at + 2, :] = local
        yield
        first_re, first_im = held_rows(first, branches), held_rows(first[branches:], branches)
        second_re, second_im = cycled_rows(second, branches), cycled_rows(second[branches:], branches)
        period = len(second_re)
        for v in range(groups):
            are, aim, bre, bim = first_re[v], first_im[v], second_re[v % period], second_im[v % period]
            product_out[v * SUB : (v + 1) * SUB, :] = are * bre - aim * bim
            at = pairs + v * SUB
            product_out[at : at + SUB, :] = are * bim + aim * bre
            yield

    def turn(pair_in, single_in, wide_out):
        for k in range(clusters):
            cos_k, sin_k = single_in[k : k + 1, :], single_in[SUB + k : SUB + k + 1, :]
            for v in range(0, groups, 2):
                both = []
                for u in (v, v + 1):
                    re = pair_in[u * SUB : (u + 1) * SUB, :]
                    im = pair_in[pairs + u * SUB : pairs + (u + 1) * SUB, :]
                    both.append((cos_k * re - sin_k * im, cos_k * im + sin_k * re))
                at = k * pairs + v * SUB
                for part in range(2):
                    wide_out[at : at + 2 * SUB, part * LANES : (part + 1) * LANES] = jnp.concatenate(
                        [both[0][part], both[1][part]], axis=0
                    ).astype(jnp.bfloat16)
                yield

    def finish(i, weighted, product_in):
        sum_re = jnp.zeros((SUB, LANES), jnp.float32)
        sum_im = sum_re
        for v in range(groups):
            rows = slice(v * SUB, (v + 1) * SUB)
            nre = product_in[rows, :]
            nim = product_in[pairs + v * SUB : pairs + (v + 1) * SUB, :]
            wre, wim = weighted[rows, :LANES], weighted[rows, LANES:]
            sum_re = sum_re + (nre * wre - nim * wim)
            sum_im = sum_im + (nre * wim + nim * wre)
            yield
        value_re = jnp.sum(sum_re, axis=0, keepdims=True)
        value_im = jnp.sum(sum_im, axis=0, keepdims=True)
        yield
        at = 2 * pairs
        factor = product_in[at : at + 1, :]
        local = product_in[at + 1 : at + 2, :].astype(jnp.int32)
        local = jnp.where(i >= 0, local, -1)
        term = (value_re * value_re + value_im * value_im) * factor
        size = acc.shape[0]
        rest = jnp.where(row_iota(size) == lax.shift_right_arithmetic(local, 7), term, 0.0)
        place[0:1, :] = local
        yield
        for n in range(3):
            part = rest.astype(jnp.bfloat16)
            placed[n * size : (n + 1) * size, :] = part
            rest = rest - part.astype(jnp.float32)
        yield

    def run(*tracks):
        total_steps = max(n for _, n in tracks)
        done = [0] * len(tracks)
        for step in range(1, total_steps + 1):
            for t, (track, n) in enumerate(tracks):
                while done[t] * total_steps < step * n:
                    next(track, None)
                    done[t] += 1
        for track, _ in tracks:
            for _ in track:
                pass

    gather_steps = 3 * LANES
    choose_steps = 20 + groups + heads
    join_steps = 4 + groups
    turn_steps = clusters * groups // 2
    finish_steps = groups + 3

    pieces = [(at, min(at + DEPTH, clusters * pairs)) for at in range(0, clusters * pairs, DEPTH)]

    def multiply(wide_in, held):
        for low, high in pieces:
            part = jnp.dot(phi[:, low:high], wide_in[low:high, :], preferred_element_type=jnp.float32)
            held[:] = [part if not held else held[0] + part]
            yield

    def step(i, p):
        load(i + 3, 1 - p).start()
        load(i + 2, p).wait()
        sums = lax.dot_general(
            placed[...],
            one_hot(place[0:1, :]),
            (((1,), (1,)), ((), ())),
            preferred_element_type=jnp.float32,
        )
        weighted = []
        run(
            (choose(i + 1, gathered[1 - p], pair[1 - p], single[1 - p]), choose_steps),
            (multiply(wide[1 - p], weighted), len(pieces)),
            (turn(pair[p], single[p], wide[p]), turn_steps),
            (join(single[p], product[p]), join_steps),
            (gather(p), gather_steps),
        )
        run((finish(i - 1, weighted[0], product[1 - p]), finish_steps))
        size = acc.shape[0]
        acc[...] += sums[:size] + sums[size : 2 * size] + sums[2 * size :]

    load(0, 0).start()
    load(1, 1).start()
    acc[...] = jnp.zeros_like(acc)
    placed[...] = jnp.zeros_like(placed)
    place[...] = jnp.zeros_like(place)
    fill_table(shard_quarters(vectors, lines), table, base)
    load(0, 0).wait()
    run((gather(0), gather_steps))
    load(2, 0).start()
    load(1, 1).wait()
    run((choose(0, gathered_a, pair_a, single_a), choose_steps), (gather(1), gather_steps))

    def two_steps(j, carry):
        step(2 * j, 0)

        @pl.when(2 * j + 1 < count + 2)
        def _():
            step(2 * j + 1, 1)

        return carry

    lax.fori_loop(0, lax.div(count + 3, 2), two_steps, 0)
    even = lax.rem(count, 2) == 0

    @pl.when(even)
    def _():
        load(0, 0).wait()

    @pl.when(jnp.logical_not(even))
    def _():
        load(0, 1).wait()

    out[...] = acc[:heads, :]


def rates_call(branches, base, heads, padded, *args):
    rows, table, phi = args[1], args[3], args[5]
    pairs = branches * branches
    singles = 2 * SUB + SLOT + 2 * branches + SUB
    vmem = pl.BlockSpec(memory_space=pltpu.VMEM)
    smem = pl.BlockSpec(memory_space=pltpu.SMEM)
    loose = pl.BlockSpec(memory_space=pl.ANY)
    rates, _ = pl.pallas_call(
        functools.partial(kernel, branches, base),
        out_shape=[
            jax.ShapeDtypeStruct((heads, LANES), jnp.float32),
            jax.ShapeDtypeStruct(table.shape, table.dtype),
        ],
        in_specs=[smem, loose] + [vmem] * 7,
        out_specs=[vmem, vmem],
        input_output_aliases={3: 1},
        scratch_shapes=[
            *[pltpu.VMEM((3 * LANES, LANES), jnp.float32)] * 2,
            *[pltpu.VMEM((2 * pairs, LANES), jnp.float32)] * 2,
            *[pltpu.VMEM((singles, LANES), jnp.float32)] * 2,
            *[pltpu.VMEM((phi.shape[1], 2 * LANES), jnp.bfloat16)] * 2,
            *[pltpu.VMEM((2 * pairs + SUB, LANES), jnp.float32)] * 2,
            pltpu.VMEM((3 * padded, LANES), jnp.bfloat16),
            pltpu.VMEM((SUB, LANES), jnp.int32),
            pltpu.VMEM((padded, LANES), jnp.float32),
            pltpu.SMEM((AHEAD, *rows.shape[1:]), jnp.int32),
            pltpu.SemaphoreType.DMA((AHEAD,)),
        ],
        compiler_params=pltpu.CompilerParams(vmem_limit_bytes=16 * 1024 * 1024),
    )(*args)
    return rates


def body(quartets, counts, eig, freq, phi, cells):
    comps, local = eig.shape
    branches = comps // 2
    shards = lax.axis_size("pb")
    workers = lax.axis_size("wa")
    held, parts, block = quartets.shape
    kept = local // workers
    heads = window(kept)
    clusters = cells.shape[0]
    offset = local * shards // 2
    both = ("pb", "wa")
    worker = lax.axis_index("wa")
    lines = freq.reshape(local // LANES, LANES)

    def swap(x):
        return lax.ppermute(x, "wa", [(i, i ^ 1) for i in range(workers)])

    def across(x, even, odd):
        pairs = []
        for p in range(shards):
            for w in range(workers):
                pairs.append((p * workers + w, (p ^ (odd if w % 2 else even)) * workers + w))
        return lax.ppermute(x, both, pairs)

    depth = local // GROUPS
    pieces = []
    if shards == GROUPS:
        which = worker % GROUPS
        rows = depth // LANES
        payload = jnp.concatenate(
            [
                lax.dynamic_slice_in_dim(eig, which * depth, depth, 1),
                lax.dynamic_slice_in_dim(lines, which * rows, rows, 0),
            ],
            axis=1,
        )
        straight = across(payload, shards - 1, shards - 1)
        one = across(eig, 1, 2)
        one_lines = across(lines, 1, 2)
        along = lax.ppermute(straight, "wa", [(i, i ^ 2) for i in range(workers)])
        pieces = [straight, swap(straight), along]
        pieces.append(swap(along))
        vectors = [eig, one, swap(one)]
        rows_of = [lines, one_lines, swap(one_lines)]
    else:
        vectors, rows_of = [eig], [lines]
        for k in range(1, shards):
            vectors.append(across(eig, k, k))
            rows_of.append(across(lines, k, k))

    slots = jnp.arange(held, dtype=jnp.int32)[:, None, None]
    coded = (jnp.where(slots < counts[0], quartets, -1) - offset).astype(jnp.int16)
    coded = coded.reshape(held * parts, block)
    line_up = [coded]
    for k in range(2, workers, 2):
        line_up.append(lax.ppermute(coded, "wa", [(i, i ^ k) for i in range(workers)]))
    column = jnp.concatenate(line_up, axis=0)
    other_column = swap(column)
    vmem = pl.BlockSpec(memory_space=pltpu.VMEM)
    smem = pl.BlockSpec(memory_space=pltpu.SMEM)
    hbm = pl.BlockSpec(memory_space=pl.ANY)
    far_space = pl.BlockSpec(memory_space=pltpu.HBM)
    total_rows = workers * held * parts
    rows, meta, order = pl.pallas_call(
        functools.partial(prepare, branches, local, kept, offset),
        out_shape=[
            jax.ShapeDtypeStruct((total_rows, LANES), jnp.int32),
            jax.ShapeDtypeStruct((total_rows, LANES), jnp.int32),
            jax.ShapeDtypeStruct((1, total_rows // parts + LANES), jnp.int32),
        ],
        in_specs=[vmem, vmem],
        out_specs=[vmem] * 3,
        compiler_params=pltpu.CompilerParams(vmem_limit_bytes=16 * 1024 * 1024),
    )(column, other_column)
    blocks = total_rows // parts
    padded = -(-heads // 16) * 16
    own_rows = -(-heads * (comps + 1) // 16) * 16
    table, own, phi, spread_cells = pl.pallas_call(
        functools.partial(begin, kept, heads),
        out_shape=[
            jax.ShapeDtypeStruct((shards * depth, LANES), jnp.float32),
            jax.ShapeDtypeStruct((own_rows, LANES), jnp.bfloat16),
            jax.ShapeDtypeStruct(phi.shape, phi.dtype),
            jax.ShapeDtypeStruct((cells.shape[1], clusters, LANES), jnp.int32),
        ],
        in_specs=[vmem] * 4,
        out_specs=[vmem] * 4,
        compiler_params=pltpu.CompilerParams(vmem_limit_bytes=16 * 1024 * 1024),
    )(eig, lines, phi, cells)
    final = len(vectors) - 1
    whole = tuple(range(1, final))
    table = pl.pallas_call(
        functools.partial(extend, whole, bool(pieces)),
        out_shape=jax.ShapeDtypeStruct(table.shape, table.dtype),
        in_specs=[vmem] * (1 + 2 * len(whole) + len(pieces)),
        out_specs=vmem,
        input_output_aliases={0: 0},
        compiler_params=pltpu.CompilerParams(vmem_limit_bytes=16 * 1024 * 1024),
    )(table, *vectors[1:final], *rows_of[1:final], *pieces)
    rates = rates_call(
        branches,
        final * depth,
        heads,
        padded,
        order,
        rows.reshape(blocks, parts, LANES),
        meta.reshape(blocks, parts, LANES),
        table,
        own,
        phi,
        spread_cells,
        vectors[final],
        rows_of[final],
    )
    rates = rates.reshape(heads * LANES)
    if heads * LANES == kept:
        return rates
    return lax.dynamic_slice_in_dim(rates, lax.axis_index("wa") * kept % LANES, kept, 0)


def solution(mesh):
    placed = (P(("pb", "wa"), None, None), P(("pb", "wa")), P(None, "pb"), P("pb"), P(), P())
    return jax.shard_map(
        body, mesh=mesh, in_specs=placed, out_specs=P(("pb", "wa")), check_vma=False
    )
```

```python
import functools
import math

import jax
import jax.numpy as jnp
from jax import lax
from jax.experimental import pallas as pl
from jax.experimental.pallas import tpu as pltpu
from jax.sharding import PartitionSpec as P


QMESH = 16
LANES = 128
SUB = 8
GROUPS = 4
SLOT = LANES // GROUPS
PARTS = 4
AHEAD = 2
DEPTH = 256

smearing = 0.5


def occupation(value):
    return 1.0 / (jnp.exp(value) - 1.0)


def row_iota(rows):
    return lax.broadcasted_iota(jnp.int32, (rows, LANES), 0)


def window(kept):
    return -(-(kept + LANES - math.gcd(kept, LANES)) // LANES)


def prepare(branches, local, kept, offset, *refs):
    pool, (rows_out, meta_out, order_out) = refs[:-3], refs[-3:]
    mine = lax.axis_index("pb")
    side = lax.rem(lax.axis_index("wa"), 2)
    start = lax.axis_index("wa") * kept
    lead = lax.rem(start, LANES)
    shards = lax.axis_size("pb")
    modes = jnp.concatenate([r[...].astype(jnp.int32) for r in pool], axis=0) + offset
    count = modes.shape[0]
    heading = (row_iota(count) & (PARTS - 1)) == 0
    safe = jnp.maximum(modes, 0)
    middle = safe.astype(jnp.float32) + 0.5
    owner = (middle * (1.0 / local)).astype(jnp.int32)
    point = (middle * (1.0 / branches)).astype(jnp.int32)
    near = owner ^ mine
    slot = near
    if shards == GROUPS:
        slot = jnp.where(near == 1, 1 + side, jnp.where(near == 2, 2 - side, near))
    inner = safe - owner * local
    depth = local // GROUPS
    group = ((inner.astype(jnp.float32) + 0.5) * (1.0 / depth)).astype(jnp.int32)
    rows_out[...] = (slot - group) * depth + inner
    following = pltpu.roll(modes, count - 1, 0)
    first = modes - start
    valid = heading & (following >= 0) & (first >= 0) & (first < kept)
    meta_out[...] = jnp.where(
        heading, jnp.where(valid, first + lead, -1), point + group * 65536
    )
    lanes = (((1,), (1,)), ((), ()))
    marks = lax.dot_general(
        jnp.ones((SUB, LANES), jnp.bfloat16),
        jnp.where(valid, 1.0, 0.0).astype(jnp.bfloat16),
        lanes,
        preferred_element_type=jnp.float32,
    )
    blocks = count // PARTS

    def index(rows, dim):
        return lax.broadcasted_iota(jnp.int32, (rows, blocks), dim)

    fold = jnp.where(index(count, 0) // PARTS == index(count, 1), 1.0, 0.0).astype(jnp.bfloat16)
    found = jnp.dot(marks.astype(jnp.bfloat16), fold, preferred_element_type=jnp.float32) > 0.5
    before = jnp.where(index(blocks, 0) <= index(blocks, 1), 1.0, 0.0).astype(jnp.bfloat16)
    rank = jnp.dot(
        jnp.where(found, 1.0, 0.0).astype(jnp.bfloat16), before, preferred_element_type=jnp.float32
    )
    spot = jnp.where(found, rank, 0.0)[0:1, :].astype(jnp.int32)
    chosen = jnp.where(index(blocks, 0) + 1 == spot, 1.0, 0.0).astype(jnp.bfloat16)
    number = index(SUB, 1)
    order = jnp.zeros((SUB, blocks), jnp.float32)
    for digit, scale in ((number & 15, 1.0), (number >> 4, 16.0)):
        order = order + scale * lax.dot_general(
            digit.astype(jnp.float32).astype(jnp.bfloat16),
            chosen,
            lanes,
            preferred_element_type=jnp.float32,
        )
    order_out[:, :blocks] = order[0:1, :].astype(jnp.int32)
    order_out[:, blocks:] = jnp.broadcast_to(rank[0:1, blocks - 1 :], (1, LANES)).astype(jnp.int32)


def shard_quarters(vectors, lines):
    depth = vectors.shape[1] // GROUPS

    def quarter(g):
        def chunk(t):
            at = g * depth + t * LANES
            row = at // LANES
            return vectors[:, at : at + LANES], lines[row : row + 1, :]

        return chunk

    return [quarter(g) for g in range(GROUPS)], depth


def fill_table(source, table, base):
    quarters, depth = source
    for t in range(depth // LANES):
        stack = []
        for quarter in quarters:
            vectors, line = quarter(t)
            stack.append(vectors.astype(jnp.float32))
            filler = SLOT - vectors.shape[0]
            stack.append(jnp.broadcast_to(line.astype(jnp.float32), (filler, LANES)))
        row = base + t * LANES
        table[row : row + LANES, :] = jnp.concatenate(stack, axis=0).T


def begin(kept, heads, vectors, lines, phi_in, cells_in, table, own, phi, cells):
    comps = vectors.shape[0]
    phi[...] = phi_in[...]
    cell = cells_in[...]
    for j in range(cell.shape[1]):
        column = cell[:, j : j + 1]
        cells[j] = jnp.broadcast_to(column if j < 3 else -column, (cell.shape[0], LANES))
    fill_table(shard_quarters(vectors, lines), table, 0)
    start = lax.axis_index("wa") * kept // LANES
    own_lines = lines[...].astype(jnp.float32)
    line_rows = row_iota(own_lines.shape[0])
    parts = []
    for h in range(heads):
        at = pl.multiple_of((start + h) * LANES, LANES)
        parts.append(vectors[:, pl.ds(at, LANES)].astype(jnp.float32))
    for h in range(heads):
        parts.append(
            jnp.sum(jnp.where(line_rows == start + h, own_lines, 0.0), axis=0, keepdims=True)
        )
    filler = own.shape[0] - heads * comps - heads
    parts.append(jnp.zeros((filler, LANES), jnp.float32))
    own[...] = jnp.concatenate(parts, axis=0).astype(jnp.bfloat16)


def extend(slots, table_in, *refs):
    table = refs[-1]
    whole = len(slots)
    for n, slot in enumerate(slots):
        vectors, lines = refs[n], refs[whole + n]
        fill_table(shard_quarters(vectors, lines), table, slot * vectors.shape[1] // GROUPS)


def held_rows(e, branches):
    out = []
    for v in range(branches * branches // SUB):
        low, high = v * SUB // branches, (v * SUB + SUB - 1) // branches
        if low == high:
            out.append(jnp.broadcast_to(e[low : low + 1], (SUB, LANES)))
        else:
            cut = high * branches - v * SUB
            out.append(jnp.where(row_iota(SUB) < cut, e[low : low + 1], e[high : high + 1]))
    return out


def cycled_rows(e, branches):
    period = math.lcm(SUB, branches)
    twice = jnp.concatenate([e[:branches]] * (period // branches), axis=0)
    return [twice[v * SUB : (v + 1) * SUB] for v in range(period // SUB)]


def kernel(
    branches,
    base,
    order,
    rows_any,
    meta,
    table_in,
    own,
    phi,
    cells,
    vectors,
    lines,
    out,
    table,
    gathered_a,
    gathered_b,
    pair_a,
    pair_b,
    single_a,
    single_b,
    wide_a,
    wide_b,
    product_a,
    product_b,
    placed,
    place,
    acc,
    spots,
    sems,
):
    comps = 2 * branches
    pairs = branches * branches
    groups = pairs // SUB
    clusters = SUB
    heads = out.shape[0]
    log = QMESH.bit_length() - 1
    last = rows_any.shape[0] - 1
    count = order[0, last + 1]
    gathered, pair, single = (gathered_a, gathered_b), (pair_a, pair_b), (single_a, single_b)
    wide, product = (wide_a, wide_b), (product_a, product_b)

    def block_at(i):
        return order[0, jnp.clip(i, 0, last)]

    def load(i, p):
        return pltpu.make_async_copy(rows_any.at[block_at(i)], spots.at[p], sems.at[p])

    def gather(p):
        into = gathered[p]
        for which in range(3):
            for n in range(LANES):
                at = which * LANES + n
                into[at : at + 1, :] = table[pl.ds(spots[p, which + 1, n], 1), :]
                yield

    def one_hot(local):
        inside = local & (LANES - 1)
        return jnp.where(row_iota(LANES) == inside, 1.0, 0.0).astype(jnp.bfloat16)

    def choose(i, rows, pair_out, single_out):
        info = meta[block_at(i)]
        local = jnp.where(i < count, info[0:1, :], -1)
        head = lax.shift_right_arithmetic(local, 7)
        spread = jnp.dot(own[...], one_hot(local), preferred_element_type=jnp.float32)
        flats = [rows[w * LANES : (w + 1) * LANES, :].T for w in range(3)]
        yield
        shift = jnp.zeros((clusters, LANES), jnp.int32)
        for which in range(3):
            p = info[which + 1 : which + 2, :] & 0xFFFF
            coords = (
                lax.shift_right_logical(p, 2 * log),
                lax.shift_right_logical(p, log) & (QMESH - 1),
                p & (QMESH - 1),
            )
            for axis in range(3):
                shift = shift + cells[3 * which + axis] * coords[axis]
            yield
        angle = (shift & (QMESH - 1)).astype(jnp.float32) * (2.0 * math.pi / QMESH)
        single_out[0:SUB, :] = jnp.cos(angle)
        yield
        single_out[SUB : 2 * SUB, :] = jnp.sin(angle)
        yield
        others = []
        for which in range(3):
            group = lax.shift_right_logical(info[which + 1 : which + 2, :], 16)
            masks = [group == g for g in range(1, GROUPS)]
            pick = []
            for r in range(0, SLOT, SUB):
                value = flats[which][r : r + SUB]
                for g in range(1, GROUPS):
                    at = g * SLOT + r
                    value = jnp.where(masks[g - 1], flats[which][at : at + SUB], value)
                pick.append(value)
                yield
            others.append(jnp.concatenate(pick, axis=0))
        second, third, fourth = others
        third_re, third_im = held_rows(third, branches), held_rows(third[branches:], branches)
        fourth_re, fourth_im = cycled_rows(fourth, branches), cycled_rows(fourth[branches:], branches)
        period = len(fourth_re)
        for v in range(groups):
            are, aim, bre, bim = third_re[v], third_im[v], fourth_re[v % period], fourth_im[v % period]
            pair_out[v * SUB : (v + 1) * SUB, :] = are * bre - aim * bim
            at = pairs + v * SUB
            pair_out[at : at + SUB, :] = -(are * bim + aim * bre)
            yield
        at = 2 * SUB
        single_out[at : at + SLOT, :] = second
        first = jnp.zeros((comps, LANES), jnp.float32)
        for h in range(heads):
            first = jnp.where(head == h, spread[h * comps : (h + 1) * comps], first)
            yield
        tail = spread[heads * comps :]
        first_freq = jnp.sum(
            jnp.where(row_iota(tail.shape[0]) == head, tail, 0.0), axis=0, keepdims=True
        )
        at += SLOT
        single_out[at : at + comps, :] = first
        at += comps
        wanted = [first_freq] + [e[comps : comps + 1] for e in others]
        wanted.append(local.astype(jnp.float32))
        for n, line in enumerate(wanted):
            single_out[at + n : at + n + 1, :] = line
        yield

    def join(single_in, product_out):
        at = 2 * SUB
        second = single_in[at : at + comps, :]
        at += SLOT
        first = single_in[at : at + comps, :]
        at += comps
        f1, f2, f3, f4, local = (single_in[at + n : at + n + 1, :] for n in range(5))
        yield
        mismatch = f1 + f2 - f3 - f4
        delta = jnp.exp(-((mismatch / smearing) ** 2)) / (smearing * math.sqrt(math.pi))
        yield
        weight = (1.0 + occupation(f2)) * occupation(f3) * occupation(f4) / occupation(f1)
        yield
        at = 2 * pairs
        product_out[at : at + 1, :] = delta * weight / (f1 * f2 * f3 * f4)
        product_out[at + 1 : at + 2, :] = local
        yield
        first_re, first_im = held_rows(first, branches), held_rows(first[branches:], branches)
        second_re, second_im = cycled_rows(second, branches), cycled_rows(second[branches:], branches)
        period = len(second_re)
        for v in range(groups):
            are, aim, bre, bim = first_re[v], first_im[v], second_re[v % period], second_im[v % period]
            product_out[v * SUB : (v + 1) * SUB, :] = are * bre - aim * bim
            at = pairs + v * SUB
            product_out[at : at + SUB, :] = are * bim + aim * bre
            yield

    def turn(pair_in, single_in, wide_out):
        for k in range(clusters):
            cos_k, sin_k = single_in[k : k + 1, :], single_in[SUB + k : SUB + k + 1, :]
            for v in range(0, groups, 2):
                both = []
                for u in (v, v + 1):
                    re = pair_in[u * SUB : (u + 1) * SUB, :]
                    im = pair_in[pairs + u * SUB : pairs + (u + 1) * SUB, :]
                    both.append((cos_k * re - sin_k * im, cos_k * im + sin_k * re))
                at = k * pairs + v * SUB
                for part in range(2):
                    wide_out[at : at + 2 * SUB, part * LANES : (part + 1) * LANES] = jnp.concatenate(
                        [both[0][part], both[1][part]], axis=0
                    ).astype(jnp.bfloat16)
                yield

    def finish(i, weighted, product_in):
        sum_re = jnp.zeros((SUB, LANES), jnp.float32)
        sum_im = sum_re
        for v in range(groups):
            rows = slice(v * SUB, (v + 1) * SUB)
            nre = product_in[rows, :]
            nim = product_in[pairs + v * SUB : pairs + (v + 1) * SUB, :]
            wre, wim = weighted[rows, :LANES], weighted[rows, LANES:]
            sum_re = sum_re + (nre * wre - nim * wim)
            sum_im = sum_im + (nre * wim + nim * wre)
            yield
        value_re = jnp.sum(sum_re, axis=0, keepdims=True)
        value_im = jnp.sum(sum_im, axis=0, keepdims=True)
        yield
        at = 2 * pairs
        factor = product_in[at : at + 1, :]
        local = product_in[at + 1 : at + 2, :].astype(jnp.int32)
        local = jnp.where(i >= 0, local, -1)
        term = (value_re * value_re + value_im * value_im) * factor
        size = acc.shape[0]
        rest = jnp.where(row_iota(size) == lax.shift_right_arithmetic(local, 7), term, 0.0)
        place[0:1, :] = local
        yield
        for n in range(3):
            part = rest.astype(jnp.bfloat16)
            placed[n * size : (n + 1) * size, :] = part
            rest = rest - part.astype(jnp.float32)
        yield

    def run(*tracks):
        total_steps = max(n for _, n in tracks)
        done = [0] * len(tracks)
        for step in range(1, total_steps + 1):
            for t, (track, n) in enumerate(tracks):
                while done[t] * total_steps < step * n:
                    next(track, None)
                    done[t] += 1
        for track, _ in tracks:
            for _ in track:
                pass

    gather_steps = 3 * LANES
    choose_steps = 20 + groups + heads
    join_steps = 4 + groups
    turn_steps = clusters * groups // 2
    finish_steps = groups + 3

    pieces = [(at, min(at + DEPTH, clusters * pairs)) for at in range(0, clusters * pairs, DEPTH)]

    def multiply(wide_in, held):
        for low, high in pieces:
            part = jnp.dot(phi[:, low:high], wide_in[low:high, :], preferred_element_type=jnp.float32)
            held[:] = [part if not held else held[0] + part]
            yield

    def step(i, p):
        load(i + 3, 1 - p).start()
        load(i + 2, p).wait()
        sums = lax.dot_general(
            placed[...],
            one_hot(place[0:1, :]),
            (((1,), (1,)), ((), ())),
            preferred_element_type=jnp.float32,
        )
        weighted = []
        run(
            (choose(i + 1, gathered[1 - p], pair[1 - p], single[1 - p]), choose_steps),
            (multiply(wide[1 - p], weighted), len(pieces)),
            (turn(pair[p], single[p], wide[p]), turn_steps),
            (join(single[p], product[p]), join_steps),
            (gather(p), gather_steps),
        )
        run((finish(i - 1, weighted[0], product[1 - p]), finish_steps))
        size = acc.shape[0]
        acc[...] += sums[:size] + sums[size : 2 * size] + sums[2 * size :]

    load(0, 0).start()
    load(1, 1).start()
    acc[...] = jnp.zeros_like(acc)
    placed[...] = jnp.zeros_like(placed)
    place[...] = jnp.zeros_like(place)
    fill_table(shard_quarters(vectors, lines), table, base)
    load(0, 0).wait()
    run((gather(0), gather_steps))
    load(2, 0).start()
    load(1, 1).wait()
    run((choose(0, gathered_a, pair_a, single_a), choose_steps), (gather(1), gather_steps))

    def two_steps(j, carry):
        step(2 * j, 0)

        @pl.when(2 * j + 1 < count + 2)
        def _():
            step(2 * j + 1, 1)

        return carry

    lax.fori_loop(0, lax.div(count + 3, 2), two_steps, 0)
    even = lax.rem(count, 2) == 0

    @pl.when(even)
    def _():
        load(0, 0).wait()

    @pl.when(jnp.logical_not(even))
    def _():
        load(0, 1).wait()

    out[...] = acc[:heads, :]


def rates_call(branches, base, heads, padded, *args):
    rows, table, phi = args[1], args[3], args[5]
    pairs = branches * branches
    singles = 2 * SUB + SLOT + 2 * branches + SUB
    vmem = pl.BlockSpec(memory_space=pltpu.VMEM)
    smem = pl.BlockSpec(memory_space=pltpu.SMEM)
    loose = pl.BlockSpec(memory_space=pl.ANY)
    rates, _ = pl.pallas_call(
        functools.partial(kernel, branches, base),
        out_shape=[
            jax.ShapeDtypeStruct((heads, LANES), jnp.float32),
            jax.ShapeDtypeStruct(table.shape, table.dtype),
        ],
        in_specs=[smem, loose] + [vmem] * 7,
        out_specs=[vmem, vmem],
        input_output_aliases={3: 1},
        scratch_shapes=[
            *[pltpu.VMEM((3 * LANES, LANES), jnp.float32)] * 2,
            *[pltpu.VMEM((2 * pairs, LANES), jnp.float32)] * 2,
            *[pltpu.VMEM((singles, LANES), jnp.float32)] * 2,
            *[pltpu.VMEM((phi.shape[1], 2 * LANES), jnp.bfloat16)] * 2,
            *[pltpu.VMEM((2 * pairs + SUB, LANES), jnp.float32)] * 2,
            pltpu.VMEM((3 * padded, LANES), jnp.bfloat16),
            pltpu.VMEM((SUB, LANES), jnp.int32),
            pltpu.VMEM((padded, LANES), jnp.float32),
            pltpu.SMEM((AHEAD, *rows.shape[1:]), jnp.int32),
            pltpu.SemaphoreType.DMA((AHEAD,)),
        ],
        compiler_params=pltpu.CompilerParams(vmem_limit_bytes=16 * 1024 * 1024),
    )(*args)
    return rates


def body(quartets, counts, eig, freq, phi, cells):
    comps, local = eig.shape
    branches = comps // 2
    shards = lax.axis_size("pb")
    workers = lax.axis_size("wa")
    held, parts, block = quartets.shape
    kept = local // workers
    heads = window(kept)
    clusters = cells.shape[0]
    offset = local * shards // 2
    both = ("pb", "wa")
    lines = freq.reshape(local // LANES, LANES)

    def swap(x):
        return lax.ppermute(x, "wa", [(i, i ^ 1) for i in range(workers)])

    def across(x, even, odd):
        pairs = []
        for p in range(shards):
            for w in range(workers):
                pairs.append((p * workers + w, (p ^ (odd if w % 2 else even)) * workers + w))
        return lax.ppermute(x, both, pairs)

    depth = local // GROUPS
    if shards == GROUPS:
        vectors, rows_of = [eig], [lines]
        for owned, kind in ((eig, vectors), (lines, rows_of)):
            one = across(owned, 1, 2)
            far = across(one, 2, 1)
            kind += [one, swap(one), far]
    else:
        vectors, rows_of = [eig], [lines]
        for k in range(1, shards):
            vectors.append(across(eig, k, k))
            rows_of.append(across(lines, k, k))

    slots = jnp.arange(held, dtype=jnp.int32)[:, None, None]
    coded = (jnp.where(slots < counts[:, None, None], quartets, -1) - offset).astype(jnp.int16)
    coded = coded.reshape(held * parts, block)
    line_up = [coded]
    for k in range(2, workers, 2):
        line_up.append(lax.ppermute(coded, "wa", [(i, i ^ k) for i in range(workers)]))
    column = jnp.concatenate(line_up, axis=0)
    other_column = swap(column)
    vmem = pl.BlockSpec(memory_space=pltpu.VMEM)
    smem = pl.BlockSpec(memory_space=pltpu.SMEM)
    hbm = pl.BlockSpec(memory_space=pl.ANY)
    far_space = pl.BlockSpec(memory_space=pltpu.HBM)
    total_rows = workers * held * parts
    rows, meta, order = pl.pallas_call(
        functools.partial(prepare, branches, local, kept, offset),
        out_shape=[
            jax.ShapeDtypeStruct((total_rows, LANES), jnp.int32),
            jax.ShapeDtypeStruct((total_rows, LANES), jnp.int32),
            jax.ShapeDtypeStruct((1, total_rows // parts + LANES), jnp.int32),
        ],
        in_specs=[vmem, vmem],
        out_specs=[vmem] * 3,
        compiler_params=pltpu.CompilerParams(vmem_limit_bytes=16 * 1024 * 1024),
    )(column, other_column)
    blocks = total_rows // parts
    padded = -(-heads // 16) * 16
    own_rows = -(-heads * (comps + 1) // 16) * 16
    table, own, phi, spread_cells = pl.pallas_call(
        functools.partial(begin, kept, heads),
        out_shape=[
            jax.ShapeDtypeStruct((shards * depth, LANES), jnp.float32),
            jax.ShapeDtypeStruct((own_rows, LANES), jnp.bfloat16),
            jax.ShapeDtypeStruct(phi.shape, phi.dtype),
            jax.ShapeDtypeStruct((cells.shape[1], clusters, LANES), jnp.int32),
        ],
        in_specs=[vmem] * 4,
        out_specs=[vmem] * 4,
        compiler_params=pltpu.CompilerParams(vmem_limit_bytes=16 * 1024 * 1024),
    )(eig, lines, phi, cells)
    final = len(vectors) - 1
    whole = tuple(range(1, final))
    table = pl.pallas_call(
        functools.partial(extend, whole),
        out_shape=jax.ShapeDtypeStruct(table.shape, table.dtype),
        in_specs=[vmem] * (1 + 2 * len(whole)),
        out_specs=vmem,
        input_output_aliases={0: 0},
        compiler_params=pltpu.CompilerParams(vmem_limit_bytes=16 * 1024 * 1024),
    )(table, *vectors[1:final], *rows_of[1:final])
    rates = rates_call(
        branches,
        final * depth,
        heads,
        padded,
        order,
        rows.reshape(blocks, parts, LANES),
        meta.reshape(blocks, parts, LANES),
        table,
        own,
        phi,
        spread_cells,
        vectors[final],
        rows_of[final],
    )
    rates = rates.reshape(heads * LANES)
    if heads * LANES == kept:
        return rates
    return lax.dynamic_slice_in_dim(rates, lax.axis_index("wa") * kept % LANES, kept, 0)


def solution(mesh):
    placed = (P(("pb", "wa"), None, None), P(("pb", "wa")), P(None, "pb"), P("pb"), P(), P())
    return jax.shard_map(
        body, mesh=mesh, in_specs=placed, out_specs=P(("pb", "wa")), check_vma=False
    )
```

```python
import functools
import math

import jax
import jax.numpy as jnp
from jax import lax
from jax.experimental import pallas as pl
from jax.experimental.pallas import tpu as pltpu
from jax.sharding import PartitionSpec as P


QMESH = 16
LANES = 128
SUB = 8
GROUPS = 4
SLOT = LANES // GROUPS
PARTS = 4
AHEAD = 2
DEPTH = 256

smearing = 0.5


def occupation(value):
    return 1.0 / (jnp.exp(value) - 1.0)


def row_iota(rows):
    return lax.broadcasted_iota(jnp.int32, (rows, LANES), 0)


def window(kept):
    return -(-(kept + LANES - math.gcd(kept, LANES)) // LANES)


def prepare(branches, local, kept, offset, *refs):
    pool, (rows_out, meta_out, order_out) = refs[:-3], refs[-3:]
    mine = lax.axis_index("pb")
    side = lax.rem(lax.axis_index("wa"), 2)
    start = lax.axis_index("wa") * kept
    lead = lax.rem(start, LANES)
    shards = lax.axis_size("pb")
    modes = jnp.concatenate([r[...].astype(jnp.int32) for r in pool], axis=0) + offset
    count = modes.shape[0]
    heading = (row_iota(count) & (PARTS - 1)) == 0
    safe = jnp.maximum(modes, 0)
    middle = safe.astype(jnp.float32) + 0.5
    owner = (middle * (1.0 / local)).astype(jnp.int32)
    point = (middle * (1.0 / branches)).astype(jnp.int32)
    near = owner ^ mine
    slot = near
    if shards == GROUPS:
        slot = jnp.where(near == 1, 1 + side, jnp.where(near == 2, 2 - side, near))
    inner = safe - owner * local
    depth = local // GROUPS
    group = ((inner.astype(jnp.float32) + 0.5) * (1.0 / depth)).astype(jnp.int32)
    rows_out[...] = (slot - group) * depth + inner
    following = pltpu.roll(modes, count - 1, 0)
    first = modes - start
    valid = heading & (following >= 0) & (first >= 0) & (first < kept)
    meta_out[...] = jnp.where(
        heading, jnp.where(valid, first + lead, -1), point + group * 65536
    )
    lanes = (((1,), (1,)), ((), ()))
    marks = lax.dot_general(
        jnp.ones((SUB, LANES), jnp.bfloat16),
        jnp.where(valid, 1.0, 0.0).astype(jnp.bfloat16),
        lanes,
        preferred_element_type=jnp.float32,
    )
    blocks = count // PARTS

    def index(rows, dim):
        return lax.broadcasted_iota(jnp.int32, (rows, blocks), dim)

    fold = jnp.where(index(count, 0) // PARTS == index(count, 1), 1.0, 0.0).astype(jnp.bfloat16)
    found = jnp.dot(marks.astype(jnp.bfloat16), fold, preferred_element_type=jnp.float32) > 0.5
    before = jnp.where(index(blocks, 0) <= index(blocks, 1), 1.0, 0.0).astype(jnp.bfloat16)
    rank = jnp.dot(
        jnp.where(found, 1.0, 0.0).astype(jnp.bfloat16), before, preferred_element_type=jnp.float32
    )
    spot = jnp.where(found, rank, 0.0)[0:1, :].astype(jnp.int32)
    chosen = jnp.where(index(blocks, 0) + 1 == spot, 1.0, 0.0).astype(jnp.bfloat16)
    number = index(SUB, 1)
    order = jnp.zeros((SUB, blocks), jnp.float32)
    for digit, scale in ((number & 15, 1.0), (number >> 4, 16.0)):
        order = order + scale * lax.dot_general(
            digit.astype(jnp.float32).astype(jnp.bfloat16),
            chosen,
            lanes,
            preferred_element_type=jnp.float32,
        )
    order_out[:, :blocks] = order[0:1, :].astype(jnp.int32)
    order_out[:, blocks:] = jnp.broadcast_to(rank[0:1, blocks - 1 :], (1, LANES)).astype(jnp.int32)


def shard_quarters(vectors, lines):
    depth = vectors.shape[1] // GROUPS

    def quarter(g):
        def chunk(t):
            at = g * depth + t * LANES
            row = at // LANES
            return vectors[:, at : at + LANES], lines[row : row + 1, :]

        return chunk

    return [quarter(g) for g in range(GROUPS)], depth


def fill_table(source, table, base):
    quarters, depth = source
    for t in range(depth // LANES):
        stack = []
        for quarter in quarters:
            vectors, line = quarter(t)
            stack.append(vectors.astype(jnp.float32))
            filler = SLOT - vectors.shape[0]
            stack.append(jnp.broadcast_to(line.astype(jnp.float32), (filler, LANES)))
        row = base + t * LANES
        table[row : row + LANES, :] = jnp.concatenate(stack, axis=0).T


def constants(phi_in, cells_in, phi, cells):
    phi[...] = phi_in[...]
    cell = cells_in[...]
    for j in range(cell.shape[1]):
        column = cell[:, j : j + 1]
        cells[j] = jnp.broadcast_to(column if j < 3 else -column, (cell.shape[0], LANES))


def begin(kept, heads, vectors, lines, table, own):
    comps = vectors.shape[0]
    fill_table(shard_quarters(vectors, lines), table, 0)
    start = lax.axis_index("wa") * kept // LANES
    own_lines = lines[...].astype(jnp.float32)
    line_rows = row_iota(own_lines.shape[0])
    parts = []
    for h in range(heads):
        at = pl.multiple_of((start + h) * LANES, LANES)
        parts.append(vectors[:, pl.ds(at, LANES)].astype(jnp.float32))
    for h in range(heads):
        parts.append(
            jnp.sum(jnp.where(line_rows == start + h, own_lines, 0.0), axis=0, keepdims=True)
        )
    filler = own.shape[0] - heads * comps - heads
    parts.append(jnp.zeros((filler, LANES), jnp.float32))
    own[...] = jnp.concatenate(parts, axis=0).astype(jnp.bfloat16)


def extend(slots, table_in, *refs):
    table = refs[-1]
    whole = len(slots)
    for n, slot in enumerate(slots):
        vectors, lines = refs[n], refs[whole + n]
        fill_table(shard_quarters(vectors, lines), table, slot * vectors.shape[1] // GROUPS)


def held_rows(e, branches):
    out = []
    for v in range(branches * branches // SUB):
        low, high = v * SUB // branches, (v * SUB + SUB - 1) // branches
        if low == high:
            out.append(jnp.broadcast_to(e[low : low + 1], (SUB, LANES)))
        else:
            cut = high * branches - v * SUB
            out.append(jnp.where(row_iota(SUB) < cut, e[low : low + 1], e[high : high + 1]))
    return out


def cycled_rows(e, branches):
    period = math.lcm(SUB, branches)
    twice = jnp.concatenate([e[:branches]] * (period // branches), axis=0)
    return [twice[v * SUB : (v + 1) * SUB] for v in range(period // SUB)]


def kernel(
    branches,
    base,
    order,
    rows_any,
    meta,
    table_in,
    own,
    phi,
    cells,
    vectors,
    lines,
    out,
    table,
    gathered_a,
    gathered_b,
    pair_a,
    pair_b,
    single_a,
    single_b,
    wide_a,
    wide_b,
    product_a,
    product_b,
    placed,
    place,
    acc,
    spots,
    sems,
):
    comps = 2 * branches
    pairs = branches * branches
    groups = pairs // SUB
    clusters = SUB
    heads = out.shape[0]
    log = QMESH.bit_length() - 1
    last = rows_any.shape[0] - 1
    count = order[0, last + 1]
    gathered, pair, single = (gathered_a, gathered_b), (pair_a, pair_b), (single_a, single_b)
    wide, product = (wide_a, wide_b), (product_a, product_b)

    def block_at(i):
        return order[0, jnp.clip(i, 0, last)]

    def load(i, p):
        return pltpu.make_async_copy(rows_any.at[block_at(i)], spots.at[p], sems.at[p])

    def gather(p):
        into = gathered[p]
        for which in range(3):
            for n in range(LANES):
                at = which * LANES + n
                into[at : at + 1, :] = table[pl.ds(spots[p, which + 1, n], 1), :]
                yield

    def one_hot(local):
        inside = local & (LANES - 1)
        return jnp.where(row_iota(LANES) == inside, 1.0, 0.0).astype(jnp.bfloat16)

    def choose(i, rows, pair_out, single_out):
        info = meta[block_at(i)]
        local = jnp.where(i < count, info[0:1, :], -1)
        head = lax.shift_right_arithmetic(local, 7)
        spread = jnp.dot(own[...], one_hot(local), preferred_element_type=jnp.float32)
        flats = [rows[w * LANES : (w + 1) * LANES, :].T for w in range(3)]
        yield
        shift = jnp.zeros((clusters, LANES), jnp.int32)
        for which in range(3):
            p = info[which + 1 : which + 2, :] & 0xFFFF
            coords = (
                lax.shift_right_logical(p, 2 * log),
                lax.shift_right_logical(p, log) & (QMESH - 1),
                p & (QMESH - 1),
            )
            for axis in range(3):
                shift = shift + cells[3 * which + axis] * coords[axis]
            yield
        angle = (shift & (QMESH - 1)).astype(jnp.float32) * (2.0 * math.pi / QMESH)
        single_out[0:SUB, :] = jnp.cos(angle)
        yield
        single_out[SUB : 2 * SUB, :] = jnp.sin(angle)
        yield
        others = []
        for which in range(3):
            group = lax.shift_right_logical(info[which + 1 : which + 2, :], 16)
            masks = [group == g for g in range(1, GROUPS)]
            pick = []
            for r in range(0, SLOT, SUB):
                value = flats[which][r : r + SUB]
                for g in range(1, GROUPS):
                    at = g * SLOT + r
                    value = jnp.where(masks[g - 1], flats[which][at : at + SUB], value)
                pick.append(value)
                yield
            others.append(jnp.concatenate(pick, axis=0))
        second, third, fourth = others
        third_re, third_im = held_rows(third, branches), held_rows(third[branches:], branches)
        fourth_re, fourth_im = cycled_rows(fourth, branches), cycled_rows(fourth[branches:], branches)
        period = len(fourth_re)
        for v in range(groups):
            are, aim, bre, bim = third_re[v], third_im[v], fourth_re[v % period], fourth_im[v % period]
            pair_out[v * SUB : (v + 1) * SUB, :] = are * bre - aim * bim
            at = pairs + v * SUB
            pair_out[at : at + SUB, :] = -(are * bim + aim * bre)
            yield
        at = 2 * SUB
        single_out[at : at + SLOT, :] = second
        first = jnp.zeros((comps, LANES), jnp.float32)
        for h in range(heads):
            first = jnp.where(head == h, spread[h * comps : (h + 1) * comps], first)
            yield
        tail = spread[heads * comps :]
        first_freq = jnp.sum(
            jnp.where(row_iota(tail.shape[0]) == head, tail, 0.0), axis=0, keepdims=True
        )
        at += SLOT
        single_out[at : at + comps, :] = first
        at += comps
        wanted = [first_freq] + [e[comps : comps + 1] for e in others]
        wanted.append(local.astype(jnp.float32))
        for n, line in enumerate(wanted):
            single_out[at + n : at + n + 1, :] = line
        yield

    def join(single_in, product_out):
        at = 2 * SUB
        second = single_in[at : at + comps, :]
        at += SLOT
        first = single_in[at : at + comps, :]
        at += comps
        f1, f2, f3, f4, local = (single_in[at + n : at + n + 1, :] for n in range(5))
        yield
        mismatch = f1 + f2 - f3 - f4
        delta = jnp.exp(-((mismatch / smearing) ** 2)) / (smearing * math.sqrt(math.pi))
        yield
        weight = (1.0 + occupation(f2)) * occupation(f3) * occupation(f4) / occupation(f1)
        yield
        at = 2 * pairs
        product_out[at : at + 1, :] = delta * weight / (f1 * f2 * f3 * f4)
        product_out[at + 1 : at + 2, :] = local
        yield
        first_re, first_im = held_rows(first, branches), held_rows(first[branches:], branches)
        second_re, second_im = cycled_rows(second, branches), cycled_rows(second[branches:], branches)
        period = len(second_re)
        for v in range(groups):
            are, aim, bre, bim = first_re[v], first_im[v], second_re[v % period], second_im[v % period]
            product_out[v * SUB : (v + 1) * SUB, :] = are * bre - aim * bim
            at = pairs + v * SUB
            product_out[at : at + SUB, :] = are * bim + aim * bre
            yield

    def turn(pair_in, single_in, wide_out):
        for k in range(clusters):
            cos_k, sin_k = single_in[k : k + 1, :], single_in[SUB + k : SUB + k + 1, :]
            for v in range(0, groups, 2):
                both = []
                for u in (v, v + 1):
                    re = pair_in[u * SUB : (u + 1) * SUB, :]
                    im = pair_in[pairs + u * SUB : pairs + (u + 1) * SUB, :]
                    both.append((cos_k * re - sin_k * im, cos_k * im + sin_k * re))
                at = k * pairs + v * SUB
                for part in range(2):
                    wide_out[at : at + 2 * SUB, part * LANES : (part + 1) * LANES] = jnp.concatenate(
                        [both[0][part], both[1][part]], axis=0
                    ).astype(jnp.bfloat16)
                yield

    def finish(i, weighted, product_in):
        sum_re = jnp.zeros((SUB, LANES), jnp.float32)
        sum_im = sum_re
        for v in range(groups):
            rows = slice(v * SUB, (v + 1) * SUB)
            nre = product_in[rows, :]
            nim = product_in[pairs + v * SUB : pairs + (v + 1) * SUB, :]
            wre, wim = weighted[rows, :LANES], weighted[rows, LANES:]
            sum_re = sum_re + (nre * wre - nim * wim)
            sum_im = sum_im + (nre * wim + nim * wre)
            yield
        value_re = jnp.sum(sum_re, axis=0, keepdims=True)
        value_im = jnp.sum(sum_im, axis=0, keepdims=True)
        yield
        at = 2 * pairs
        factor = product_in[at : at + 1, :]
        local = product_in[at + 1 : at + 2, :].astype(jnp.int32)
        local = jnp.where(i >= 0, local, -1)
        term = (value_re * value_re + value_im * value_im) * factor
        size = acc.shape[0]
        rest = jnp.where(row_iota(size) == lax.shift_right_arithmetic(local, 7), term, 0.0)
        place[0:1, :] = local
        yield
        for n in range(3):
            part = rest.astype(jnp.bfloat16)
            placed[n * size : (n + 1) * size, :] = part
            rest = rest - part.astype(jnp.float32)
        yield

    def run(*tracks):
        total_steps = max(n for _, n in tracks)
        done = [0] * len(tracks)
        for step in range(1, total_steps + 1):
            for t, (track, n) in enumerate(tracks):
                while done[t] * total_steps < step * n:
                    next(track, None)
                    done[t] += 1
        for track, _ in tracks:
            for _ in track:
                pass

    gather_steps = 3 * LANES
    choose_steps = 20 + groups + heads
    join_steps = 4 + groups
    turn_steps = clusters * groups // 2
    finish_steps = groups + 3

    pieces = [(at, min(at + DEPTH, clusters * pairs)) for at in range(0, clusters * pairs, DEPTH)]

    def multiply(wide_in, held):
        for low, high in pieces:
            part = jnp.dot(phi[:, low:high], wide_in[low:high, :], preferred_element_type=jnp.float32)
            held[:] = [part if not held else held[0] + part]
            yield

    def step(i, p):
        load(i + 3, 1 - p).start()
        load(i + 2, p).wait()
        sums = lax.dot_general(
            placed[...],
            one_hot(place[0:1, :]),
            (((1,), (1,)), ((), ())),
            preferred_element_type=jnp.float32,
        )
        weighted = []
        run(
            (choose(i + 1, gathered[1 - p], pair[1 - p], single[1 - p]), choose_steps),
            (multiply(wide[1 - p], weighted), len(pieces)),
            (turn(pair[p], single[p], wide[p]), turn_steps),
            (join(single[p], product[p]), join_steps),
            (gather(p), gather_steps),
        )
        run((finish(i - 1, weighted[0], product[1 - p]), finish_steps))
        size = acc.shape[0]
        acc[...] += sums[:size] + sums[size : 2 * size] + sums[2 * size :]

    load(0, 0).start()
    load(1, 1).start()
    acc[...] = jnp.zeros_like(acc)
    placed[...] = jnp.zeros_like(placed)
    place[...] = jnp.zeros_like(place)
    fill_table(shard_quarters(vectors, lines), table, base)
    load(0, 0).wait()
    run((gather(0), gather_steps))
    load(2, 0).start()
    load(1, 1).wait()
    run((choose(0, gathered_a, pair_a, single_a), choose_steps), (gather(1), gather_steps))

    def two_steps(j, carry):
        step(2 * j, 0)

        @pl.when(2 * j + 1 < count + 2)
        def _():
            step(2 * j + 1, 1)

        return carry

    lax.fori_loop(0, lax.div(count + 3, 2), two_steps, 0)
    even = lax.rem(count, 2) == 0

    @pl.when(even)
    def _():
        load(0, 0).wait()

    @pl.when(jnp.logical_not(even))
    def _():
        load(0, 1).wait()

    out[...] = acc[:heads, :]


def rates_call(branches, base, heads, padded, *args):
    rows, table, phi = args[1], args[3], args[5]
    pairs = branches * branches
    singles = 2 * SUB + SLOT + 2 * branches + SUB
    vmem = pl.BlockSpec(memory_space=pltpu.VMEM)
    smem = pl.BlockSpec(memory_space=pltpu.SMEM)
    loose = pl.BlockSpec(memory_space=pl.ANY)
    rates, _ = pl.pallas_call(
        functools.partial(kernel, branches, base),
        out_shape=[
            jax.ShapeDtypeStruct((heads, LANES), jnp.float32),
            jax.ShapeDtypeStruct(table.shape, table.dtype),
        ],
        in_specs=[smem, loose] + [vmem] * 7,
        out_specs=[vmem, vmem],
        input_output_aliases={3: 1},
        scratch_shapes=[
            *[pltpu.VMEM((3 * LANES, LANES), jnp.float32)] * 2,
            *[pltpu.VMEM((2 * pairs, LANES), jnp.float32)] * 2,
            *[pltpu.VMEM((singles, LANES), jnp.float32)] * 2,
            *[pltpu.VMEM((phi.shape[1], 2 * LANES), jnp.bfloat16)] * 2,
            *[pltpu.VMEM((2 * pairs + SUB, LANES), jnp.float32)] * 2,
            pltpu.VMEM((3 * padded, LANES), jnp.bfloat16),
            pltpu.VMEM((SUB, LANES), jnp.int32),
            pltpu.VMEM((padded, LANES), jnp.float32),
            pltpu.SMEM((AHEAD, *rows.shape[1:]), jnp.int32),
            pltpu.SemaphoreType.DMA((AHEAD,)),
        ],
        compiler_params=pltpu.CompilerParams(vmem_limit_bytes=16 * 1024 * 1024),
    )(*args)
    return rates


def body(quartets, counts, eig, freq, phi, cells):
    comps, local = eig.shape
    branches = comps // 2
    shards = lax.axis_size("pb")
    workers = lax.axis_size("wa")
    held, parts, block = quartets.shape
    kept = local // workers
    heads = window(kept)
    clusters = cells.shape[0]
    offset = local * shards // 2
    both = ("pb", "wa")
    lines = freq.reshape(local // LANES, LANES)

    def swap(x):
        return lax.ppermute(x, "wa", [(i, i ^ 1) for i in range(workers)])

    def across(x, even, odd):
        pairs = []
        for p in range(shards):
            for w in range(workers):
                pairs.append((p * workers + w, (p ^ (odd if w % 2 else even)) * workers + w))
        return lax.ppermute(x, both, pairs)

    depth = local // GROUPS
    if shards == GROUPS:
        one = across(eig, 1, 2)
        far = across(one, 2, 1)
        vectors = [eig, one, swap(one), far]
        one_lines = across(lines, 1, 2)
        far_lines = across(lines, shards - 1, shards - 1)
        rows_of = [lines, one_lines, swap(one_lines), far_lines]
    else:
        vectors, rows_of = [eig], [lines]
        for k in range(1, shards):
            vectors.append(across(eig, k, k))
            rows_of.append(across(lines, k, k))

    slots = jnp.arange(held, dtype=jnp.int32)[:, None, None]
    coded = (jnp.where(slots < counts[:, None, None], quartets, -1) - offset).astype(jnp.int16)
    coded = coded.reshape(held * parts, block)
    line_up = [coded]
    for k in range(2, workers, 2):
        line_up.append(lax.ppermute(coded, "wa", [(i, i ^ k) for i in range(workers)]))
    column = jnp.concatenate(line_up, axis=0)
    other_column = swap(column)
    vmem = pl.BlockSpec(memory_space=pltpu.VMEM)
    smem = pl.BlockSpec(memory_space=pltpu.SMEM)
    hbm = pl.BlockSpec(memory_space=pl.ANY)
    far_space = pl.BlockSpec(memory_space=pltpu.HBM)
    total_rows = workers * held * parts
    rows, meta, order = pl.pallas_call(
        functools.partial(prepare, branches, local, kept, offset),
        out_shape=[
            jax.ShapeDtypeStruct((total_rows, LANES), jnp.int32),
            jax.ShapeDtypeStruct((total_rows, LANES), jnp.int32),
            jax.ShapeDtypeStruct((1, total_rows // parts + LANES), jnp.int32),
        ],
        in_specs=[vmem, vmem],
        out_specs=[vmem] * 3,
        compiler_params=pltpu.CompilerParams(vmem_limit_bytes=16 * 1024 * 1024),
    )(column, other_column)
    blocks = total_rows // parts
    padded = -(-heads // 16) * 16
    own_rows = -(-heads * (comps + 1) // 16) * 16
    phi, spread_cells = pl.pallas_call(
        constants,
        out_shape=[
            jax.ShapeDtypeStruct(phi.shape, phi.dtype),
            jax.ShapeDtypeStruct((cells.shape[1], clusters, LANES), jnp.int32),
        ],
        in_specs=[vmem] * 2,
        out_specs=[vmem] * 2,
        compiler_params=pltpu.CompilerParams(vmem_limit_bytes=16 * 1024 * 1024),
    )(phi, cells)
    table, own = pl.pallas_call(
        functools.partial(begin, kept, heads),
        out_shape=[
            jax.ShapeDtypeStruct((shards * depth, LANES), jnp.float32),
            jax.ShapeDtypeStruct((own_rows, LANES), jnp.bfloat16),
        ],
        in_specs=[vmem] * 2,
        out_specs=[vmem] * 2,
        compiler_params=pltpu.CompilerParams(vmem_limit_bytes=16 * 1024 * 1024),
    )(eig, lines)
    final = len(vectors) - 1
    whole = tuple(range(1, final))
    table = pl.pallas_call(
        functools.partial(extend, whole),
        out_shape=jax.ShapeDtypeStruct(table.shape, table.dtype),
        in_specs=[vmem] * (1 + 2 * len(whole)),
        out_specs=vmem,
        input_output_aliases={0: 0},
        compiler_params=pltpu.CompilerParams(vmem_limit_bytes=16 * 1024 * 1024),
    )(table, *vectors[1:final], *rows_of[1:final])
    rates = rates_call(
        branches,
        final * depth,
        heads,
        padded,
        order,
        rows.reshape(blocks, parts, LANES),
        meta.reshape(blocks, parts, LANES),
        table,
        own,
        phi,
        spread_cells,
        vectors[final],
        rows_of[final],
    )
    rates = rates.reshape(heads * LANES)
    if heads * LANES == kept:
        return rates
    return lax.dynamic_slice_in_dim(rates, lax.axis_index("wa") * kept % LANES, kept, 0)


def solution(mesh):
    placed = (P(("pb", "wa"), None, None), P(("pb", "wa")), P(None, "pb"), P("pb"), P(), P())
    return jax.shard_map(
        body, mesh=mesh, in_specs=placed, out_specs=P(("pb", "wa")), check_vma=False
    )
```

```python
import functools
import math

import jax
import jax.numpy as jnp
from jax import lax
from jax.experimental import pallas as pl
from jax.experimental.pallas import tpu as pltpu
from jax.sharding import PartitionSpec as P


QMESH = 16
LANES = 128
SUB = 8
GROUPS = 4
SLOT = LANES // GROUPS
PARTS = 4
AHEAD = 2
DEPTH = 256

smearing = 0.5


def occupation(value):
    return 1.0 / (jnp.exp(value) - 1.0)


def row_iota(rows):
    return lax.broadcasted_iota(jnp.int32, (rows, LANES), 0)


def window(kept):
    return -(-(kept + LANES - math.gcd(kept, LANES)) // LANES)


def prepare(branches, local, kept, offset, *refs):
    pool, (rows_out, meta_out, order_out) = refs[:-3], refs[-3:]
    mine = lax.axis_index("pb")
    side = lax.rem(lax.axis_index("wa"), 2)
    start = lax.axis_index("wa") * kept
    lead = lax.rem(start, LANES)
    shards = lax.axis_size("pb")
    modes = jnp.concatenate([r[...].astype(jnp.int32) for r in pool], axis=0) + offset
    count = modes.shape[0]
    heading = (row_iota(count) & (PARTS - 1)) == 0
    safe = jnp.maximum(modes, 0)
    middle = safe.astype(jnp.float32) + 0.5
    owner = (middle * (1.0 / local)).astype(jnp.int32)
    point = (middle * (1.0 / branches)).astype(jnp.int32)
    near = owner ^ mine
    slot = near
    if shards == GROUPS:
        slot = jnp.where(near == 1, 1 + side, jnp.where(near == 2, 2 - side, near))
    inner = safe - owner * local
    depth = local // GROUPS
    group = ((inner.astype(jnp.float32) + 0.5) * (1.0 / depth)).astype(jnp.int32)
    rows_out[...] = (slot - group) * depth + inner
    following = pltpu.roll(modes, count - 1, 0)
    first = modes - start
    valid = heading & (following >= 0) & (first >= 0) & (first < kept)
    meta_out[...] = jnp.where(
        heading, jnp.where(valid, first + lead, -1), point + group * 65536
    )
    lanes = (((1,), (1,)), ((), ()))
    marks = lax.dot_general(
        jnp.ones((SUB, LANES), jnp.bfloat16),
        jnp.where(valid, 1.0, 0.0).astype(jnp.bfloat16),
        lanes,
        preferred_element_type=jnp.float32,
    )
    blocks = count // PARTS

    def index(rows, dim):
        return lax.broadcasted_iota(jnp.int32, (rows, blocks), dim)

    fold = jnp.where(index(count, 0) // PARTS == index(count, 1), 1.0, 0.0).astype(jnp.bfloat16)
    found = jnp.dot(marks.astype(jnp.bfloat16), fold, preferred_element_type=jnp.float32) > 0.5
    before = jnp.where(index(blocks, 0) <= index(blocks, 1), 1.0, 0.0).astype(jnp.bfloat16)
    rank = jnp.dot(
        jnp.where(found, 1.0, 0.0).astype(jnp.bfloat16), before, preferred_element_type=jnp.float32
    )
    spot = jnp.where(found, rank, 0.0)[0:1, :].astype(jnp.int32)
    chosen = jnp.where(index(blocks, 0) + 1 == spot, 1.0, 0.0).astype(jnp.bfloat16)
    number = index(SUB, 1)
    order = jnp.zeros((SUB, blocks), jnp.float32)
    for digit, scale in ((number & 15, 1.0), (number >> 4, 16.0)):
        order = order + scale * lax.dot_general(
            digit.astype(jnp.float32).astype(jnp.bfloat16),
            chosen,
            lanes,
            preferred_element_type=jnp.float32,
        )
    order_out[:, :blocks] = order[0:1, :].astype(jnp.int32)
    order_out[:, blocks:] = jnp.broadcast_to(rank[0:1, blocks - 1 :], (1, LANES)).astype(jnp.int32)


def shard_quarters(vectors, lines):
    depth = vectors.shape[1] // GROUPS

    def quarter(g):
        def chunk(t):
            at = g * depth + t * LANES
            row = at // LANES
            return vectors[:, at : at + LANES], lines[row : row + 1, :]

        return chunk

    return [quarter(g) for g in range(GROUPS)], depth


def fill_table(source, table, base):
    quarters, depth = source
    for t in range(depth // LANES):
        stack = []
        for quarter in quarters:
            vectors, line = quarter(t)
            stack.append(vectors.astype(jnp.float32))
            filler = SLOT - vectors.shape[0]
            stack.append(jnp.broadcast_to(line.astype(jnp.float32), (filler, LANES)))
        row = base + t * LANES
        table[row : row + LANES, :] = jnp.concatenate(stack, axis=0).T


def constants(phi_in, cells_in, phi, cells):
    phi[...] = phi_in[...]
    cell = cells_in[...]
    for j in range(cell.shape[1]):
        column = cell[:, j : j + 1]
        cells[j] = jnp.broadcast_to(column if j < 3 else -column, (cell.shape[0], LANES))


def begin(kept, heads, vectors, lines, table, own):
    comps = vectors.shape[0]
    fill_table(shard_quarters(vectors, lines), table, 0)
    start = lax.axis_index("wa") * kept // LANES
    own_lines = lines[...].astype(jnp.float32)
    line_rows = row_iota(own_lines.shape[0])
    parts = []
    for h in range(heads):
        at = pl.multiple_of((start + h) * LANES, LANES)
        parts.append(vectors[:, pl.ds(at, LANES)].astype(jnp.float32))
    for h in range(heads):
        parts.append(
            jnp.sum(jnp.where(line_rows == start + h, own_lines, 0.0), axis=0, keepdims=True)
        )
    filler = own.shape[0] - heads * comps - heads
    parts.append(jnp.zeros((filler, LANES), jnp.float32))
    own[...] = jnp.concatenate(parts, axis=0).astype(jnp.bfloat16)


def extend(slots, table_in, *refs):
    table = refs[-1]
    whole = len(slots)
    for n, slot in enumerate(slots):
        vectors, lines = refs[n], refs[whole + n]
        fill_table(shard_quarters(vectors, lines), table, slot * vectors.shape[1] // GROUPS)


def held_rows(e, branches):
    out = []
    for v in range(branches * branches // SUB):
        low, high = v * SUB // branches, (v * SUB + SUB - 1) // branches
        if low == high:
            out.append(jnp.broadcast_to(e[low : low + 1], (SUB, LANES)))
        else:
            cut = high * branches - v * SUB
            out.append(jnp.where(row_iota(SUB) < cut, e[low : low + 1], e[high : high + 1]))
    return out


def cycled_rows(e, branches):
    period = math.lcm(SUB, branches)
    twice = jnp.concatenate([e[:branches]] * (period // branches), axis=0)
    return [twice[v * SUB : (v + 1) * SUB] for v in range(period // SUB)]


def kernel(
    branches,
    base,
    order,
    rows_any,
    meta,
    table_in,
    own,
    phi,
    cells,
    vectors,
    lines,
    out,
    table,
    gathered_a,
    gathered_b,
    pair_a,
    pair_b,
    single_a,
    single_b,
    wide_a,
    wide_b,
    product_a,
    product_b,
    placed,
    place,
    acc,
    spots,
    sems,
):
    comps = 2 * branches
    pairs = branches * branches
    groups = pairs // SUB
    clusters = SUB
    heads = out.shape[0]
    log = QMESH.bit_length() - 1
    last = rows_any.shape[0] - 1
    count = order[0, last + 1]
    gathered, pair, single = (gathered_a, gathered_b), (pair_a, pair_b), (single_a, single_b)
    wide, product = (wide_a, wide_b), (product_a, product_b)

    def block_at(i):
        return order[0, jnp.clip(i, 0, last)]

    def load(i, p):
        return pltpu.make_async_copy(rows_any.at[block_at(i)], spots.at[p], sems.at[p])

    def gather(p):
        into = gathered[p]
        for which in range(3):
            for n in range(LANES):
                at = which * LANES + n
                into[at : at + 1, :] = table[pl.ds(spots[p, which + 1, n], 1), :]
                yield

    def one_hot(local):
        inside = local & (LANES - 1)
        return jnp.where(row_iota(LANES) == inside, 1.0, 0.0).astype(jnp.bfloat16)

    def choose(i, rows, pair_out, single_out):
        info = meta[block_at(i)]
        local = jnp.where(i < count, info[0:1, :], -1)
        head = lax.shift_right_arithmetic(local, 7)
        spread = jnp.dot(own[...], one_hot(local), preferred_element_type=jnp.float32)
        flats = [rows[w * LANES : (w + 1) * LANES, :].T for w in range(3)]
        yield
        shift = jnp.zeros((clusters, LANES), jnp.int32)
        for which in range(3):
            p = info[which + 1 : which + 2, :] & 0xFFFF
            coords = (
                lax.shift_right_logical(p, 2 * log),
                lax.shift_right_logical(p, log) & (QMESH - 1),
                p & (QMESH - 1),
            )
            for axis in range(3):
                shift = shift + cells[3 * which + axis] * coords[axis]
            yield
        angle = (shift & (QMESH - 1)).astype(jnp.float32) * (2.0 * math.pi / QMESH)
        single_out[0:SUB, :] = jnp.cos(angle)
        yield
        single_out[SUB : 2 * SUB, :] = jnp.sin(angle)
        yield
        others = []
        for which in range(3):
            group = lax.shift_right_logical(info[which + 1 : which + 2, :], 16)
            masks = [group == g for g in range(1, GROUPS)]
            pick = []
            for r in range(0, SLOT, SUB):
                value = flats[which][r : r + SUB]
                for g in range(1, GROUPS):
                    at = g * SLOT + r
                    value = jnp.where(masks[g - 1], flats[which][at : at + SUB], value)
                pick.append(value)
                yield
            others.append(jnp.concatenate(pick, axis=0))
        second, third, fourth = others
        third_re, third_im = held_rows(third, branches), held_rows(third[branches:], branches)
        fourth_re, fourth_im = cycled_rows(fourth, branches), cycled_rows(fourth[branches:], branches)
        period = len(fourth_re)
        for v in range(groups):
            are, aim, bre, bim = third_re[v], third_im[v], fourth_re[v % period], fourth_im[v % period]
            pair_out[v * SUB : (v + 1) * SUB, :] = are * bre - aim * bim
            at = pairs + v * SUB
            pair_out[at : at + SUB, :] = -(are * bim + aim * bre)
            yield
        at = 2 * SUB
        single_out[at : at + SLOT, :] = second
        first = jnp.zeros((comps, LANES), jnp.float32)
        for h in range(heads):
            first = jnp.where(head == h, spread[h * comps : (h + 1) * comps], first)
            yield
        tail = spread[heads * comps :]
        first_freq = jnp.sum(
            jnp.where(row_iota(tail.shape[0]) == head, tail, 0.0), axis=0, keepdims=True
        )
        at += SLOT
        single_out[at : at + comps, :] = first
        at += comps
        wanted = [first_freq] + [e[comps : comps + 1] for e in others]
        wanted.append(local.astype(jnp.float32))
        for n, line in enumerate(wanted):
            single_out[at + n : at + n + 1, :] = line
        yield

    def join(single_in, product_out):
        at = 2 * SUB
        second = single_in[at : at + comps, :]
        at += SLOT
        first = single_in[at : at + comps, :]
        at += comps
        f1, f2, f3, f4, local = (single_in[at + n : at + n + 1, :] for n in range(5))
        yield
        mismatch = f1 + f2 - f3 - f4
        delta = jnp.exp(-((mismatch / smearing) ** 2)) / (smearing * math.sqrt(math.pi))
        yield
        weight = (1.0 + occupation(f2)) * occupation(f3) * occupation(f4) / occupation(f1)
        yield
        at = 2 * pairs
        product_out[at : at + 1, :] = delta * weight / (f1 * f2 * f3 * f4)
        product_out[at + 1 : at + 2, :] = local
        yield
        first_re, first_im = held_rows(first, branches), held_rows(first[branches:], branches)
        second_re, second_im = cycled_rows(second, branches), cycled_rows(second[branches:], branches)
        period = len(second_re)
        for v in range(groups):
            are, aim, bre, bim = first_re[v], first_im[v], second_re[v % period], second_im[v % period]
            product_out[v * SUB : (v + 1) * SUB, :] = are * bre - aim * bim
            at = pairs + v * SUB
            product_out[at : at + SUB, :] = are * bim + aim * bre
            yield

    def turn(pair_in, single_in, wide_out):
        for k in range(clusters):
            cos_k, sin_k = single_in[k : k + 1, :], single_in[SUB + k : SUB + k + 1, :]
            for v in range(0, groups, 2):
                both = []
                for u in (v, v + 1):
                    re = pair_in[u * SUB : (u + 1) * SUB, :]
                    im = pair_in[pairs + u * SUB : pairs + (u + 1) * SUB, :]
                    both.append((cos_k * re - sin_k * im, cos_k * im + sin_k * re))
                at = k * pairs + v * SUB
                for part in range(2):
                    wide_out[at : at + 2 * SUB, part * LANES : (part + 1) * LANES] = jnp.concatenate(
                        [both[0][part], both[1][part]], axis=0
                    ).astype(jnp.bfloat16)
                yield

    def finish(i, weighted, product_in):
        sum_re = jnp.zeros((SUB, LANES), jnp.float32)
        sum_im = sum_re
        for v in range(groups):
            rows = slice(v * SUB, (v + 1) * SUB)
            nre = product_in[rows, :]
            nim = product_in[pairs + v * SUB : pairs + (v + 1) * SUB, :]
            wre, wim = weighted[rows, :LANES], weighted[rows, LANES:]
            sum_re = sum_re + (nre * wre - nim * wim)
            sum_im = sum_im + (nre * wim + nim * wre)
            yield
        value_re = jnp.sum(sum_re, axis=0, keepdims=True)
        value_im = jnp.sum(sum_im, axis=0, keepdims=True)
        yield
        at = 2 * pairs
        factor = product_in[at : at + 1, :]
        local = product_in[at + 1 : at + 2, :].astype(jnp.int32)
        local = jnp.where(i >= 0, local, -1)
        term = (value_re * value_re + value_im * value_im) * factor
        size = acc.shape[0]
        rest = jnp.where(row_iota(size) == lax.shift_right_arithmetic(local, 7), term, 0.0)
        place[0:1, :] = local
        yield
        for n in range(3):
            part = rest.astype(jnp.bfloat16)
            placed[n * size : (n + 1) * size, :] = part
            rest = rest - part.astype(jnp.float32)
        yield

    def run(*tracks):
        total_steps = max(n for _, n in tracks)
        done = [0] * len(tracks)
        for step in range(1, total_steps + 1):
            for t, (track, n) in enumerate(tracks):
                while done[t] * total_steps < step * n:
                    next(track, None)
                    done[t] += 1

    gather_steps = 3 * LANES
    choose_steps = 20 + groups + heads
    join_steps = 4 + groups
    turn_steps = clusters * groups // 2
    finish_steps = groups + 3

    def drain(*tracks):
        for track in tracks:
            for _ in track:
                pass

    pieces = [(at, min(at + DEPTH, clusters * pairs)) for at in range(0, clusters * pairs, DEPTH)]

    def multiply(wide_in, held):
        for low, high in pieces:
            part = jnp.dot(phi[:, low:high], wide_in[low:high, :], preferred_element_type=jnp.float32)
            held[:] = [part if not held else held[0] + part]
            yield

    def scatter():
        return lax.dot_general(
            placed[...],
            one_hot(place[0:1, :]),
            (((1,), (1,)), ((), ())),
            preferred_element_type=jnp.float32,
        )

    def add(sums):
        size = acc.shape[0]
        acc[...] += sums[:size] + sums[size : 2 * size] + sums[2 * size :]

    def step(i, p):
        load(i + 3, 1 - p).start()
        load(i + 2, p).wait()
        sums = scatter()
        weighted = []
        chosen = choose(i + 1, gathered[1 - p], pair[1 - p], single[1 - p])
        product_of = multiply(wide[1 - p], weighted)
        turned = turn(pair[p], single[p], wide[p])
        joined = join(single[p], product[p])
        rows = gather(p)
        run((product_of, len(pieces)), (turned, turn_steps), (rows, 240))
        drain(product_of)
        done = finish(i - 1, weighted[0], product[1 - p])
        run((chosen, choose_steps), (joined, join_steps), (done, finish_steps), (rows, gather_steps - 240))
        drain(chosen, turned, joined, rows, done)
        add(sums)

    def last_terms(p):
        sums = scatter()
        weighted = []
        drain(multiply(wide[1 - p], weighted))
        drain(finish(count - 1, weighted[0], product[1 - p]))
        add(sums)
        add(scatter())
        load(0, p).wait()

    load(0, 0).start()
    load(1, 1).start()
    acc[...] = jnp.zeros_like(acc)
    placed[...] = jnp.zeros_like(placed)
    place[...] = jnp.zeros_like(place)
    fill_table(shard_quarters(vectors, lines), table, base)
    load(0, 0).wait()
    drain(gather(0))
    load(2, 0).start()
    load(1, 1).wait()
    first, second = choose(0, gathered_a, pair_a, single_a), gather(1)
    run((first, choose_steps), (second, gather_steps))
    drain(first, second)

    def two_steps(j, carry):
        step(2 * j, 0)

        @pl.when(2 * j + 1 < count)
        def _():
            step(2 * j + 1, 1)

        return carry

    lax.fori_loop(0, lax.div(count + 1, 2), two_steps, 0)
    even = lax.rem(count, 2) == 0

    @pl.when(even)
    def _():
        last_terms(0)

    @pl.when(jnp.logical_not(even))
    def _():
        last_terms(1)

    out[...] = acc[:heads, :]


def rates_call(branches, base, heads, padded, *args):
    rows, table, phi = args[1], args[3], args[5]
    pairs = branches * branches
    singles = 2 * SUB + SLOT + 2 * branches + SUB
    vmem = pl.BlockSpec(memory_space=pltpu.VMEM)
    smem = pl.BlockSpec(memory_space=pltpu.SMEM)
    loose = pl.BlockSpec(memory_space=pl.ANY)
    rates, _ = pl.pallas_call(
        functools.partial(kernel, branches, base),
        out_shape=[
            jax.ShapeDtypeStruct((heads, LANES), jnp.float32),
            jax.ShapeDtypeStruct(table.shape, table.dtype),
        ],
        in_specs=[smem, loose] + [vmem] * 7,
        out_specs=[vmem, vmem],
        input_output_aliases={3: 1},
        scratch_shapes=[
            *[pltpu.VMEM((3 * LANES, LANES), jnp.float32)] * 2,
            *[pltpu.VMEM((2 * pairs, LANES), jnp.float32)] * 2,
            *[pltpu.VMEM((singles, LANES), jnp.float32)] * 2,
            *[pltpu.VMEM((phi.shape[1], 2 * LANES), jnp.bfloat16)] * 2,
            *[pltpu.VMEM((2 * pairs + SUB, LANES), jnp.float32)] * 2,
            pltpu.VMEM((3 * padded, LANES), jnp.bfloat16),
            pltpu.VMEM((SUB, LANES), jnp.int32),
            pltpu.VMEM((padded, LANES), jnp.float32),
            pltpu.SMEM((AHEAD, *rows.shape[1:]), jnp.int32),
            pltpu.SemaphoreType.DMA((AHEAD,)),
        ],
        compiler_params=pltpu.CompilerParams(vmem_limit_bytes=16 * 1024 * 1024),
    )(*args)
    return rates


def body(quartets, counts, eig, freq, phi, cells):
    comps, local = eig.shape
    branches = comps // 2
    shards = lax.axis_size("pb")
    workers = lax.axis_size("wa")
    held, parts, block = quartets.shape
    kept = local // workers
    heads = window(kept)
    clusters = cells.shape[0]
    offset = local * shards // 2
    both = ("pb", "wa")
    lines = freq.reshape(local // LANES, LANES)

    def swap(x):
        return lax.ppermute(x, "wa", [(i, i ^ 1) for i in range(workers)])

    def across(x, even, odd):
        pairs = []
        for p in range(shards):
            for w in range(workers):
                pairs.append((p * workers + w, (p ^ (odd if w % 2 else even)) * workers + w))
        return lax.ppermute(x, both, pairs)

    depth = local // GROUPS
    if shards == GROUPS:
        one = across(eig, 1, 2)
        far = across(one, 2, 1)
        vectors = [eig, one, swap(one), far]
        one_lines = across(lines, 1, 2)
        far_lines = across(lines, shards - 1, shards - 1)
        rows_of = [lines, one_lines, swap(one_lines), far_lines]
    else:
        vectors, rows_of = [eig], [lines]
        for k in range(1, shards):
            vectors.append(across(eig, k, k))
            rows_of.append(across(lines, k, k))

    slots = jnp.arange(held, dtype=jnp.int32)[:, None, None]
    coded = (jnp.where(slots < counts[:, None, None], quartets, -1) - offset).astype(jnp.int16)
    coded = coded.reshape(held * parts, block)
    line_up = [coded]
    for k in range(2, workers, 2):
        line_up.append(lax.ppermute(coded, "wa", [(i, i ^ k) for i in range(workers)]))
    column = jnp.concatenate(line_up, axis=0)
    other_column = swap(column)
    vmem = pl.BlockSpec(memory_space=pltpu.VMEM)
    smem = pl.BlockSpec(memory_space=pltpu.SMEM)
    hbm = pl.BlockSpec(memory_space=pl.ANY)
    far_space = pl.BlockSpec(memory_space=pltpu.HBM)
    total_rows = workers * held * parts
    rows, meta, order = pl.pallas_call(
        functools.partial(prepare, branches, local, kept, offset),
        out_shape=[
            jax.ShapeDtypeStruct((total_rows, LANES), jnp.int32),
            jax.ShapeDtypeStruct((total_rows, LANES), jnp.int32),
            jax.ShapeDtypeStruct((1, total_rows // parts + LANES), jnp.int32),
        ],
        in_specs=[vmem, vmem],
        out_specs=[vmem] * 3,
        compiler_params=pltpu.CompilerParams(vmem_limit_bytes=16 * 1024 * 1024),
    )(column, other_column)
    blocks = total_rows // parts
    padded = -(-heads // 16) * 16
    own_rows = -(-heads * (comps + 1) // 16) * 16
    phi, spread_cells = pl.pallas_call(
        constants,
        out_shape=[
            jax.ShapeDtypeStruct(phi.shape, phi.dtype),
            jax.ShapeDtypeStruct((cells.shape[1], clusters, LANES), jnp.int32),
        ],
        in_specs=[vmem] * 2,
        out_specs=[vmem] * 2,
        compiler_params=pltpu.CompilerParams(vmem_limit_bytes=16 * 1024 * 1024),
    )(phi, cells)
    table, own = pl.pallas_call(
        functools.partial(begin, kept, heads),
        out_shape=[
            jax.ShapeDtypeStruct((shards * depth, LANES), jnp.float32),
            jax.ShapeDtypeStruct((own_rows, LANES), jnp.bfloat16),
        ],
        in_specs=[vmem] * 2,
        out_specs=[vmem] * 2,
        compiler_params=pltpu.CompilerParams(vmem_limit_bytes=16 * 1024 * 1024),
    )(eig, lines)
    final = len(vectors) - 1
    whole = tuple(range(1, final))
    table = pl.pallas_call(
        functools.partial(extend, whole),
        out_shape=jax.ShapeDtypeStruct(table.shape, table.dtype),
        in_specs=[vmem] * (1 + 2 * len(whole)),
        out_specs=vmem,
        input_output_aliases={0: 0},
        compiler_params=pltpu.CompilerParams(vmem_limit_bytes=16 * 1024 * 1024),
    )(table, *vectors[1:final], *rows_of[1:final])
    rates = rates_call(
        branches,
        final * depth,
        heads,
        padded,
        order,
        rows.reshape(blocks, parts, LANES),
        meta.reshape(blocks, parts, LANES),
        table,
        own,
        phi,
        spread_cells,
        vectors[final],
        rows_of[final],
    )
    rates = rates.reshape(heads * LANES)
    if heads * LANES == kept:
        return rates
    return lax.dynamic_slice_in_dim(rates, lax.axis_index("wa") * kept % LANES, kept, 0)


def solution(mesh):
    placed = (P(("pb", "wa"), None, None), P(("pb", "wa")), P(None, "pb"), P("pb"), P(), P())
    return jax.shard_map(
        body, mesh=mesh, in_specs=placed, out_specs=P(("pb", "wa")), check_vma=False
    )
```

```python
import functools
import math

import jax
import jax.numpy as jnp
from jax import lax
from jax.experimental import pallas as pl
from jax.experimental.pallas import tpu as pltpu
from jax.sharding import PartitionSpec as P


QMESH = 16
LANES = 128
SUB = 8
GROUPS = 4
SLOT = LANES // GROUPS
PARTS = 4
AHEAD = 2
DEPTH = 256

smearing = 0.5


def occupation(value):
    return 1.0 / (jnp.exp(value) - 1.0)


def row_iota(rows):
    return lax.broadcasted_iota(jnp.int32, (rows, LANES), 0)


def window(kept):
    return -(-(kept + LANES - math.gcd(kept, LANES)) // LANES)


def prepare(branches, local, kept, offset, *refs):
    pool, (rows_out, meta_out, order_out) = refs[:-3], refs[-3:]
    mine = lax.axis_index("pb")
    side = lax.rem(lax.axis_index("wa"), 2)
    start = lax.axis_index("wa") * kept
    lead = lax.rem(start, LANES)
    shards = lax.axis_size("pb")
    modes = jnp.concatenate([r[...].astype(jnp.int32) for r in pool], axis=0) + offset
    count = modes.shape[0]
    heading = (row_iota(count) & (PARTS - 1)) == 0
    safe = jnp.maximum(modes, 0)
    middle = safe.astype(jnp.float32) + 0.5
    owner = (middle * (1.0 / local)).astype(jnp.int32)
    point = (middle * (1.0 / branches)).astype(jnp.int32)
    near = owner ^ mine
    slot = near
    if shards == GROUPS:
        slot = jnp.where(near == 1, 1 + side, jnp.where(near == 2, 2 - side, near))
    inner = safe - owner * local
    depth = local // GROUPS
    group = ((inner.astype(jnp.float32) + 0.5) * (1.0 / depth)).astype(jnp.int32)
    rows_out[...] = (slot - group) * depth + inner
    following = pltpu.roll(modes, count - 1, 0)
    first = modes - start
    valid = heading & (following >= 0) & (first >= 0) & (first < kept)
    meta_out[...] = jnp.where(
        heading, jnp.where(valid, first + lead, -1), point + group * 65536
    )
    lanes = (((1,), (1,)), ((), ()))
    marks = lax.dot_general(
        jnp.ones((SUB, LANES), jnp.bfloat16),
        jnp.where(valid, 1.0, 0.0).astype(jnp.bfloat16),
        lanes,
        preferred_element_type=jnp.float32,
    )
    blocks = count // PARTS

    def index(rows, dim):
        return lax.broadcasted_iota(jnp.int32, (rows, blocks), dim)

    fold = jnp.where(index(count, 0) // PARTS == index(count, 1), 1.0, 0.0).astype(jnp.bfloat16)
    found = jnp.dot(marks.astype(jnp.bfloat16), fold, preferred_element_type=jnp.float32) > 0.5
    before = jnp.where(index(blocks, 0) <= index(blocks, 1), 1.0, 0.0).astype(jnp.bfloat16)
    rank = jnp.dot(
        jnp.where(found, 1.0, 0.0).astype(jnp.bfloat16), before, preferred_element_type=jnp.float32
    )
    spot = jnp.where(found, rank, 0.0)[0:1, :].astype(jnp.int32)
    chosen = jnp.where(index(blocks, 0) + 1 == spot, 1.0, 0.0).astype(jnp.bfloat16)
    number = index(SUB, 1)
    order = jnp.zeros((SUB, blocks), jnp.float32)
    for digit, scale in ((number & 15, 1.0), (number >> 4, 16.0)):
        order = order + scale * lax.dot_general(
            digit.astype(jnp.float32).astype(jnp.bfloat16),
            chosen,
            lanes,
            preferred_element_type=jnp.float32,
        )
    order_out[:, :blocks] = order[0:1, :].astype(jnp.int32)
    order_out[:, blocks:] = jnp.broadcast_to(rank[0:1, blocks - 1 :], (1, LANES)).astype(jnp.int32)


def shard_quarters(vectors, lines):
    depth = vectors.shape[1] // GROUPS

    def quarter(g):
        def chunk(t):
            at = g * depth + t * LANES
            row = at // LANES
            return vectors[:, at : at + LANES], lines[row : row + 1, :]

        return chunk

    return [quarter(g) for g in range(GROUPS)], depth


def fill_table(source, table, base):
    quarters, depth = source
    for t in range(depth // LANES):
        stack = []
        for quarter in quarters:
            vectors, line = quarter(t)
            stack.append(vectors.astype(jnp.float32))
            filler = SLOT - vectors.shape[0]
            stack.append(jnp.broadcast_to(line.astype(jnp.float32), (filler, LANES)))
        row = base + t * LANES
        table[row : row + LANES, :] = jnp.concatenate(stack, axis=0).T


def constants(phi_in, cells_in, phi, cells):
    phi[...] = phi_in[...]
    cell = cells_in[...]
    for j in range(cell.shape[1]):
        column = cell[:, j : j + 1]
        cells[j] = jnp.broadcast_to(column if j < 3 else -column, (cell.shape[0], LANES))


def begin(kept, heads, vectors, lines, table, own):
    comps = vectors.shape[0]
    fill_table(shard_quarters(vectors, lines), table, 0)
    start = lax.axis_index("wa") * kept // LANES
    own_lines = lines[...].astype(jnp.float32)
    line_rows = row_iota(own_lines.shape[0])
    parts = []
    for h in range(heads):
        at = pl.multiple_of((start + h) * LANES, LANES)
        parts.append(vectors[:, pl.ds(at, LANES)].astype(jnp.float32))
    for h in range(heads):
        parts.append(
            jnp.sum(jnp.where(line_rows == start + h, own_lines, 0.0), axis=0, keepdims=True)
        )
    filler = own.shape[0] - heads * comps - heads
    parts.append(jnp.zeros((filler, LANES), jnp.float32))
    own[...] = jnp.concatenate(parts, axis=0).astype(jnp.bfloat16)


def extend(slots, table_in, *refs):
    table = refs[-1]
    whole = len(slots)
    for n, slot in enumerate(slots):
        vectors, lines = refs[n], refs[whole + n]
        fill_table(shard_quarters(vectors, lines), table, slot * vectors.shape[1] // GROUPS)


def held_rows(e, branches):
    out = []
    for v in range(branches * branches // SUB):
        low, high = v * SUB // branches, (v * SUB + SUB - 1) // branches
        if low == high:
            out.append(jnp.broadcast_to(e[low : low + 1], (SUB, LANES)))
        else:
            cut = high * branches - v * SUB
            out.append(jnp.where(row_iota(SUB) < cut, e[low : low + 1], e[high : high + 1]))
    return out


def cycled_rows(e, branches):
    period = math.lcm(SUB, branches)
    twice = jnp.concatenate([e[:branches]] * (period // branches), axis=0)
    return [twice[v * SUB : (v + 1) * SUB] for v in range(period // SUB)]


def kernel(
    branches,
    base,
    order,
    rows_any,
    meta,
    table_in,
    own,
    phi,
    cells,
    vectors,
    lines,
    out,
    table,
    gathered_a,
    gathered_b,
    pair_a,
    pair_b,
    single_a,
    single_b,
    wide_a,
    wide_b,
    product_a,
    product_b,
    result_a,
    result_b,
    placed,
    place,
    acc,
    spots,
    sems,
):
    comps = 2 * branches
    pairs = branches * branches
    groups = pairs // SUB
    clusters = SUB
    heads = out.shape[0]
    log = QMESH.bit_length() - 1
    last = rows_any.shape[0] - 1
    count = order[0, last + 1]
    gathered, pair, single = (gathered_a, gathered_b), (pair_a, pair_b), (single_a, single_b)
    wide, product = (wide_a, wide_b), (product_a, product_b)
    result = (result_a, result_b)

    def block_at(i):
        return order[0, jnp.clip(i, 0, last)]

    def load(i, p):
        return pltpu.make_async_copy(rows_any.at[block_at(i)], spots.at[p], sems.at[p])

    def gather(p):
        into = gathered[p]
        for which in range(3):
            for n in range(LANES):
                at = which * LANES + n
                into[at : at + 1, :] = table[pl.ds(spots[p, which + 1, n], 1), :]
                yield

    def one_hot(local):
        inside = local & (LANES - 1)
        return jnp.where(row_iota(LANES) == inside, 1.0, 0.0).astype(jnp.bfloat16)

    def choose(i, rows, pair_out, single_out):
        info = meta[block_at(i)]
        local = jnp.where(i < count, info[0:1, :], -1)
        head = lax.shift_right_arithmetic(local, 7)
        spread = jnp.dot(own[...], one_hot(local), preferred_element_type=jnp.float32)
        flats = [rows[w * LANES : (w + 1) * LANES, :].T for w in range(3)]
        yield
        shift = jnp.zeros((clusters, LANES), jnp.int32)
        for which in range(3):
            p = info[which + 1 : which + 2, :] & 0xFFFF
            coords = (
                lax.shift_right_logical(p, 2 * log),
                lax.shift_right_logical(p, log) & (QMESH - 1),
                p & (QMESH - 1),
            )
            for axis in range(3):
                shift = shift + cells[3 * which + axis] * coords[axis]
            yield
        angle = (shift & (QMESH - 1)).astype(jnp.float32) * (2.0 * math.pi / QMESH)
        single_out[0:SUB, :] = jnp.cos(angle)
        yield
        single_out[SUB : 2 * SUB, :] = jnp.sin(angle)
        yield
        others = []
        for which in range(3):
            group = lax.shift_right_logical(info[which + 1 : which + 2, :], 16)
            masks = [group == g for g in range(1, GROUPS)]
            pick = []
            for r in range(0, SLOT, SUB):
                value = flats[which][r : r + SUB]
                for g in range(1, GROUPS):
                    at = g * SLOT + r
                    value = jnp.where(masks[g - 1], flats[which][at : at + SUB], value)
                pick.append(value)
                yield
            others.append(jnp.concatenate(pick, axis=0))
        second, third, fourth = others
        third_re, third_im = held_rows(third, branches), held_rows(third[branches:], branches)
        fourth_re, fourth_im = cycled_rows(fourth, branches), cycled_rows(fourth[branches:], branches)
        period = len(fourth_re)
        for v in range(groups):
            are, aim, bre, bim = third_re[v], third_im[v], fourth_re[v % period], fourth_im[v % period]
            pair_out[v * SUB : (v + 1) * SUB, :] = are * bre - aim * bim
            at = pairs + v * SUB
            pair_out[at : at + SUB, :] = -(are * bim + aim * bre)
            yield
        at = 2 * SUB
        single_out[at : at + SLOT, :] = second
        first = jnp.zeros((comps, LANES), jnp.float32)
        for h in range(heads):
            first = jnp.where(head == h, spread[h * comps : (h + 1) * comps], first)
            yield
        tail = spread[heads * comps :]
        first_freq = jnp.sum(
            jnp.where(row_iota(tail.shape[0]) == head, tail, 0.0), axis=0, keepdims=True
        )
        at += SLOT
        single_out[at : at + comps, :] = first
        at += comps
        wanted = [first_freq] + [e[comps : comps + 1] for e in others]
        wanted.append(local.astype(jnp.float32))
        for n, line in enumerate(wanted):
            single_out[at + n : at + n + 1, :] = line
        yield

    def join(single_in, product_out):
        at = 2 * SUB
        second = single_in[at : at + comps, :]
        at += SLOT
        first = single_in[at : at + comps, :]
        at += comps
        f1, f2, f3, f4, local = (single_in[at + n : at + n + 1, :] for n in range(5))
        yield
        mismatch = f1 + f2 - f3 - f4
        delta = jnp.exp(-((mismatch / smearing) ** 2)) / (smearing * math.sqrt(math.pi))
        yield
        weight = (1.0 + occupation(f2)) * occupation(f3) * occupation(f4) / occupation(f1)
        yield
        at = 2 * pairs
        product_out[at : at + 1, :] = delta * weight / (f1 * f2 * f3 * f4)
        product_out[at + 1 : at + 2, :] = local
        yield
        first_re, first_im = held_rows(first, branches), held_rows(first[branches:], branches)
        second_re, second_im = cycled_rows(second, branches), cycled_rows(second[branches:], branches)
        period = len(second_re)
        for v in range(groups):
            are, aim, bre, bim = first_re[v], first_im[v], second_re[v % period], second_im[v % period]
            product_out[v * SUB : (v + 1) * SUB, :] = are * bre - aim * bim
            at = pairs + v * SUB
            product_out[at : at + SUB, :] = are * bim + aim * bre
            yield

    def turn(pair_in, single_in, wide_out):
        for k in range(clusters):
            cos_k, sin_k = single_in[k : k + 1, :], single_in[SUB + k : SUB + k + 1, :]
            for v in range(0, groups, 2):
                both = []
                for u in (v, v + 1):
                    re = pair_in[u * SUB : (u + 1) * SUB, :]
                    im = pair_in[pairs + u * SUB : pairs + (u + 1) * SUB, :]
                    both.append((cos_k * re - sin_k * im, cos_k * im + sin_k * re))
                at = k * pairs + v * SUB
                for part in range(2):
                    wide_out[at : at + 2 * SUB, part * LANES : (part + 1) * LANES] = jnp.concatenate(
                        [both[0][part], both[1][part]], axis=0
                    ).astype(jnp.bfloat16)
                yield

    def finish(i, result_in, product_in):
        sum_re = jnp.zeros((SUB, LANES), jnp.float32)
        sum_im = sum_re
        for v in range(groups):
            rows = slice(v * SUB, (v + 1) * SUB)
            nre = product_in[rows, :]
            nim = product_in[pairs + v * SUB : pairs + (v + 1) * SUB, :]
            wre, wim = result_in[rows, :LANES], result_in[rows, LANES:]
            sum_re = sum_re + (nre * wre - nim * wim)
            sum_im = sum_im + (nre * wim + nim * wre)
            yield
        value_re = jnp.sum(sum_re, axis=0, keepdims=True)
        value_im = jnp.sum(sum_im, axis=0, keepdims=True)
        yield
        at = 2 * pairs
        factor = product_in[at : at + 1, :]
        local = product_in[at + 1 : at + 2, :].astype(jnp.int32)
        local = jnp.where(i >= 0, local, -1)
        term = (value_re * value_re + value_im * value_im) * factor
        size = acc.shape[0]
        rest = jnp.where(row_iota(size) == lax.shift_right_arithmetic(local, 7), term, 0.0)
        place[0:1, :] = local
        yield
        for n in range(3):
            part = rest.astype(jnp.bfloat16)
            placed[n * size : (n + 1) * size, :] = part
            rest = rest - part.astype(jnp.float32)
        yield

    def run(*tracks):
        total_steps = max(n for _, n in tracks)
        done = [0] * len(tracks)
        for step in range(1, total_steps + 1):
            for t, (track, n) in enumerate(tracks):
                while done[t] * total_steps < step * n:
                    next(track, None)
                    done[t] += 1

    gather_steps = 3 * LANES
    choose_steps = 20 + groups + heads
    join_steps = 4 + groups
    turn_steps = clusters * groups // 2
    finish_steps = groups + 3

    def drain(*tracks):
        for track in tracks:
            for _ in track:
                pass

    pieces = [(at, min(at + DEPTH, clusters * pairs)) for at in range(0, clusters * pairs, DEPTH)]

    def multiply(wide_in, result_out):
        whole = None
        for low, high in pieces:
            part = jnp.dot(phi[:, low:high], wide_in[low:high, :], preferred_element_type=jnp.float32)
            whole = part if whole is None else whole + part
            yield
        result_out[...] = whole
        yield

    def scatter():
        return lax.dot_general(
            placed[...],
            one_hot(place[0:1, :]),
            (((1,), (1,)), ((), ())),
            preferred_element_type=jnp.float32,
        )

    def add(sums):
        size = acc.shape[0]
        acc[...] += sums[:size] + sums[size : 2 * size] + sums[2 * size :]

    def step(i, p):
        load(i + 3, 1 - p).start()
        load(i + 2, p).wait()
        sums = scatter()
        joined = join(single[1 - p], product[1 - p])
        next(joined)
        chosen = choose(i + 1, gathered[1 - p], pair[1 - p], single[1 - p])
        multiplied = multiply(wide[1 - p], result[1 - p])
        turned = turn(pair[p], single[p], wide[p])
        done = finish(i - 2, result[p], product[p])
        rows = gather(p)
        run(
            (multiplied, len(pieces) + 1),
            (done, finish_steps),
            (chosen, choose_steps),
            (turned, turn_steps),
            (joined, join_steps),
            (rows, gather_steps),
        )
        drain(multiplied, done, chosen, turned, joined, rows)
        add(sums)

    def last_terms(p):
        sums = scatter()
        drain(join(single[1 - p], product[1 - p]), multiply(wide[1 - p], result[1 - p]))
        drain(finish(count - 2, result[p], product[p]))
        add(sums)
        add(scatter())
        drain(finish(count - 1, result[1 - p], product[1 - p]))
        add(scatter())
        load(0, p).wait()

    load(0, 0).start()
    load(1, 1).start()
    acc[...] = jnp.zeros_like(acc)
    placed[...] = jnp.zeros_like(placed)
    place[...] = jnp.zeros_like(place)
    fill_table(shard_quarters(vectors, lines), table, base)
    load(0, 0).wait()
    drain(gather(0))
    load(2, 0).start()
    load(1, 1).wait()
    first, second = choose(0, gathered_a, pair_a, single_a), gather(1)
    run((first, choose_steps), (second, gather_steps))
    drain(first, second)

    def two_steps(j, carry):
        step(2 * j, 0)

        @pl.when(2 * j + 1 < count)
        def _():
            step(2 * j + 1, 1)

        return carry

    lax.fori_loop(0, lax.div(count + 1, 2), two_steps, 0)
    even = lax.rem(count, 2) == 0

    @pl.when(even)
    def _():
        last_terms(0)

    @pl.when(jnp.logical_not(even))
    def _():
        last_terms(1)

    out[...] = acc[:heads, :]


def rates_call(branches, base, heads, padded, *args):
    rows, table, phi = args[1], args[3], args[5]
    pairs = branches * branches
    singles = 2 * SUB + SLOT + 2 * branches + SUB
    vmem = pl.BlockSpec(memory_space=pltpu.VMEM)
    smem = pl.BlockSpec(memory_space=pltpu.SMEM)
    loose = pl.BlockSpec(memory_space=pl.ANY)
    rates, _ = pl.pallas_call(
        functools.partial(kernel, branches, base),
        out_shape=[
            jax.ShapeDtypeStruct((heads, LANES), jnp.float32),
            jax.ShapeDtypeStruct(table.shape, table.dtype),
        ],
        in_specs=[smem, loose] + [vmem] * 7,
        out_specs=[vmem, vmem],
        input_output_aliases={3: 1},
        scratch_shapes=[
            *[pltpu.VMEM((3 * LANES, LANES), jnp.float32)] * 2,
            *[pltpu.VMEM((2 * pairs, LANES), jnp.float32)] * 2,
            *[pltpu.VMEM((singles, LANES), jnp.float32)] * 2,
            *[pltpu.VMEM((phi.shape[1], 2 * LANES), jnp.bfloat16)] * 2,
            *[pltpu.VMEM((2 * pairs + SUB, LANES), jnp.float32)] * 2,
            *[pltpu.VMEM((pairs, 2 * LANES), jnp.float32)] * 2,
            pltpu.VMEM((3 * padded, LANES), jnp.bfloat16),
            pltpu.VMEM((SUB, LANES), jnp.int32),
            pltpu.VMEM((padded, LANES), jnp.float32),
            pltpu.SMEM((AHEAD, *rows.shape[1:]), jnp.int32),
            pltpu.SemaphoreType.DMA((AHEAD,)),
        ],
        compiler_params=pltpu.CompilerParams(vmem_limit_bytes=16 * 1024 * 1024),
    )(*args)
    return rates


def body(quartets, counts, eig, freq, phi, cells):
    comps, local = eig.shape
    branches = comps // 2
    shards = lax.axis_size("pb")
    workers = lax.axis_size("wa")
    held, parts, block = quartets.shape
    kept = local // workers
    heads = window(kept)
    clusters = cells.shape[0]
    offset = local * shards // 2
    both = ("pb", "wa")
    lines = freq.reshape(local // LANES, LANES)

    def swap(x):
        return lax.ppermute(x, "wa", [(i, i ^ 1) for i in range(workers)])

    def across(x, even, odd):
        pairs = []
        for p in range(shards):
            for w in range(workers):
                pairs.append((p * workers + w, (p ^ (odd if w % 2 else even)) * workers + w))
        return lax.ppermute(x, both, pairs)

    depth = local // GROUPS
    if shards == GROUPS:
        one = across(eig, 1, 2)
        far = across(one, 2, 1)
        vectors = [eig, one, swap(one), far]
        one_lines = across(lines, 1, 2)
        far_lines = across(lines, shards - 1, shards - 1)
        rows_of = [lines, one_lines, swap(one_lines), far_lines]
    else:
        vectors, rows_of = [eig], [lines]
        for k in range(1, shards):
            vectors.append(across(eig, k, k))
            rows_of.append(across(lines, k, k))

    slots = jnp.arange(held, dtype=jnp.int32)[:, None, None]
    coded = (jnp.where(slots < counts[:, None, None], quartets, -1) - offset).astype(jnp.int16)
    coded = coded.reshape(held * parts, block)
    line_up = [coded]
    for k in range(2, workers, 2):
        line_up.append(lax.ppermute(coded, "wa", [(i, i ^ k) for i in range(workers)]))
    column = jnp.concatenate(line_up, axis=0)
    other_column = swap(column)
    vmem = pl.BlockSpec(memory_space=pltpu.VMEM)
    smem = pl.BlockSpec(memory_space=pltpu.SMEM)
    hbm = pl.BlockSpec(memory_space=pl.ANY)
    far_space = pl.BlockSpec(memory_space=pltpu.HBM)
    total_rows = workers * held * parts
    rows, meta, order = pl.pallas_call(
        functools.partial(prepare, branches, local, kept, offset),
        out_shape=[
            jax.ShapeDtypeStruct((total_rows, LANES), jnp.int32),
            jax.ShapeDtypeStruct((total_rows, LANES), jnp.int32),
            jax.ShapeDtypeStruct((1, total_rows // parts + LANES), jnp.int32),
        ],
        in_specs=[vmem, vmem],
        out_specs=[vmem] * 3,
        compiler_params=pltpu.CompilerParams(vmem_limit_bytes=16 * 1024 * 1024),
    )(column, other_column)
    blocks = total_rows // parts
    padded = -(-heads // 16) * 16
    own_rows = -(-heads * (comps + 1) // 16) * 16
    phi, spread_cells = pl.pallas_call(
        constants,
        out_shape=[
            jax.ShapeDtypeStruct(phi.shape, phi.dtype),
            jax.ShapeDtypeStruct((cells.shape[1], clusters, LANES), jnp.int32),
        ],
        in_specs=[vmem] * 2,
        out_specs=[vmem] * 2,
        compiler_params=pltpu.CompilerParams(vmem_limit_bytes=16 * 1024 * 1024),
    )(phi, cells)
    table, own = pl.pallas_call(
        functools.partial(begin, kept, heads),
        out_shape=[
            jax.ShapeDtypeStruct((shards * depth, LANES), jnp.float32),
            jax.ShapeDtypeStruct((own_rows, LANES), jnp.bfloat16),
        ],
        in_specs=[vmem] * 2,
        out_specs=[vmem] * 2,
        compiler_params=pltpu.CompilerParams(vmem_limit_bytes=16 * 1024 * 1024),
    )(eig, lines)
    final = len(vectors) - 1
    whole = tuple(range(1, final))
    table = pl.pallas_call(
        functools.partial(extend, whole),
        out_shape=jax.ShapeDtypeStruct(table.shape, table.dtype),
        in_specs=[vmem] * (1 + 2 * len(whole)),
        out_specs=vmem,
        input_output_aliases={0: 0},
        compiler_params=pltpu.CompilerParams(vmem_limit_bytes=16 * 1024 * 1024),
    )(table, *vectors[1:final], *rows_of[1:final])
    rates = rates_call(
        branches,
        final * depth,
        heads,
        padded,
        order,
        rows.reshape(blocks, parts, LANES),
        meta.reshape(blocks, parts, LANES),
        table,
        own,
        phi,
        spread_cells,
        vectors[final],
        rows_of[final],
    )
    rates = rates.reshape(heads * LANES)
    if heads * LANES == kept:
        return rates
    return lax.dynamic_slice_in_dim(rates, lax.axis_index("wa") * kept % LANES, kept, 0)


def solution(mesh):
    placed = (P(("pb", "wa"), None, None), P(("pb", "wa")), P(None, "pb"), P("pb"), P(), P())
    return jax.shard_map(
        body, mesh=mesh, in_specs=placed, out_specs=P(("pb", "wa")), check_vma=False
    )
```

```python
import functools
import math

import jax
import jax.numpy as jnp
from jax import lax
from jax.experimental import pallas as pl
from jax.experimental.pallas import tpu as pltpu
from jax.sharding import PartitionSpec as P


QMESH = 16
LANES = 128
SUB = 8
GROUPS = 4
SLOT = LANES // GROUPS
PARTS = 4
AHEAD = 4
DEPTH = 256

smearing = 0.5


def occupation(value):
    return 1.0 / (jnp.exp(value) - 1.0)


def row_iota(rows):
    return lax.broadcasted_iota(jnp.int32, (rows, LANES), 0)


def window(kept):
    return -(-(kept + LANES - math.gcd(kept, LANES)) // LANES)


def prepare(branches, local, kept, offset, *refs):
    pool, (rows_out, meta_out, order_out) = refs[:-3], refs[-3:]
    mine = lax.axis_index("pb")
    side = lax.rem(lax.axis_index("wa"), 2)
    start = lax.axis_index("wa") * kept
    lead = lax.rem(start, LANES)
    shards = lax.axis_size("pb")
    modes = jnp.concatenate([r[...].astype(jnp.int32) for r in pool], axis=0) + offset
    count = modes.shape[0]
    heading = (row_iota(count) & (PARTS - 1)) == 0
    safe = jnp.maximum(modes, 0)
    middle = safe.astype(jnp.float32) + 0.5
    owner = (middle * (1.0 / local)).astype(jnp.int32)
    point = (middle * (1.0 / branches)).astype(jnp.int32)
    near = owner ^ mine
    slot = near
    if shards == GROUPS:
        slot = jnp.where(near == 1, 1 + side, jnp.where(near == 2, 2 - side, near))
    inner = safe - owner * local
    depth = local // GROUPS
    group = ((inner.astype(jnp.float32) + 0.5) * (1.0 / depth)).astype(jnp.int32)
    rows_out[...] = (slot - group) * depth + inner
    following = pltpu.roll(modes, count - 1, 0)
    first = modes - start
    valid = heading & (following >= 0) & (first >= 0) & (first < kept)
    meta_out[...] = jnp.where(
        heading, jnp.where(valid, first + lead, -1), point + group * 65536
    )
    lanes = (((1,), (1,)), ((), ()))
    marks = lax.dot_general(
        jnp.ones((SUB, LANES), jnp.bfloat16),
        jnp.where(valid, 1.0, 0.0).astype(jnp.bfloat16),
        lanes,
        preferred_element_type=jnp.float32,
    )
    blocks = count // PARTS

    def index(rows, dim):
        return lax.broadcasted_iota(jnp.int32, (rows, blocks), dim)

    fold = jnp.where(index(count, 0) // PARTS == index(count, 1), 1.0, 0.0).astype(jnp.bfloat16)
    found = jnp.dot(marks.astype(jnp.bfloat16), fold, preferred_element_type=jnp.float32) > 0.5
    before = jnp.where(index(blocks, 0) <= index(blocks, 1), 1.0, 0.0).astype(jnp.bfloat16)
    rank = jnp.dot(
        jnp.where(found, 1.0, 0.0).astype(jnp.bfloat16), before, preferred_element_type=jnp.float32
    )
    spot = jnp.where(found, rank, 0.0)[0:1, :].astype(jnp.int32)
    chosen = jnp.where(index(blocks, 0) + 1 == spot, 1.0, 0.0).astype(jnp.bfloat16)
    number = index(SUB, 1)
    order = jnp.zeros((SUB, blocks), jnp.float32)
    for digit, scale in ((number & 15, 1.0), (number >> 4, 16.0)):
        order = order + scale * lax.dot_general(
            digit.astype(jnp.float32).astype(jnp.bfloat16),
            chosen,
            lanes,
            preferred_element_type=jnp.float32,
        )
    order_out[:, :blocks] = order[0:1, :].astype(jnp.int32)
    order_out[:, blocks:] = jnp.broadcast_to(rank[0:1, blocks - 1 :], (1, LANES)).astype(jnp.int32)


def shard_quarters(vectors, lines):
    depth = vectors.shape[1] // GROUPS

    def quarter(g):
        def chunk(t):
            at = g * depth + t * LANES
            row = at // LANES
            return vectors[:, at : at + LANES], lines[row : row + 1, :]

        return chunk

    return [quarter(g) for g in range(GROUPS)], depth


def fill_table(source, table, base):
    quarters, depth = source
    for t in range(depth // LANES):
        stack = []
        for quarter in quarters:
            vectors, line = quarter(t)
            stack.append(vectors.astype(jnp.float32))
            filler = SLOT - vectors.shape[0]
            stack.append(jnp.broadcast_to(line.astype(jnp.float32), (filler, LANES)))
        row = base + t * LANES
        table[row : row + LANES, :] = jnp.concatenate(stack, axis=0).T


def constants(phi_in, cells_in, phi, cells):
    phi[...] = phi_in[...]
    cell = cells_in[...]
    for j in range(cell.shape[1]):
        column = cell[:, j : j + 1]
        cells[j] = jnp.broadcast_to(column if j < 3 else -column, (cell.shape[0], LANES))


def begin(kept, heads, vectors, lines, table, own):
    comps = vectors.shape[0]
    fill_table(shard_quarters(vectors, lines), table, 0)
    start = lax.axis_index("wa") * kept // LANES
    own_lines = lines[...].astype(jnp.float32)
    line_rows = row_iota(own_lines.shape[0])
    parts = []
    for h in range(heads):
        at = pl.multiple_of((start + h) * LANES, LANES)
        parts.append(vectors[:, pl.ds(at, LANES)].astype(jnp.float32))
    for h in range(heads):
        parts.append(
            jnp.sum(jnp.where(line_rows == start + h, own_lines, 0.0), axis=0, keepdims=True)
        )
    filler = own.shape[0] - heads * comps - heads
    parts.append(jnp.zeros((filler, LANES), jnp.float32))
    own[...] = jnp.concatenate(parts, axis=0).astype(jnp.bfloat16)


def extend(slots, table_in, *refs):
    table = refs[-1]
    whole = len(slots)
    for n, slot in enumerate(slots):
        vectors, lines = refs[n], refs[whole + n]
        fill_table(shard_quarters(vectors, lines), table, slot * vectors.shape[1] // GROUPS)


def held_rows(e, branches):
    out = []
    for v in range(branches * branches // SUB):
        low, high = v * SUB // branches, (v * SUB + SUB - 1) // branches
        if low == high:
            out.append(jnp.broadcast_to(e[low : low + 1], (SUB, LANES)))
        else:
            cut = high * branches - v * SUB
            out.append(jnp.where(row_iota(SUB) < cut, e[low : low + 1], e[high : high + 1]))
    return out


def cycled_rows(e, branches):
    period = math.lcm(SUB, branches)
    twice = jnp.concatenate([e[:branches]] * (period // branches), axis=0)
    return [twice[v * SUB : (v + 1) * SUB] for v in range(period // SUB)]


def kernel(
    branches,
    base,
    order,
    rows_any,
    meta,
    table_in,
    own,
    phi,
    cells,
    vectors,
    lines,
    out,
    table,
    gathered_a,
    gathered_b,
    pair_a,
    pair_b,
    single_a,
    single_b,
    wide_a,
    wide_b,
    product_a,
    product_b,
    result_a,
    result_b,
    placed,
    place,
    acc,
    spots,
    sems,
):
    comps = 2 * branches
    pairs = branches * branches
    groups = pairs // SUB
    clusters = SUB
    heads = out.shape[0]
    log = QMESH.bit_length() - 1
    last = rows_any.shape[0] - 1
    count = order[0, last + 1]
    gathered, pair, single = (gathered_a, gathered_b), (pair_a, pair_b), (single_a, single_b)
    wide, product = (wide_a, wide_b), (product_a, product_b)
    result = (result_a, result_b)

    def block_at(i):
        return order[0, jnp.clip(i, 0, last)]

    def load(i, slot):
        return pltpu.make_async_copy(rows_any.at[block_at(i)], spots.at[slot], sems.at[slot])

    def gather(slot):
        into = gathered[slot % 2]
        for which in range(3):
            for n in range(LANES):
                at = which * LANES + n
                into[at : at + 1, :] = table[pl.ds(spots[slot, which + 1, n], 1), :]
                yield

    def one_hot(local):
        inside = local & (LANES - 1)
        return jnp.where(row_iota(LANES) == inside, 1.0, 0.0).astype(jnp.bfloat16)

    def choose(i, rows, pair_out, single_out):
        info = meta[block_at(i)]
        local = jnp.where(i < count, info[0:1, :], -1)
        head = lax.shift_right_arithmetic(local, 7)
        spread = jnp.dot(own[...], one_hot(local), preferred_element_type=jnp.float32)
        flats = [rows[w * LANES : (w + 1) * LANES, :].T for w in range(3)]
        yield
        shift = jnp.zeros((clusters, LANES), jnp.int32)
        for which in range(3):
            p = info[which + 1 : which + 2, :] & 0xFFFF
            coords = (
                lax.shift_right_logical(p, 2 * log),
                lax.shift_right_logical(p, log) & (QMESH - 1),
                p & (QMESH - 1),
            )
            for axis in range(3):
                shift = shift + cells[3 * which + axis] * coords[axis]
            yield
        angle = (shift & (QMESH - 1)).astype(jnp.float32) * (2.0 * math.pi / QMESH)
        single_out[0:SUB, :] = jnp.cos(angle)
        yield
        single_out[SUB : 2 * SUB, :] = jnp.sin(angle)
        yield
        others = []
        for which in range(3):
            group = lax.shift_right_logical(info[which + 1 : which + 2, :], 16)
            masks = [group == g for g in range(1, GROUPS)]
            pick = []
            for r in range(0, SLOT, SUB):
                value = flats[which][r : r + SUB]
                for g in range(1, GROUPS):
                    at = g * SLOT + r
                    value = jnp.where(masks[g - 1], flats[which][at : at + SUB], value)
                pick.append(value)
                yield
            others.append(jnp.concatenate(pick, axis=0))
        second, third, fourth = others
        third_re, third_im = held_rows(third, branches), held_rows(third[branches:], branches)
        fourth_re, fourth_im = cycled_rows(fourth, branches), cycled_rows(fourth[branches:], branches)
        period = len(fourth_re)
        for v in range(groups):
            are, aim, bre, bim = third_re[v], third_im[v], fourth_re[v % period], fourth_im[v % period]
            pair_out[v * SUB : (v + 1) * SUB, :] = are * bre - aim * bim
            at = pairs + v * SUB
            pair_out[at : at + SUB, :] = -(are * bim + aim * bre)
            yield
        at = 2 * SUB
        single_out[at : at + SLOT, :] = second
        first = jnp.zeros((comps, LANES), jnp.float32)
        for h in range(heads):
            first = jnp.where(head == h, spread[h * comps : (h + 1) * comps], first)
            yield
        tail = spread[heads * comps :]
        first_freq = jnp.sum(
            jnp.where(row_iota(tail.shape[0]) == head, tail, 0.0), axis=0, keepdims=True
        )
        at += SLOT
        single_out[at : at + comps, :] = first
        at += comps
        wanted = [first_freq] + [e[comps : comps + 1] for e in others]
        wanted.append(local.astype(jnp.float32))
        for n, line in enumerate(wanted):
            single_out[at + n : at + n + 1, :] = line
        yield

    def join(single_in, product_out):
        at = 2 * SUB
        second = single_in[at : at + comps, :]
        at += SLOT
        first = single_in[at : at + comps, :]
        at += comps
        f1, f2, f3, f4, local = (single_in[at + n : at + n + 1, :] for n in range(5))
        yield
        mismatch = f1 + f2 - f3 - f4
        delta = jnp.exp(-((mismatch / smearing) ** 2)) / (smearing * math.sqrt(math.pi))
        yield
        weight = (1.0 + occupation(f2)) * occupation(f3) * occupation(f4) / occupation(f1)
        yield
        at = 2 * pairs
        product_out[at : at + 1, :] = delta * weight / (f1 * f2 * f3 * f4)
        product_out[at + 1 : at + 2, :] = local
        yield
        first_re, first_im = held_rows(first, branches), held_rows(first[branches:], branches)
        second_re, second_im = cycled_rows(second, branches), cycled_rows(second[branches:], branches)
        period = len(second_re)
        for v in range(groups):
            are, aim, bre, bim = first_re[v], first_im[v], second_re[v % period], second_im[v % period]
            product_out[v * SUB : (v + 1) * SUB, :] = are * bre - aim * bim
            at = pairs + v * SUB
            product_out[at : at + SUB, :] = are * bim + aim * bre
            yield

    def turn(pair_in, single_in, wide_out):
        for k in range(clusters):
            cos_k, sin_k = single_in[k : k + 1, :], single_in[SUB + k : SUB + k + 1, :]
            for v in range(0, groups, 2):
                both = []
                for u in (v, v + 1):
                    re = pair_in[u * SUB : (u + 1) * SUB, :]
                    im = pair_in[pairs + u * SUB : pairs + (u + 1) * SUB, :]
                    both.append((cos_k * re - sin_k * im, cos_k * im + sin_k * re))
                at = k * pairs + v * SUB
                for part in range(2):
                    wide_out[at : at + 2 * SUB, part * LANES : (part + 1) * LANES] = jnp.concatenate(
                        [both[0][part], both[1][part]], axis=0
                    ).astype(jnp.bfloat16)
                yield

    def finish(i, result_in, product_in):
        sum_re = jnp.zeros((SUB, LANES), jnp.float32)
        sum_im = sum_re
        for v in range(groups):
            rows = slice(v * SUB, (v + 1) * SUB)
            nre = product_in[rows, :]
            nim = product_in[pairs + v * SUB : pairs + (v + 1) * SUB, :]
            wre, wim = result_in[rows, :LANES], result_in[rows, LANES:]
            sum_re = sum_re + (nre * wre - nim * wim)
            sum_im = sum_im + (nre * wim + nim * wre)
            yield
        value_re = jnp.sum(sum_re, axis=0, keepdims=True)
        value_im = jnp.sum(sum_im, axis=0, keepdims=True)
        yield
        at = 2 * pairs
        factor = product_in[at : at + 1, :]
        local = product_in[at + 1 : at + 2, :].astype(jnp.int32)
        local = jnp.where(i >= 0, local, -1)
        term = (value_re * value_re + value_im * value_im) * factor
        size = acc.shape[0]
        rest = jnp.where(row_iota(size) == lax.shift_right_arithmetic(local, 7), term, 0.0)
        place[0:1, :] = local
        yield
        for n in range(3):
            part = rest.astype(jnp.bfloat16)
            placed[n * size : (n + 1) * size, :] = part
            rest = rest - part.astype(jnp.float32)
        yield

    def run(*tracks):
        total_steps = max(n for _, n in tracks)
        done = [0] * len(tracks)
        for step in range(1, total_steps + 1):
            for t, (track, n) in enumerate(tracks):
                while done[t] * total_steps < step * n:
                    next(track, None)
                    done[t] += 1

    gather_steps = 3 * LANES
    choose_steps = 20 + groups + heads
    join_steps = 4 + groups
    turn_steps = clusters * groups // 2
    finish_steps = groups + 3

    def drain(*tracks):
        for track in tracks:
            for _ in track:
                pass

    pieces = [(at, min(at + DEPTH, clusters * pairs)) for at in range(0, clusters * pairs, DEPTH)]

    def multiply(wide_in, result_out):
        whole = None
        for low, high in pieces:
            part = jnp.dot(phi[:, low:high], wide_in[low:high, :], preferred_element_type=jnp.float32)
            whole = part if whole is None else whole + part
            yield
        result_out[...] = whole
        yield

    def scatter():
        return lax.dot_general(
            placed[...],
            one_hot(place[0:1, :]),
            (((1,), (1,)), ((), ())),
            preferred_element_type=jnp.float32,
        )

    def add(sums):
        size = acc.shape[0]
        acc[...] += sums[:size] + sums[size : 2 * size] + sums[2 * size :]

    def step(i, turn_of):
        p = turn_of % 2
        load(i + AHEAD + 1, (turn_of + 1) % AHEAD).start()
        load(i + 2, (turn_of + 2) % AHEAD).wait()
        sums = scatter()
        joined = join(single[1 - p], product[1 - p])
        next(joined)
        chosen = choose(i + 1, gathered[1 - p], pair[1 - p], single[1 - p])
        multiplied = multiply(wide[1 - p], result[1 - p])
        turned = turn(pair[p], single[p], wide[p])
        done = finish(i - 2, result[p], product[p])
        rows = gather((turn_of + 2) % AHEAD)
        run(
            (multiplied, len(pieces) + 1),
            (done, finish_steps),
            (chosen, choose_steps),
            (turned, turn_steps),
            (joined, join_steps),
            (rows, gather_steps),
        )
        drain(multiplied, done, chosen, turned, joined, rows)
        add(sums)

    def last_terms(p):
        sums = scatter()
        drain(join(single[1 - p], product[1 - p]), multiply(wide[1 - p], result[1 - p]))
        drain(finish(count - 2, result[p], product[p]))
        add(sums)
        add(scatter())
        drain(finish(count - 1, result[1 - p], product[1 - p]))
        add(scatter())

    for i in range(AHEAD):
        load(i, i).start()
    acc[...] = jnp.zeros_like(acc)
    placed[...] = jnp.zeros_like(placed)
    place[...] = jnp.zeros_like(place)
    fill_table(shard_quarters(vectors, lines), table, base)
    load(0, 0).wait()
    drain(gather(0))
    load(AHEAD, 0).start()
    load(1, 1).wait()
    first, second = choose(0, gathered_a, pair_a, single_a), gather(1)
    run((first, choose_steps), (second, gather_steps))
    drain(first, second)

    def one_round(j, carry):
        step(AHEAD * j, 0)
        for turn_of in range(1, AHEAD):

            @pl.when(AHEAD * j + turn_of < count)
            def _():
                step(AHEAD * j + turn_of, turn_of)

        return carry

    lax.fori_loop(0, lax.div(count + AHEAD - 1, AHEAD), one_round, 0)
    for i in range(2, AHEAD + 1):
        load(0, lax.rem(count + i, AHEAD)).wait()
    even = lax.rem(count, 2) == 0

    @pl.when(even)
    def _():
        last_terms(0)

    @pl.when(jnp.logical_not(even))
    def _():
        last_terms(1)

    out[...] = acc[:heads, :]


def rates_call(branches, base, heads, padded, *args):
    rows, table, phi = args[1], args[3], args[5]
    pairs = branches * branches
    singles = 2 * SUB + SLOT + 2 * branches + SUB
    vmem = pl.BlockSpec(memory_space=pltpu.VMEM)
    smem = pl.BlockSpec(memory_space=pltpu.SMEM)
    loose = pl.BlockSpec(memory_space=pl.ANY)
    rates, _ = pl.pallas_call(
        functools.partial(kernel, branches, base),
        out_shape=[
            jax.ShapeDtypeStruct((heads, LANES), jnp.float32),
            jax.ShapeDtypeStruct(table.shape, table.dtype),
        ],
        in_specs=[smem, loose] + [vmem] * 7,
        out_specs=[vmem, vmem],
        input_output_aliases={3: 1},
        scratch_shapes=[
            *[pltpu.VMEM((3 * LANES, LANES), jnp.float32)] * 2,
            *[pltpu.VMEM((2 * pairs, LANES), jnp.float32)] * 2,
            *[pltpu.VMEM((singles, LANES), jnp.float32)] * 2,
            *[pltpu.VMEM((phi.shape[1], 2 * LANES), jnp.bfloat16)] * 2,
            *[pltpu.VMEM((2 * pairs + SUB, LANES), jnp.float32)] * 2,
            *[pltpu.VMEM((pairs, 2 * LANES), jnp.float32)] * 2,
            pltpu.VMEM((3 * padded, LANES), jnp.bfloat16),
            pltpu.VMEM((SUB, LANES), jnp.int32),
            pltpu.VMEM((padded, LANES), jnp.float32),
            pltpu.SMEM((AHEAD, *rows.shape[1:]), jnp.int32),
            pltpu.SemaphoreType.DMA((AHEAD,)),
        ],
        compiler_params=pltpu.CompilerParams(vmem_limit_bytes=16 * 1024 * 1024),
    )(*args)
    return rates


def body(quartets, counts, eig, freq, phi, cells):
    comps, local = eig.shape
    branches = comps // 2
    shards = lax.axis_size("pb")
    workers = lax.axis_size("wa")
    held, parts, block = quartets.shape
    kept = local // workers
    heads = window(kept)
    clusters = cells.shape[0]
    offset = local * shards // 2
    both = ("pb", "wa")
    lines = freq.reshape(local // LANES, LANES)

    def swap(x):
        return lax.ppermute(x, "wa", [(i, i ^ 1) for i in range(workers)])

    def across(x, even, odd):
        pairs = []
        for p in range(shards):
            for w in range(workers):
                pairs.append((p * workers + w, (p ^ (odd if w % 2 else even)) * workers + w))
        return lax.ppermute(x, both, pairs)

    depth = local // GROUPS
    if shards == GROUPS:
        one = across(eig, 1, 2)
        far = across(one, 2, 1)
        vectors = [eig, one, swap(one), far]
        one_lines = across(lines, 1, 2)
        far_lines = across(lines, shards - 1, shards - 1)
        rows_of = [lines, one_lines, swap(one_lines), far_lines]
    else:
        vectors, rows_of = [eig], [lines]
        for k in range(1, shards):
            vectors.append(across(eig, k, k))
            rows_of.append(across(lines, k, k))

    slots = jnp.arange(held, dtype=jnp.int32)[:, None, None]
    coded = (jnp.where(slots < counts[:, None, None], quartets, -1) - offset).astype(jnp.int16)
    coded = coded.reshape(held * parts, block)
    line_up = [coded]
    for k in range(2, workers, 2):
        line_up.append(lax.ppermute(coded, "wa", [(i, i ^ k) for i in range(workers)]))
    column = jnp.concatenate(line_up, axis=0)
    other_column = swap(column)
    vmem = pl.BlockSpec(memory_space=pltpu.VMEM)
    smem = pl.BlockSpec(memory_space=pltpu.SMEM)
    hbm = pl.BlockSpec(memory_space=pl.ANY)
    far_space = pl.BlockSpec(memory_space=pltpu.HBM)
    total_rows = workers * held * parts
    rows, meta, order = pl.pallas_call(
        functools.partial(prepare, branches, local, kept, offset),
        out_shape=[
            jax.ShapeDtypeStruct((total_rows, LANES), jnp.int32),
            jax.ShapeDtypeStruct((total_rows, LANES), jnp.int32),
            jax.ShapeDtypeStruct((1, total_rows // parts + LANES), jnp.int32),
        ],
        in_specs=[vmem, vmem],
        out_specs=[vmem] * 3,
        compiler_params=pltpu.CompilerParams(vmem_limit_bytes=16 * 1024 * 1024),
    )(column, other_column)
    blocks = total_rows // parts
    padded = -(-heads // 16) * 16
    own_rows = -(-heads * (comps + 1) // 16) * 16
    phi, spread_cells = pl.pallas_call(
        constants,
        out_shape=[
            jax.ShapeDtypeStruct(phi.shape, phi.dtype),
            jax.ShapeDtypeStruct((cells.shape[1], clusters, LANES), jnp.int32),
        ],
        in_specs=[vmem] * 2,
        out_specs=[vmem] * 2,
        compiler_params=pltpu.CompilerParams(vmem_limit_bytes=16 * 1024 * 1024),
    )(phi, cells)
    table, own = pl.pallas_call(
        functools.partial(begin, kept, heads),
        out_shape=[
            jax.ShapeDtypeStruct((shards * depth, LANES), jnp.float32),
            jax.ShapeDtypeStruct((own_rows, LANES), jnp.bfloat16),
        ],
        in_specs=[vmem] * 2,
        out_specs=[vmem] * 2,
        compiler_params=pltpu.CompilerParams(vmem_limit_bytes=16 * 1024 * 1024),
    )(eig, lines)
    final = len(vectors) - 1
    whole = tuple(range(1, final))
    table = pl.pallas_call(
        functools.partial(extend, whole),
        out_shape=jax.ShapeDtypeStruct(table.shape, table.dtype),
        in_specs=[vmem] * (1 + 2 * len(whole)),
        out_specs=vmem,
        input_output_aliases={0: 0},
        compiler_params=pltpu.CompilerParams(vmem_limit_bytes=16 * 1024 * 1024),
    )(table, *vectors[1:final], *rows_of[1:final])
    rates = rates_call(
        branches,
        final * depth,
        heads,
        padded,
        order,
        rows.reshape(blocks, parts, LANES),
        meta.reshape(blocks, parts, LANES),
        table,
        own,
        phi,
        spread_cells,
        vectors[final],
        rows_of[final],
    )
    rates = rates.reshape(heads * LANES)
    if heads * LANES == kept:
        return rates
    return lax.dynamic_slice_in_dim(rates, lax.axis_index("wa") * kept % LANES, kept, 0)


def solution(mesh):
    placed = (P(("pb", "wa"), None, None), P(("pb", "wa")), P(None, "pb"), P("pb"), P(), P())
    return jax.shard_map(
        body, mesh=mesh, in_specs=placed, out_specs=P(("pb", "wa")), check_vma=False
    )
```
